32 devices in a mesh: dp: 1 (over z), tp: 4 (over y), cp: 8 (over x, core).
Axes of the slice: x: 4, y: 4, z: 1, core: 2. Of those that a mesh axis runs over, the one named last changes fastest.
The devices are a block of a 4x4x8 slice.
Arguments:
- x_suffix: bfloat16 [8192, 3072], P(('dp', 'cp'))
- k_prefix: bfloat16 [8192, 8, 128], P(('dp', 'cp'), 'tp')
- v_prefix: bfloat16 [8192, 8, 128], P(('dp', 'cp'), 'tp')
- norm_attn: bfloat16 [3072], replicated
- w_query: bfloat16 [3072, 3072], P(None, 'tp')
- w_key: bfloat16 [3072, 1024], P(None, 'tp')
- w_value: bfloat16 [3072, 1024], P(None, 'tp')
- w_out: bfloat16 [3072, 3072], P('tp')
- norm_mlp: bfloat16 [3072], replicated
- w_gate: bfloat16 [3072, 8192], P(None, 'tp')
- w_up: bfloat16 [3072, 8192], P(None, 'tp')
- w_down: bfloat16 [8192, 3072], P('tp')
Outputs:
- output 1: bfloat16 [8192, 3072], P(('dp', 'cp'))
- output 2: bfloat16 [8192, 8, 128], P(('dp', 'cp'), 'tp')
- output 3: bfloat16 [8192, 8, 128], P(('dp', 'cp'), 'tp')
All inputs are finite; a program needn't handle non-finite values.
Results may differ from the reference program's by a relative error of at most 0.0109944.
Values are sent between devices in bfloat16 or wider.
A program may use at most 768 MiB of HBM per device.

```python
import jax
import jax.numpy as jnp
from jax import lax

D = 3072
HEADS = 24
KV_HEADS = 8
HEAD = 128
FF = 8192
SEQ_GROUPS = 8
PREFIX_DEV = 1024
SUFFIX_BLK = 512

PREFIX = SEQ_GROUPS * PREFIX_DEV
SUFFIX = 2 * SEQ_GROUPS * SUFFIX_BLK
GROUP_RATIO = HEADS // KV_HEADS
ROPE_THETA = 500000.0
NORM_EPS = 1e-5


def setup_inputs(seed: int = 0, part: int = 0) -> dict:
    shared_keys = jax.random.split(jax.random.key(seed), 9)
    part_keys = jax.random.split(jax.random.fold_in(jax.random.key(seed + 1), part), 3)
    out_std = 2.0 * ((PREFIX + SUFFIX // 2) / (HEADS * HEAD)) ** 0.5

    def normal_draw(rng_key, dims, std_dev):
        return (jax.random.normal(rng_key, dims, jnp.float32) * std_dev).astype(jnp.bfloat16)

    def gain_draw(rng_key):
        return jax.random.uniform(rng_key, (D,), jnp.float32, 0.5, 1.5).astype(jnp.bfloat16)

    return {
        'x_suffix': normal_draw(part_keys[0], (SUFFIX, D), 1.0),
        'k_prefix': normal_draw(part_keys[1], (PREFIX, KV_HEADS, HEAD), 1.0),
        'v_prefix': normal_draw(part_keys[2], (PREFIX, KV_HEADS, HEAD), 1.0),
        'norm_attn': gain_draw(shared_keys[0]),
        'w_query': normal_draw(shared_keys[1], (D, HEADS * HEAD), D ** -0.5),
        'w_key': normal_draw(shared_keys[2], (D, KV_HEADS * HEAD), D ** -0.5),
        'w_value': normal_draw(shared_keys[3], (D, KV_HEADS * HEAD), D ** -0.5),
        'w_out': normal_draw(shared_keys[4], (HEADS * HEAD, D), out_std),
        'norm_mlp': gain_draw(shared_keys[5]),
        'w_gate': normal_draw(shared_keys[6], (D, FF), D ** -0.5),
        'w_up': normal_draw(shared_keys[7], (D, FF), D ** -0.5),
        'w_down': normal_draw(shared_keys[8], (FF, D), 2.0 * FF ** -0.5),
    }


def suffix_positions():
    row_ids = jnp.arange(SUFFIX, dtype=jnp.int32)
    owner_dev = row_ids // (2 * SUFFIX_BLK)
    local_row = row_ids % (2 * SUFFIX_BLK)
    blk_idx = jnp.where(local_row < SUFFIX_BLK, owner_dev, 2 * SEQ_GROUPS - 1 - owner_dev)
    return PREFIX + blk_idx * SUFFIX_BLK + local_row % SUFFIX_BLK


def rope_tables(positions):
    inv_freq = ROPE_THETA ** (-jnp.arange(0, HEAD, 2, dtype=jnp.float32) / HEAD)
    angles = positions.astype(jnp.float32)[:, None] * inv_freq[None, :]
    return jnp.cos(angles), jnp.sin(angles)


def apply_rope(values, cos_tab, sin_tab):
    half_dim = HEAD // 2
    first_half = values[..., :half_dim]
    second_half = values[..., half_dim:]
    cos_rows = cos_tab[:, None, :]
    sin_rows = sin_tab[:, None, :]
    return jnp.concatenate([first_half * cos_rows - second_half * sin_rows, second_half * cos_rows + first_half * sin_rows], axis=-1)


def rms_norm(values, gain_vec):
    vals32 = values.astype(jnp.float32)
    inv_rms = lax.rsqrt(jnp.mean(vals32 * vals32, axis=-1, keepdims=True) + NORM_EPS)
    return (vals32 * inv_rms * gain_vec.astype(jnp.float32)).astype(jnp.bfloat16)


def reference(x_suffix, k_prefix, v_prefix, norm_attn, w_query, w_key, w_value, w_out, norm_mlp, w_gate, w_up, w_down):
    positions = suffix_positions()
    cos_tab, sin_tab = rope_tables(positions)
    hidden = rms_norm(x_suffix, norm_attn)
    q_proj = jnp.dot(hidden, w_query, preferred_element_type=jnp.float32).reshape(SUFFIX, HEADS, HEAD)
    q_rot = apply_rope(q_proj, cos_tab, sin_tab).astype(jnp.bfloat16)
    k_proj = jnp.dot(hidden, w_key, preferred_element_type=jnp.float32).reshape(SUFFIX, KV_HEADS, HEAD)
    k_suffix = apply_rope(k_proj, cos_tab, sin_tab).astype(jnp.bfloat16)
    v_suffix = jnp.dot(hidden, w_value, preferred_element_type=jnp.float32).astype(jnp.bfloat16).reshape(SUFFIX, KV_HEADS, HEAD)
    keys_all = jnp.moveaxis(jnp.concatenate([k_prefix, k_suffix], axis=0), 1, 0)
    vals_all = jnp.moveaxis(jnp.concatenate([v_prefix, v_suffix], axis=0), 1, 0)
    key_pos = jnp.concatenate([jnp.arange(PREFIX, dtype=jnp.int32), positions])
    q_blocks = jnp.moveaxis(q_rot.reshape(2 * SEQ_GROUPS, SUFFIX_BLK, KV_HEADS, GROUP_RATIO, HEAD), 2, 1)
    pos_blocks = positions.reshape(2 * SEQ_GROUPS, SUFFIX_BLK)
    score_scale = HEAD ** -0.5

    def attend_block(blk_args):
        q_blk, q_pos = blk_args
        visible = (key_pos[None, :] <= q_pos[:, None])[:, None, :]

        def attend_head(head_args):
            q_head, k_head, v_head = head_args
            scores = jnp.einsum('brd,kd->brk', q_head.astype(jnp.float32), k_head.astype(jnp.float32)) * score_scale
            scores = jnp.where(visible, scores, -jnp.inf)
            row_max = jnp.max(scores, axis=-1, keepdims=True)
            weights = jnp.exp(scores - row_max)
            denom_sum = jnp.sum(weights, axis=-1, keepdims=True)
            numer_sum = jnp.einsum('brk,kd->brd', weights.astype(jnp.bfloat16).astype(jnp.float32), v_head.astype(jnp.float32))
            return (numer_sum / denom_sum).astype(jnp.bfloat16)

        return lax.map(attend_head, (q_blk, keys_all, vals_all))

    attn_heads = lax.map(attend_block, (q_blocks, pos_blocks))
    attn_heads = jnp.moveaxis(attn_heads, 1, 2).reshape(SUFFIX, HEADS * HEAD)
    resid_mid = x_suffix.astype(jnp.float32) + jnp.dot(attn_heads, w_out, preferred_element_type=jnp.float32)
    hidden_mlp = rms_norm(resid_mid, norm_mlp)
    gate_proj = jnp.dot(hidden_mlp, w_gate, preferred_element_type=jnp.float32)
    up_proj = jnp.dot(hidden_mlp, w_up, preferred_element_type=jnp.float32)
    act_mid = (jax.nn.silu(gate_proj) * up_proj).astype(jnp.bfloat16)
    x_out = (resid_mid + jnp.dot(act_mid, w_down, preferred_element_type=jnp.float32)).astype(jnp.bfloat16)
    return (x_out, k_suffix, v_suffix)
```

```python
import functools

import jax
import jax.numpy as jnp
from jax import lax
from jax.experimental import pallas as pl
from jax.experimental.pallas import tpu as pltpu
from jax.sharding import PartitionSpec as P

ROPE_THETA = 500000.0
NORM_EPS = 1e-5
LOG2E = 1.4426950408889634
F32 = jnp.float32
BF16 = jnp.bfloat16
MESH = pl.DeviceIdType.MESH
COLS = 512


def block_positions(owner, groups, blk_len, prefix_len):
    local_row = jnp.arange(2 * blk_len, dtype=jnp.int32)
    blk_idx = jnp.where(local_row < blk_len, owner, 2 * groups - 1 - owner)
    return prefix_len + blk_idx * blk_len + local_row % blk_len


def rms_norm(values, gain_vec):
    vals32 = values.astype(F32)
    inv_rms = lax.rsqrt(jnp.mean(vals32 * vals32, axis=-1, keepdims=True) + NORM_EPS)
    return (vals32 * inv_rms * gain_vec.astype(F32)).astype(BF16)


def fold_rows(values, op):
    rows, cols = values.shape
    return op(values.reshape(rows // 8, 8, cols), axis=0)


def pipeline(n_steps, where, q_ref, keys, vals, m_ref, l_ref, a_ref, s_bufs, p_bufs, x_bufs, c_bufs, depth):
    rows = min(256, depth)

    def scores(t, slot):
        col, key = where(t)
        q = q_ref[:, pl.ds(col, COLS)]
        top = None
        for r in range(0, depth, rows):
            k = keys[pl.ds(pl.multiple_of(key + r, rows), rows), :]
            s = jnp.dot(jnp.concatenate([k, k], axis=1), q, preferred_element_type=F32)
            s_bufs[slot][r : r + rows, :] = s
            t8 = fold_rows(s, jnp.max)
            top = t8 if top is None else jnp.maximum(top, t8)
        x_bufs[slot][...] = top

    def softmax(t, slot):
        col, _ = where(t)
        cols = pl.ds(col, COLS)
        m_old = m_ref[:, cols]
        m_new = jnp.maximum(m_old, jnp.max(x_bufs[slot][...], axis=0, keepdims=True))
        corr = jnp.exp2(m_old - m_new)
        total = None
        for r in range(0, depth, rows):
            p = jnp.exp2(s_bufs[slot][r : r + rows, :] - m_new)
            t8 = fold_rows(p, jnp.sum)
            total = t8 if total is None else total + t8
            p_bufs[slot][r : r + rows, :] = p.astype(BF16)
        l_ref[:, cols] = l_ref[:, cols] * corr + total
        m_ref[:, cols] = m_new
        c_bufs[slot][...] = corr

    def values(t, slot):
        col, key = where(t)
        cols = pl.ds(col, COLS)
        v = vals[:, pl.ds(key, depth)]
        a_ref[:, cols] = a_ref[:, cols] * c_bufs[slot][...] + jnp.dot(v, p_bufs[slot][...], preferred_element_type=F32)

    scores(0, 0)
    if n_steps == 1:
        softmax(0, 0)
        values(0, 0)
        return
    scores(1, 1)
    softmax(0, 0)
    pairs = (n_steps - 2) // 2

    def body(i, carry):
        t = 2 * i
        scores(t + 2, 0)
        softmax(t + 1, 1)
        values(t, 0)
        scores(t + 3, 1)
        softmax(t + 2, 0)
        values(t + 1, 1)
        return carry

    lax.fori_loop(0, pairs, body, 0)
    t = 2 * pairs
    if n_steps % 2:
        scores(t + 2, 0)
        softmax(t + 1, 1)
        values(t, 0)
        softmax(t + 2, 0)
        values(t + 1, 1)
        values(t + 2, 0)
    else:
        softmax(t + 1, 1)
        values(t, 0)
        values(t + 1, 1)


def masked_steps(n_steps, where, q_ref, keys, vals, m_ref, l_ref, a_ref, s_buf, p_buf, depth):
    def body(t, carry):
        col, key = where(t)
        cols = pl.ds(col, COLS)
        k = keys[pl.ds(key, depth), :]
        s = jnp.dot(jnp.concatenate([k, k], axis=1), q_ref[:, cols], preferred_element_type=F32)
        seen = lax.broadcasted_iota(jnp.int32, s.shape, 0) <= lax.broadcasted_iota(jnp.int32, s.shape, 1)
        s = jnp.where(seen, s, -jnp.inf)
        s_buf[...] = s
        m_old = m_ref[:, cols]
        m_new = jnp.maximum(m_old, jnp.max(fold_rows(s, jnp.max), axis=0, keepdims=True))
        corr = jnp.exp2(m_old - m_new)
        p = jnp.exp2(s_buf[...] - m_new)
        l_ref[:, cols] = l_ref[:, cols] * corr + fold_rows(p, jnp.sum)
        m_ref[:, cols] = m_new
        p_buf[...] = p.astype(BF16)
        v = vals[:, pl.ds(key, depth)]
        a_ref[:, cols] = a_ref[:, cols] * corr + jnp.dot(v, p_buf[...], preferred_element_type=F32)
        return carry

    lax.fori_loop(0, n_steps, body, 0)


def attend(plan, q, k_list, v_list, state, depth, last=False, name="attend"):
    n = len(k_list)
    head_dim, n_cols = q.shape[0] // 2, q.shape[1]
    sizes = [k.shape[0] for k in k_list]
    n_keys = sum(sizes)
    first = state is None

    def kernel(*refs):
        q_ref, refs = refs[0], refs[1:]
        k_refs, v_refs, refs = refs[:n], refs[n : 2 * n], refs[2 * n :]
        if not first:
            m_in, l_in, a_in, refs = refs[0], refs[1], refs[2], refs[3:]
        if last:
            o_ref, refs = refs[0], refs[1:]
            m_ref, l_ref, a_ref, refs = refs[0], refs[1], refs[2], refs[3:]
        else:
            m_ref, l_ref, a_ref, refs = refs[0], refs[1], refs[2], refs[3:]
        keys, vals, s0, s1, p0, p1, x0, x1, c0, c1, sems = refs
        copies = []
        off = 0
        for i in range(n):
            copies.append(pltpu.make_async_copy(k_refs[i], keys.at[pl.ds(off, sizes[i]), :], sems.at[2 * i]))
            copies.append(pltpu.make_async_copy(v_refs[i], vals.at[:, pl.ds(off, sizes[i])], sems.at[2 * i + 1]))
            off += sizes[i]
        for c in copies:
            c.start()
        if first:
            m_ref[...] = jnp.full_like(m_ref, -jnp.inf)
            l_ref[...] = jnp.zeros_like(l_ref)
            a_ref[...] = jnp.zeros_like(a_ref)
        else:
            m_ref[...] = m_in[...]
            l_ref[...] = l_in[...]
            a_ref[...] = a_in[...]
        for c in copies:
            c.wait()
        plan(q_ref, keys, vals, m_ref, l_ref, a_ref, (s0, s1), (p0, p1), (x0, x1), (c0, c1))
        if last:
            for col in range(0, n_cols, COLS):
                inv = 1.0 / jnp.sum(l_ref[:, col : col + COLS], axis=0, keepdims=True)
                o_ref[:, col : col + COLS] = (a_ref[:, col : col + COLS] * inv).astype(BF16)

    vmem = pl.BlockSpec(memory_space=pltpu.VMEM)
    hbm = pl.BlockSpec(memory_space=pl.ANY)
    state_shapes = [(1, n_cols), (8, n_cols), (head_dim, n_cols)]
    scratch = [pltpu.VMEM(s, F32) for s in state_shapes] if last else []
    scratch += [pltpu.VMEM((n_keys, head_dim), BF16), pltpu.VMEM((head_dim, n_keys), BF16)]
    scratch += [pltpu.VMEM((depth, COLS), F32)] * 2 + [pltpu.VMEM((depth, COLS), BF16)] * 2
    scratch += [pltpu.VMEM((8, COLS), F32)] * 2 + [pltpu.VMEM((1, COLS), F32)] * 2
    scratch += [pltpu.SemaphoreType.DMA((2 * n,))]
    if last:
        out_shape = [jax.ShapeDtypeStruct((head_dim, n_cols), BF16)]
    else:
        out_shape = [jax.ShapeDtypeStruct(s, F32) for s in state_shapes]
    pairs = n_cols * n_keys
    return pl.pallas_call(
        kernel,
        in_specs=[vmem] + [hbm] * (2 * n) + ([] if first else [vmem] * 3),
        out_specs=[vmem] * len(out_shape),
        out_shape=out_shape,
        scratch_shapes=scratch,
        compiler_params=pltpu.CompilerParams(vmem_limit_bytes=48 * 2**20),
        cost_estimate=pl.CostEstimate(flops=4 * pairs * head_dim, bytes_accessed=6 * 2**20, transcendentals=pairs),
        name=name,
    )(q, *k_list, *v_list, *([] if first else state))


def mlp_call(x_loc, o_all, w_out_all, norm_mlp, w_gate, w_up, w_down, tps):
    rows, d = x_loc.shape
    d_in = o_all.shape[1]
    ff = w_gate.shape[1]
    chunk = 256
    n_chunks = rows // chunk
    quarter = chunk // tps
    half = quarter // 2
    tile = 512
    gate_tile = tile // 2
    n_a, n_b, n_c = d // tile, ff // gate_tile, d // tile
    per = n_a + n_b + n_c
    total = per * n_chunks
    slots = 3

    def kernel(x_hbm, o_hbm, wo_hbm, g_ref, wg_hbm, wu_hbm, wd_hbm, out_hbm, w_buf, o_buf, x_buf, y_buf, h_buf, act_buf, part, got1, got2, y_own, fin,
               w_sem, o_sem, x_sem, s1, r1, s2, r2, s3, r3, s4, r4, c_sem):
        t = lax.axis_index("tp")
        right, left, far = lax.rem(t + 1, tps), lax.rem(t + tps - 1, tps), lax.rem(t + 2, tps)
        barrier = pltpu.get_barrier_semaphore()
        for who in (left, right):
            pl.semaphore_signal(barrier, inc=1, device_id={"tp": who}, device_id_type=MESH)
        pl.semaphore_wait(barrier, 2)

        def w_copies(kind, i, slot):
            if kind == 0:
                return [pltpu.make_async_copy(wo_hbm.at[:, pl.ds(pl.multiple_of(i * tile, tile), tile)], w_buf.at[slot], w_sem.at[slot, 0])]
            if kind == 1:
                at = pl.ds(pl.multiple_of(i * gate_tile, gate_tile), gate_tile)
                return [
                    pltpu.make_async_copy(wg_hbm.at[:, at], w_buf.at[slot, :, pl.ds(0, gate_tile)], w_sem.at[slot, 0]),
                    pltpu.make_async_copy(wu_hbm.at[:, at], w_buf.at[slot, :, pl.ds(gate_tile, gate_tile)], w_sem.at[slot, 1]),
                ]
            return [pltpu.make_async_copy(wd_hbm.at[:, pl.ds(pl.multiple_of(i * tile, tile), tile)], w_buf.at[slot, pl.ds(0, ff)], w_sem.at[slot, 0])]

        def fetch(g):
            i, slot = lax.rem(g, per), lax.rem(g, slots)

            @pl.when((g < total) & (i < n_a))
            def _():
                for c in w_copies(0, i, slot):
                    c.start()

            @pl.when((g < total) & (i >= n_a) & (i < n_a + n_b))
            def _():
                for c in w_copies(1, i - n_a, slot):
                    c.start()

            @pl.when((g < total) & (i >= n_a + n_b))
            def _():
                for c in w_copies(2, i - n_a - n_b, slot):
                    c.start()

        def row_copies(c, slot):
            at = pl.ds(pl.multiple_of(c * chunk, chunk), chunk)
            return [
                pltpu.make_async_copy(o_hbm.at[at], o_buf.at[slot], o_sem.at[slot]),
                pltpu.make_async_copy(x_hbm.at[at], x_buf.at[slot], x_sem.at[slot]),
            ]

        def remote(src, dst, send, recv, who):
            return pltpu.make_async_remote_copy(src_ref=src, dst_ref=dst, send_sem=send, recv_sem=recv, device_id={"tp": who}, device_id_type=MESH)

        def at_rows(q, first, size):
            return pl.ds(pl.multiple_of(q * quarter + first, half), size)

        def first_sends(c):
            return [
                remote(part.at[c, at_rows(far, 0, half)], got1.at[c, 0], s1.at[c, 0], r1.at[c, 0], right),
                remote(part.at[c, at_rows(far, half, half)], got1.at[c, 1], s1.at[c, 1], r1.at[c, 1], left),
                remote(part.at[c, at_rows(right, half, half)], got2.at[c, 0, pl.ds(half, half)], s2.at[c, 0], r2.at[c, 0], right),
                remote(part.at[c, at_rows(left, 0, half)], got2.at[c, 1, pl.ds(0, half)], s2.at[c, 1], r2.at[c, 1], left),
            ]

        def second_sends(c):
            return [
                remote(part.at[c, at_rows(right, 0, half)], got2.at[c, 0, pl.ds(0, half)], s2.at[c, 2], r2.at[c, 2], right),
                remote(part.at[c, at_rows(left, half, half)], got2.at[c, 1, pl.ds(half, half)], s2.at[c, 3], r2.at[c, 3], left),
            ]

        def out_rows(c, q, first, size):
            return out_hbm.at[pl.ds(pl.multiple_of(c * chunk + q * quarter + first, half), size)]

        def gather_sends(c):
            return [
                remote(fin.at[c], out_rows(c, t, 0, quarter), s3.at[c, 0], r3.at[c, 0], right),
                remote(fin.at[c], out_rows(c, t, 0, quarter), s3.at[c, 1], r3.at[c, 1], left),
            ]

        def gather_recvs(c):
            return [
                remote(fin.at[c], out_rows(c, left, 0, quarter), s3.at[c, 0], r3.at[c, 0], right),
                remote(fin.at[c], out_rows(c, right, 0, quarter), s3.at[c, 1], r3.at[c, 1], left),
            ]

        def forward_sends(c):
            return [
                remote(out_rows(c, left, 0, half), out_rows(c, left, 0, half), s4.at[c, 0], r4.at[c, 0], right),
                remote(out_rows(c, right, half, half), out_rows(c, right, half, half), s4.at[c, 1], r4.at[c, 1], left),
            ]

        def forward_recvs(c):
            return [
                remote(out_rows(c, far, 0, half), out_rows(c, far, 0, half), s4.at[c, 0], r4.at[c, 0], right),
                remote(out_rows(c, far, half, half), out_rows(c, far, half, half), s4.at[c, 1], r4.at[c, 1], left),
            ]

        def own_copy(c):
            return pltpu.make_async_copy(fin.at[c], out_rows(c, t, 0, quarter), c_sem.at[c])

        def middle(c):
            one, two = first_sends(c)[:2]
            nxt = second_sends(c)
            one.wait_recv()
            part[c, at_rows(right, 0, half), :] += got1[c, 0]
            nxt[0].start()
            two.wait_recv()
            part[c, at_rows(left, half, half), :] += got1[c, 1]
            nxt[1].start()

        def finish(c):
            for s in first_sends(c)[2:] + second_sends(c):
                s.wait_recv()
            fin[c] = (y_own[c] + (part[c, at_rows(t, 0, quarter), :] + (got2[c, 0] + got2[c, 1]))).astype(BF16)
            own_copy(c).start()
            for s in gather_sends(c):
                s.start()

        def forward(c):
            a, b = gather_recvs(c)
            nxt = forward_sends(c)
            a.wait_recv()
            nxt[0].start()
            b.wait_recv()
            nxt[1].start()

        def drain(c):
            for s in forward_recvs(c):
                s.wait_recv()
            for s in first_sends(c) + second_sends(c) + gather_sends(c) + forward_sends(c):
                s.wait_send()
            own_copy(c).wait()

        for c in row_copies(0, 0):
            c.start()
        fetch(0)
        fetch(1)

        def step(c, carry):
            base = c * per
            row_slot = lax.rem(c, 2)
            for cp in row_copies(c, row_slot):
                cp.wait()

            @pl.when(c + 1 < n_chunks)
            def _():
                for cp in row_copies(c + 1, 1 - row_slot):
                    cp.start()

            def tile_a(i, carry):
                g = base + i
                fetch(g + 2)
                slot = lax.rem(g, slots)
                for cp in w_copies(0, i, slot):
                    cp.wait()
                at = pl.ds(pl.multiple_of(i * tile, tile), tile)
                y_buf[:, at] = x_buf[row_slot, :, at].astype(F32) + jnp.dot(o_buf[row_slot], w_buf[slot], preferred_element_type=F32)
                return carry

            lax.fori_loop(0, n_a, tile_a, 0)

            y_own[c] = y_buf[pl.ds(pl.multiple_of(t * quarter, quarter), quarter), :]

            def norm(i, carry):
                at = pl.ds(pl.multiple_of(i * 32, 32), 32)
                y = y_buf[at, :]
                inv = lax.rsqrt(jnp.mean(y * y, axis=-1, keepdims=True) + NORM_EPS)
                h_buf[at, :] = (y * inv * g_ref[...]).astype(BF16)
                return carry

            lax.fori_loop(0, chunk // 32, norm, 0)

            @pl.when(c >= 2)
            def _():
                forward(c - 2)

            def tile_b(i, carry):
                g = base + n_a + i
                fetch(g + 2)
                slot = lax.rem(g, slots)
                for cp in w_copies(1, i, slot):
                    cp.wait()
                both = jnp.dot(h_buf[...], w_buf[slot], preferred_element_type=F32)
                gate, up = both[:, :gate_tile], both[:, gate_tile:]
                act_buf[:, pl.ds(pl.multiple_of(i * gate_tile, gate_tile), gate_tile)] = (jax.nn.silu(gate) * up).astype(BF16)
                return carry

            lax.fori_loop(0, n_b, tile_b, 0)

            @pl.when(c >= 1)
            def _():
                middle(c - 1)

            def tile_c(i, carry):
                g = base + n_a + n_b + i
                fetch(g + 2)
                slot = lax.rem(g, slots)
                for cp in w_copies(2, i, slot):
                    cp.wait()
                part[c, :, pl.ds(pl.multiple_of(i * tile, tile), tile)] = jnp.dot(act_buf[...], w_buf[slot, 0:ff, :], preferred_element_type=F32)
                return carry

            lax.fori_loop(0, n_c, tile_c, 0)
            for s in first_sends(c):
                s.start()

            @pl.when(c >= 1)
            def _():
                finish(c - 1)

            return carry

        lax.fori_loop(0, n_chunks, step, 0)
        last = n_chunks - 1
        middle(last)
        forward(last - 1)
        finish(last)
        forward(last)

        def end(c, carry):
            drain(c)
            return carry

        lax.fori_loop(0, n_chunks, end, 0)

    hbm = pl.BlockSpec(memory_space=pl.ANY)
    vmem = pl.BlockSpec(memory_space=pltpu.VMEM)
    dma = pltpu.SemaphoreType.DMA
    return pl.pallas_call(
        kernel,
        in_specs=[hbm, hbm, hbm, vmem, hbm, hbm, hbm],
        out_specs=hbm,
        out_shape=jax.ShapeDtypeStruct((rows, d), BF16),
        scratch_shapes=[
            pltpu.VMEM((slots, d_in, tile), BF16),
            pltpu.VMEM((2, chunk, d_in), BF16),
            pltpu.VMEM((2, chunk, d), BF16),
            pltpu.VMEM((chunk, d), F32),
            pltpu.VMEM((chunk, d), BF16),
            pltpu.VMEM((chunk, ff), BF16),
            pltpu.VMEM((n_chunks, chunk, d), F32),
            pltpu.VMEM((n_chunks, 2, half, d), F32),
            pltpu.VMEM((n_chunks, 2, quarter, d), F32),
            pltpu.VMEM((n_chunks, quarter, d), F32),
            pltpu.VMEM((n_chunks, quarter, d), BF16),
            dma((slots, 2)), dma((2,)), dma((2,)),
            dma((n_chunks, 2)), dma((n_chunks, 2)),
            dma((n_chunks, 4)), dma((n_chunks, 4)),
            dma((n_chunks, 2)), dma((n_chunks, 2)),
            dma((n_chunks, 2)), dma((n_chunks, 2)),
            dma((n_chunks,)),
        ],
        compiler_params=pltpu.CompilerParams(collective_id=3, has_side_effects=True, vmem_limit_bytes=62 * 2**20),
        cost_estimate=pl.CostEstimate(flops=2 * rows * (d_in * d + 3 * d * ff), bytes_accessed=2**28, transcendentals=rows * ff),
        name="mlp",
    )(x_loc, o_all, w_out_all, norm_mlp.astype(F32).reshape(1, d), w_gate, w_up, w_down)


def solution(mesh):
    groups = mesh.shape["cp"]
    tps = mesh.shape["tp"]
    chips = groups // 2

    def around(axis_len, step):
        return [(i, (i + step) % axis_len) for i in range(axis_len)]

    swap = [(i, i + 1 - 2 * (i % 2)) for i in range(groups)]

    def partner(v):
        return lax.ppermute(v, "cp", swap)

    def exchange(k, v):
        k_l, v_l = lax.ppermute(k, "cp", around(groups, 2)), lax.ppermute(v, "cp", around(groups, 2))
        k_r, v_r = lax.ppermute(k, "cp", around(groups, -2)), lax.ppermute(v, "cp", around(groups, -2))
        k_o = lax.ppermute(k_l, "cp", around(groups, 2))
        v_o = lax.ppermute(v_r, "cp", around(groups, -2))
        return (k_l, v_l), (k_o, v_o), (k_r, v_r)

    def local_layer(x_loc, kp_loc, vp_loc, norm_attn, w_query, w_key, w_value, w_out, norm_mlp, w_gate, w_up, w_down):
        rows = x_loc.shape[0]
        blk = rows // 2
        pre_dev, kv_loc, hd = kp_loc.shape
        heads_loc = w_query.shape[1] // hd
        ratio = heads_loc // kv_loc
        assert kv_loc == 2 and chips == 4 and blk == COLS
        prefix_len = pre_dev * groups
        me = lax.axis_index("cp")
        core = lax.rem(me, 2)
        chip = lax.div(me, 2)

        def mine(v, axis):
            return lax.dynamic_index_in_dim(v, core, axis, keepdims=False)

        def theirs(v, axis):
            return lax.dynamic_index_in_dim(v, 1 - core, axis, keepdims=False)

        kp_t = kp_loc.reshape(pre_dev, kv_loc, hd)
        vp_t = jnp.transpose(vp_loc, (1, 2, 0))
        kp = jnp.concatenate([mine(kp_t, 1), partner(theirs(kp_t, 1))], axis=0)
        vp = jnp.concatenate([mine(vp_t, 0), partner(theirs(vp_t, 0))], axis=1)
        pre_l, pre_o, pre_r = exchange(kp, vp)

        hidden = rms_norm(x_loc, norm_attn)
        pos = block_positions(me, groups, blk, prefix_len)
        inv_freq = ROPE_THETA ** (-jnp.arange(0, hd, 2, dtype=F32) / hd)
        angles = pos.astype(F32)[:, None] * inv_freq[None, :]
        cos_tab, sin_tab = jnp.cos(angles), jnp.sin(angles)
        half = hd // 2

        k_proj = jnp.dot(hidden, w_key, preferred_element_type=F32).reshape(rows, kv_loc, hd)
        k_a, k_b = k_proj[..., :half], k_proj[..., half:]
        cs, sn = cos_tab[:, None, :], sin_tab[:, None, :]
        k_new = jnp.concatenate([k_a * cs - k_b * sn, k_b * cs + k_a * sn], axis=-1).astype(BF16)
        v_new = jnp.dot(hidden, w_value, preferred_element_type=F32).astype(BF16).reshape(rows, kv_loc, hd)
        v_t = jnp.transpose(v_new, (1, 2, 0))

        q_t = lax.dot_general(w_query, hidden, (((0,), (1,)), ((), ())), preferred_element_type=F32).reshape(kv_loc, ratio, hd, rows)
        q_a, q_b = q_t[:, :, :half, :], q_t[:, :, half:, :]
        cs, sn = cos_tab.T, sin_tab.T
        q_t = lax.reduce_precision(jnp.concatenate([q_a * cs - q_b * sn, q_b * cs + q_a * sn], axis=2), 8, 7).astype(BF16)

        def columns(v):
            return jnp.transpose(v.reshape(ratio, hd, 2, blk), (1, 2, 0, 3)).reshape(hd, 2 * ratio * blk)

        q_all = jnp.concatenate([columns(mine(q_t, 0)), columns(partner(theirs(q_t, 0)))], axis=1)
        q_scaled = q_all.astype(F32) * (LOG2E * hd**-0.5)
        q_hi = lax.reduce_precision(q_scaled, 8, 7)
        q_lo = q_scaled - q_hi
        q2 = jnp.concatenate([q_hi.astype(BF16), q_lo.astype(BF16)], axis=0)

        ks_m, ks_p = mine(k_new, 1), partner(theirs(k_new, 1))
        vs_m, vs_p = mine(v_t, 0), partner(theirs(v_t, 0))
        k_e = jnp.concatenate([ks_m[:blk], ks_p[:blk]], axis=0)
        k_f = jnp.concatenate([ks_m[blk:], ks_p[blk:]], axis=0)
        v_e = jnp.concatenate([vs_m[:, :blk], vs_p[:, :blk]], axis=1)
        v_f = jnp.concatenate([vs_m[:, blk:], vs_p[:, blk:]], axis=1)
        suf_e = exchange(k_e, v_e)
        suf_f = exchange(k_f, v_f)

        n_cols = q2.shape[1]
        side = n_cols // 2
        late = side // 2
        tiles = late // COLS

        def prefix_plan(n_keys, depth):
            per = n_keys // depth

            def where(t):
                return pl.multiple_of(lax.div(t, per) * COLS, COLS), pl.multiple_of(lax.rem(t, per) * depth, depth)

            def plan(*refs):
                pipeline((n_cols // COLS) * per, where, *refs, depth)

            return plan

        def local_plan(q_ref, keys, vals, m_ref, l_ref, a_ref, s, p, x, c):
            own = lax.rem(lax.axis_index("cp"), 2)

            def where(t):
                who, u = lax.div(t, 3 * tiles), lax.rem(t, 3 * tiles)
                tile, which = lax.div(u, 3), lax.rem(u, 3)
                is_late = jnp.where(who == 0, 1 - own, own)
                far = which == 2
                col = who * side + jnp.where(far, is_late, 1) * late + tile * COLS
                key = jnp.where(far, is_late * 2 * COLS + (1 - who) * COLS, which * COLS)
                return pl.multiple_of(col, COLS), pl.multiple_of(key, COLS)

            pipeline(6 * tiles, where, q_ref, keys, vals, m_ref, l_ref, a_ref, s, p, x, c, COLS)

            def diagonal(t):
                who, u = lax.div(t, 2 * tiles), lax.rem(t, 2 * tiles)
                is_late, tile = lax.div(u, tiles), lax.rem(u, tiles)
                col = who * side + is_late * late + tile * COLS
                key = is_late * 2 * COLS + who * COLS
                return pl.multiple_of(col, COLS), pl.multiple_of(key, COLS)

            masked_steps(4 * tiles, diagonal, q_ref, keys, vals, m_ref, l_ref, a_ref, s[0], p[0], COLS)

        def remote_plan(q_ref, keys, vals, m_ref, l_ref, a_ref, s, p, x, c):
            my_chip = lax.div(lax.axis_index("cp"), 2)
            n_rem = chips - 1
            pair = 2 * COLS

            def where(t):
                who, u = lax.div(t, 2 * n_rem * tiles), lax.rem(t, 2 * n_rem * tiles)
                tile, which = lax.div(u, 2 * n_rem), lax.rem(u, 2 * n_rem)
                second = which >= n_rem
                back = jnp.where(second, which - n_rem, which)
                is_late = jnp.where(second & (back + 1 <= my_chip), 0, 1)
                col = who * side + is_late * late + tile * COLS
                key = jnp.where(second & (is_late == 1), (n_rem + back) * pair, back * pair)
                return pl.multiple_of(col, COLS), pl.multiple_of(key, COLS)

            pipeline(4 * n_rem * tiles, where, q_ref, keys, vals, m_ref, l_ref, a_ref, s, p, x, c, pair)

        depth = 2 * COLS
        st = attend(prefix_plan(2 * pre_dev, depth), q2, [kp], [vp], None, depth, name="attend_own")
        st = attend(local_plan, q2, [k_e, k_f], [v_e, v_f], st, COLS, name="attend_local")
        st = attend(prefix_plan(4 * pre_dev, depth), q2, [pre_l[0], pre_r[0]], [pre_l[1], pre_r[1]], st, depth, name="attend_sides")
        st = attend(prefix_plan(2 * pre_dev, depth), q2, [pre_o[0]], [pre_o[1]], st, depth, name="attend_far")
        (o_t,) = attend(
            remote_plan, q2, [e[0] for e in suf_e] + [f[0] for f in suf_f], [e[1] for e in suf_e] + [f[1] for f in suf_f], st, depth, last=True, name="attend_rest"
        )

        def heads(v):
            return jnp.transpose(v.reshape(hd, 2, ratio, blk), (1, 3, 2, 0)).reshape(rows, ratio * hd)

        o_mine = heads(o_t[:, :side])
        o_far = partner(heads(o_t[:, side:]))
        first, second = jnp.where(core == 0, o_mine, o_far), jnp.where(core == 0, o_far, o_mine)
        attn = jnp.concatenate([first, second], axis=1)
        o_all = lax.all_gather(attn, "tp", axis=1, tiled=True)
        w_out_all = lax.all_gather(w_out, "tp", axis=0, tiled=True)
        x_out = mlp_call(x_loc, o_all, w_out_all, norm_mlp, w_gate, w_up, w_down, tps)
        return x_out, k_new, v_new

    row_spec = P(("dp", "cp"), None)
    kv_spec = P(("dp", "cp"), "tp", None)
    col_spec = P(None, "tp")
    row_split = P("tp", None)
    vec_spec = P(None)
    return jax.shard_map(
        local_layer,
        mesh=mesh,
        in_specs=(row_spec, kv_spec, kv_spec, vec_spec, col_spec, col_spec, col_spec, row_split, vec_spec, col_spec, col_spec, row_split),
        out_specs=(row_spec, kv_spec, kv_spec),
        check_vma=False,
    )
```

```python
import jax
import jax.numpy as jnp
from jax import lax
from jax.experimental import pallas as pl
from jax.experimental.pallas import tpu as pltpu
from jax.sharding import PartitionSpec as P

ROPE_THETA = 500000.0
NORM_EPS = 1e-5
LOG2E = 1.4426950408889634
F32 = jnp.float32
BF16 = jnp.bfloat16
MESH = pl.DeviceIdType.MESH
LANES = 128
SUB = 8
TILE = 256
NORM_ROWS = 32
WIDE = 512
VMEM_LIMIT = 63 * 2**20
S_LIMIT, V_LIMIT = 60.0, 40.0
HBM = pl.BlockSpec(memory_space=pl.ANY)
VMEM = pl.BlockSpec(memory_space=pltpu.VMEM)
(KP, VP, KE, VE, KL, VL, QE, QL, OE, OL) = range(10)
(K_RIGHT, V_RIGHT, K_LEFT, V_LEFT, K_ON, V_ON) = range(6)
(P_OWN, P_SIB, EARLY, LATE) = range(4)
(UP, DOWN, ON_UP, ON_DOWN) = range(4)


def scoped(name):
    def deco(f):
        def g(*a):
            with jax.named_scope(name):
                return f(*a)

        return g

    return deco


def dma(*shape):
    return pltpu.SemaphoreType.DMA(shape)


def start(copies):
    for c in copies:
        c.start()


def span(at, size, unit=LANES):
    return pl.ds(pl.multiple_of(at, unit), size)


def both(v):
    return lax.rem(v, 2)


def fold_rows(values, op):
    rows, cols = values.shape
    return op(values.reshape(rows // SUB, SUB, cols), axis=0)


def rms(x):
    return x * lax.rsqrt(jnp.mean(x * x, axis=-1, keepdims=True) + NORM_EPS)


def loop(n, body):
    lax.fori_loop(0, n, lambda i, c: (body(i), c)[1], 0)


def remote(src, dst, sems, i, who):
    send, recv = sems
    return pltpu.make_async_remote_copy(src_ref=src, dst_ref=dst, send_sem=send.at[i], recv_sem=recv.at[i], device_id=who, device_id_type=MESH)


def gather_steps(at, sems, ranks, src=None):
    here, up, down, over, size = ranks
    half = size // 2
    to_up, to_down = {"tp": up}, {"tp": down}

    def move(i, rank, first, n, who, other=None):
        ref = at(rank, first, n)
        return remote(ref if other is None else other, ref, sems, i, who)

    sends = [
        move(UP, here, 0, size, to_up, src),
        move(DOWN, here, 0, size, to_down, src),
        move(ON_UP, down, 0, half, to_up),
        move(ON_DOWN, up, half, half, to_down),
    ]
    brings = [
        move(UP, down, 0, size, to_up),
        move(DOWN, up, 0, size, to_down),
        move(ON_UP, over, 0, half, to_up),
        move(ON_DOWN, over, half, half, to_down),
    ]
    return sends, brings


def attention_call(exact, x_loc, kp2, vp2, cos_tab, sin_tab, norm_attn, w_query, w_key, w_value, w_out, groups, tps):
    rows, d = x_loc.shape
    blk = rows // 2
    hd = kp2.shape[1] // 2
    heads = w_query.shape[1] // hd
    ratio = heads // 2
    pre = kp2.shape[0]
    chips = groups // 2
    assert chips == tps == 4 and pre == rows and hd == LANES and ratio == 3
    deep = 2 * blk
    n_wide = heads * hd
    side = ratio * 2 * blk
    half_side = side // 2
    per_chip = 2 * pre
    suf = chips * per_chip
    send = suf + chips * 2 * rows
    send_pre = send + rows
    d_out = w_out.shape[1]
    w_half = d_out // 2
    w_rows = w_out.shape[0]
    scale = LOG2E * hd**-0.5
    n_proj = n_wide + 4 * hd

    def kernel(x_hbm, kp_hbm, vp_hbm, cos_ref, sin_ref, g_ref, wq_hbm, wk_hbm, wv_hbm, wo_hbm,
               k_out, v_out, oe_hbm, ol_hbm, wall_hbm, plain_out,
               w_buf, x_buf, h_0, h_1, q3, keys, vals, vp_buf, l_ref, a_ref, p_0, p_1, o_st, o_snd, size_all, size_tp, *rest):
        if exact:
            m_ref, s_0, s_1, t_0, t_1, c_0, c_1, *rest = rest
        l_sem, x_sem, sw_s, sw_r, x_s, x_r, w_s, w_r, d_s, d_r, o_s, o_r, z_s, z_r, y_s, y_r = rest
        me, t = lax.axis_index("cp"), lax.axis_index("tp")
        core, chip = both(me), lax.div(me, 2)
        sib = {"cp": me + 1 - 2 * core}
        x_right, x_left = {"cp": lax.rem(me + 2, groups)}, {"cp": lax.rem(me + groups - 2, groups)}
        up, down, over = [lax.rem(t + j, tps) for j in (1, tps - 1, 2)]

        def local(i, src, dst):
            return pltpu.make_async_copy(src, dst, l_sem.at[i])

        def x_copy(i):
            return pltpu.make_async_copy(x_hbm.at[span(i * TILE, TILE)], x_buf.at[both(i)], x_sem.at[both(i)])

        vp_copy = local(0, vp_hbm, vp_buf)
        kp_copy = local(1, kp_hbm.at[:, span(core * hd, hd)], keys.at[pl.ds(0, pre)])
        w_copies = [
            local(2, wq_hbm, w_buf.at[:, pl.ds(0, n_wide)]),
            local(3, wk_hbm, w_buf.at[:, pl.ds(n_wide, 2 * hd)]),
            local(4, wv_hbm, w_buf.at[:, pl.ds(n_wide + 2 * hd, 2 * hd)]),
        ]
        start([vp_copy, kp_copy, x_copy(0)] + w_copies + [x_copy(1)])

        greeted = [sib, x_right, x_left, {"tp": up}, {"tp": down}]
        if not exact:
            greeted = [{"cp": lax.rem(me + j, groups)} for j in range(1, groups)] + [{"tp": lax.rem(t + j, tps)} for j in range(1, tps)]
        barrier = pltpu.get_barrier_semaphore()
        for who in greeted:
            pl.semaphore_signal(barrier, inc=1, device_id=who, device_id_type=MESH)

        def w_place(which):
            return lambda rank, first, size: wall_hbm.at[span(rank * w_rows + first, size), span(which * w_half, w_half)]

        w_ranks = (t, up, down, over, w_rows)
        w_sends, w_brings = gather_steps(w_place(core), (w_s, w_r), w_ranks, wo_hbm.at[:, span(core * w_half, w_half)])
        w_theirs = gather_steps(w_place(1 - core), (d_s, d_r), w_ranks)[1]

        def w_share(i):
            ref = w_brings[i].dst_ref
            return remote(ref, ref, (d_s, d_r), i, sib)

        def o_cols(which):
            return span(which * ratio * hd, ratio * hd)

        def swap(i, arriving=False):
            if i == KP:
                src, dst = kp_hbm.at[:, span((1 - core) * hd, hd)], keys.at[pl.ds(pre, pre)]
            elif i == VP:
                src, dst = vals.at[pl.ds(send_pre, pre)], vals.at[pl.ds(pre, pre)]
            elif i in (KE, VE, KL, VL):
                buf, late = keys if i in (KE, KL) else vals, i in (KL, VL)
                src, dst = buf.at[pl.ds(send + late * blk, blk)], buf.at[pl.ds(suf + late * deep + blk, blk)]
            elif i in (QE, QL):
                at = pl.ds((i - QE) * half_side, half_side)
                src, dst = q3.at[2, :, at], q3.at[1, :, at]
            else:
                src, dst = o_snd.at[i - OE], o_st.at[i - OE, :, o_cols(1 - core if arriving else core)]
            return remote(src, dst, (sw_s, sw_r), i, sib)

        def region(item, slot):
            if item in (P_OWN, P_SIB):
                return pl.ds(slot * per_chip + item * pre, pre)
            return pl.ds(suf + (2 * slot + item - EARLY) * deep, deep)

        def ring(item):
            plan = {K_RIGHT: (keys, 0, 1, x_right), V_RIGHT: (vals, 0, 1, x_right), K_LEFT: (keys, 0, 3, x_left), V_LEFT: (vals, 0, 3, x_left),
                    K_ON: (keys, 1, 2, x_right), V_ON: (vals, 3, 2, x_left)}
            return [remote(buf.at[region(item, a)], buf.at[region(item, b)], (x_s.at[item], x_r.at[item]), i, who) for i, (buf, a, b, who) in plan.items()]

        @scoped("ring_on")
        def pass_on(item):
            got = ring(item)
            got[K_RIGHT].wait_recv()
            got[K_ON].start()
            got[V_LEFT].wait_recv()
            got[V_ON].start()

        @scoped("wait_sides")
        def sides_here(item):
            got = ring(item)
            got[V_RIGHT].wait_recv()
            got[K_LEFT].wait_recv()

        @scoped("wait_far")
        def far_here(item):
            got = ring(item)
            got[K_ON].wait_recv()
            got[V_ON].wait_recv()

        h_bufs = (h_0, h_1)

        def norm(i, slot):
            g = g_ref[...].astype(F32)[None, :]
            for r in range(0, TILE, NORM_ROWS):
                h_bufs[slot][r : r + NORM_ROWS, :] = (rms(x_buf[slot, r : r + NORM_ROWS, :].astype(F32)) * g).astype(BF16)

        if not exact:
            size_all[0] = jnp.zeros(size_all.shape[1:], F32)

        def note(i, v):
            if not exact:
                size_all[0, i : i + 1, :] = jnp.maximum(size_all[0, i : i + 1, :], v)

        def note_rows(i, v):
            if not exact:
                n2 = jnp.sum(v * v, axis=1, keepdims=True)
                note(i, jnp.broadcast_to(jnp.max(n2, axis=0, keepdims=True), (1, LANES)))

        def project(i, slot):
            h_tile = h_bufs[slot]
            late, sub = lax.div(i, blk // TILE), lax.rem(i, blk // TILE)
            at_rows = span(i * TILE, TILE)
            tab = span(sub * TILE, TILE)
            first = lax.broadcasted_iota(jnp.int32, (TILE, hd), 1) < hd // 2

            def table(ref):
                v = ref[tab, :]
                w = pltpu.roll(v, hd // 2, 1)
                return jnp.where(first == (late == 0), v, w)

            cos, sin = table(cos_ref), table(sin_ref)
            sin = jnp.where(first, -sin, sin)

            def rope(v):
                return v * cos + pltpu.roll(v, hd // 2, 1) * sin

            for pair in range(0, n_proj, 2 * hd):
                out = jnp.dot(h_tile[...], w_buf[:, pair : pair + 2 * hd], preferred_element_type=F32)
                for hh in range(2):
                    v = out[:, hh * hd : (hh + 1) * hd]
                    head = pair // hd + hh
                    lanes = pl.ds(hh * hd, hd)
                    at = jnp.where(core == hh, suf + late * deep, send + late * blk) + sub * TILE
                    if head < heads:
                        q_t = rope(v).astype(BF16).astype(F32).T
                        if not exact:
                            n2 = jnp.max(jnp.sum(fold_rows(q_t * q_t, jnp.sum), axis=0, keepdims=True), axis=1, keepdims=True)
                            note(0, jnp.broadcast_to(n2, (1, LANES)))
                        q_t = q_t * scale
                        hi = q_t.astype(BF16)
                        idx = jnp.where(core == head // ratio, 0, 2)
                        col = span(late * half_side + (head % ratio) * blk + sub * TILE, TILE)
                        q3[idx, pl.ds(0, hd), col] = hi
                        q3[idx, pl.ds(hd, hd), col] = (q_t - hi.astype(F32)).astype(BF16)
                    elif head < heads + 2:
                        k = rope(v).astype(BF16)
                        k_out[at_rows, lanes] = k
                        keys[span(at, TILE), :] = k
                        note_rows(1, k.astype(F32))
                    else:
                        v = v.astype(BF16)
                        v_out[at_rows, lanes] = v
                        v_t = v.astype(F32).T
                        if not exact:
                            note(2, jnp.max(fold_rows(jnp.abs(v.astype(F32)), jnp.max), axis=0, keepdims=True))
                        for b in range(0, TILE, LANES):
                            vals[span(at + b, LANES), :] = v_t[:, b : b + LANES].astype(BF16)

        vp_copy.wait()
        for j in range(2):
            at = jnp.where(core == j, 0, send_pre)
            for b in range(0, pre, LANES):
                v = vp_buf[b : b + LANES, j * hd : (j + 1) * hd].astype(F32)
                vals[span(at + b, LANES), :] = v.T.astype(BF16)
        x_copy(0).wait()
        norm(0, 0)
        kp_copy.wait()
        pl.semaphore_wait(barrier, len(greeted))
        start([swap(KP), swap(VP)] + ring(P_OWN)[:K_ON] + w_sends[:ON_UP])
        if not exact:
            for r in range(0, pre, TILE):
                note(2, jnp.max(fold_rows(jnp.maximum(*[jnp.abs(vp_buf[r : r + TILE, j * hd : (j + 1) * hd].astype(F32)) for j in range(2)]), jnp.max), axis=0, keepdims=True))
                note_rows(1, keys[r : r + TILE, :].astype(F32))
        with jax.named_scope("w_wait"):
            for c in w_copies:
                c.wait()

        n_tiles = rows // TILE

        @scoped("project")
        def two_tiles(j):
            i = 2 * j
            x_copy(i + 1).wait()

            @pl.when(i + 2 < n_tiles)
            def _():
                x_copy(i + 2).start()

            norm(i + 1, 1)
            project(i, 0)

            @pl.when(j == 0)
            def _():
                swap(KP).wait_recv()
                swap(VP).wait_recv()
                start(ring(P_SIB)[:K_ON])

            @pl.when(i + 2 < n_tiles)
            def _():
                x_copy(i + 3).start()
                x_copy(i + 2).wait()

            norm(i + 2, 0)
            project(i + 1, 1)

            @pl.when(j == 0)
            def _():
                start([swap(i) for i in (KE, VE, QE)])

        loop(n_tiles // 2, two_tiles)
        start([swap(i) for i in (KL, VL, QL)])

        def size_copies():
            out = []
            for j in range(1, groups):
                out.append(remote(size_all.at[0], size_all.at[j], (z_s, z_r), j, {"cp": lax.rem(me + j, groups)}))
            return out

        def size_on():
            return [remote(size_tp.at[0], size_tp.at[j], (y_s, y_r), j, {"tp": lax.rem(t + j, tps)}) for j in range(1, tps)]

        def sizes_meet():
            for c in size_copies():
                c.wait_recv()
            size_tp[0] = jnp.max(size_all[...], axis=0)
            start(size_on())

        if not exact:
            start(size_copies())
        if exact:
            m_ref[...] = jnp.full_like(m_ref, -jnp.inf)
        l_ref[...] = jnp.zeros_like(l_ref)
        a_ref[...] = jnp.zeros_like(a_ref)
        with jax.named_scope("swap_wait"):
            for i in range(KE, OE):
                swap(i).wait_recv()

        p_bufs = (p_0, p_1)
        if exact:
            s_bufs, t_bufs, c_bufs = (s_0, s_1), (t_0, t_1), (c_0, c_1)
        part = TILE
        lead = 2 if exact else 1
        unroll = 2 if exact else 4

        def state_at(step):
            who, late, head = step[:3]
            return span(who * side + late * half_side + head * blk, blk)

        def scores(step, slot, shifts):
            who, late, head, key = step
            q = q3[who, :, span(late * half_side + head * blk, blk)]
            cols = state_at(step)
            top = None
            for r in range(0, deep, part):
                k = keys[span(key + r, part), :]
                s = jnp.dot(jnp.concatenate([k, k], axis=1), q, preferred_element_type=F32)
                if shifts is not None:
                    row = lax.broadcasted_iota(jnp.int32, s.shape, 0) + r % blk
                    col = lax.broadcasted_iota(jnp.int32, s.shape, 1) + shifts[r // blk]
                    s = jnp.where(row <= col, s, -jnp.inf)
                if exact:
                    s_bufs[slot][r : r + part, :] = s
                    t8 = fold_rows(s, jnp.max)
                    top = t8 if top is None else jnp.maximum(top, t8)
                else:
                    p = jnp.exp2(s)
                    p_bufs[slot][r : r + part, :] = p.astype(BF16)
                    t8 = fold_rows(p, jnp.sum)
                    top = t8 if top is None else top + t8
            if exact:
                t_bufs[slot][...] = top
            else:
                l_ref[:, cols] += top

        def softmax(step, slot):
            cols = state_at(step)
            m_old = m_ref[:, cols]
            m_new = jnp.maximum(m_old, jnp.max(t_bufs[slot][...], axis=0, keepdims=True))
            corr = jnp.exp2(m_old - m_new)
            total = None
            for r in range(0, deep, part):
                p = jnp.exp2(s_bufs[slot][r : r + part, :] - m_new)
                t8 = fold_rows(p, jnp.sum)
                total = t8 if total is None else total + t8
                p_bufs[slot][r : r + part, :] = p.astype(BF16)
            l_ref[:, cols] = l_ref[:, cols] * corr + total
            m_ref[:, cols] = m_new
            c_bufs[slot][...] = corr

        def values(step, slot):
            cols, key = state_at(step), step[3]
            v = jnp.concatenate([vals[span(key + b, LANES), :] for b in range(0, deep, LANES)], axis=1)
            pv = jnp.dot(v, p_bufs[slot][...], preferred_element_type=F32)
            a_ref[:, cols] = a_ref[:, cols] * c_bufs[slot][...] + pv if exact else a_ref[:, cols] + pv

        def run(n_steps, where, service, mask=None):
            def sc(u, slot):
                scores(where(u), slot, None if mask is None else mask(where(u)))

            def sm(u, slot):
                if exact:
                    softmax(where(u), slot)

            for u in range(lead):
                sc(u, u)
            sm(0, 0)
            slot = lambda u: u % 2

            @scoped("body")
            def body(i):
                service(i)
                for u in range(unroll):
                    sc(unroll * i + u + lead, slot(u + lead))
                    sm(unroll * i + u + 1, slot(u + 1))
                    values(where(unroll * i + u), slot(u))

            trips = (n_steps - lead) // unroll
            loop(trips, body)
            for u in range(unroll * trips, n_steps):
                if u + lead < n_steps:
                    sc(u + lead, slot(u + lead))
                if u + 1 < n_steps:
                    sm(u + 1, slot(u + 1))
                values(where(u), slot(u))

        def own_where(u):
            who, rest = lax.div(u, 2 * ratio), lax.rem(u, 2 * ratio)
            late, head = lax.div(rest, ratio), lax.rem(rest, ratio)
            return who, late, head, suf + late * deep

        def own_mask(step):
            who, late = step[:2]
            q_core = jnp.where(who == 0, core, 1 - core)
            seen = jnp.where(late == 0, q_core, 1 - q_core)
            other = (2 * seen - 1) * blk
            return jnp.where(who == 0, 0, other), jnp.where(who == 0, other, 0)

        with jax.named_scope("run_own"):
            run(4 * ratio, own_where, lambda i: None, own_mask)

        qt = 2 * ratio
        pc = per_chip // deep
        n_sides, n_far = 2 * qt * pc, qt * pc
        b1 = 2 * qt * pc
        b2 = b1 + qt
        b3 = b2 + n_sides
        b4 = b3 + n_far
        b5 = b4 + qt * chip
        b7 = b5 + n_sides + n_far
        b8 = b7 + qt * (chips - 1)
        n_main = b4 + n_sides + n_far + 2 * qt * (chips - 1)

        def where(u):
            late = (u >= b5).astype(jnp.int32)
            v = u - jnp.where(u >= b5, b5 - b2, 0)
            j = v - b2
            q_i, r = lax.div(j, 2 * pc), lax.rem(j, 2 * pc)
            key = (1 + 2 * lax.div(r, pc)) * per_chip + lax.rem(r, pc) * deep
            j = v - b3
            q_i = jnp.where(v < b3, q_i, lax.div(j, pc))
            key = jnp.where(v < b3, key, 2 * per_chip + lax.rem(j, pc) * deep)
            j = u - b4
            here = (u >= b4) & (u < b5)
            q_i = jnp.where(here, lax.rem(j, qt), q_i)
            key = jnp.where(here, suf + (1 + lax.div(j, qt)) * 2 * deep, key)
            j = u - b7
            here = u >= b7
            q_i = jnp.where(here, lax.div(j, chips - 1), q_i)
            key = jnp.where(here, suf + (1 + lax.rem(j, chips - 1)) * 2 * deep, key)
            j = u - b8
            here = u >= b8
            q_i = jnp.where(here, lax.rem(j, qt), q_i)
            key = jnp.where(here, suf + (1 + chip + lax.div(j, qt)) * 2 * deep + deep, key)
            here = u < b2
            q_i = jnp.where(here, u - b1, q_i)
            key = jnp.where(here, suf, key)
            late = jnp.where(here, 1, late)
            tile = lax.div(u, pc)
            here = u < b1
            q_i = jnp.where(here, lax.rem(tile, qt), q_i)
            late = jnp.where(here, lax.div(tile, qt), late)
            key = jnp.where(here, lax.rem(u, pc) * deep, key)
            return lax.div(q_i, ratio), late, lax.rem(q_i, ratio), key

        @scoped("finalize")
        def finalize(h):
            for who in range(2):
                for head in range(ratio):
                    at = who * side + h * half_side + head * blk
                    inv = 1.0 / jnp.sum(l_ref[:, at : at + blk], axis=0, keepdims=True)
                    o = (a_ref[:, at : at + blk] * inv).T.astype(BF16)
                    if who == 0:
                        o_st[h, :, span(core * ratio * hd + head * hd, hd)] = o
                    else:
                        o_snd[h, :, pl.ds(head * hd, hd)] = o
            swap(OE + h).start()

        def o_place(rank, first, size):
            return oe_hbm.at[pl.ds(first, size), span(rank * n_wide, n_wide)]

        o_sends, o_brings = gather_steps(o_place, (o_s, o_r), (t, up, down, over, blk), o_st.at[0])

        def o_keep(h):
            return local(h, o_st.at[h], (oe_hbm, ol_hbm)[h].at[:, span(t * n_wide, n_wide)])

        def at_trip(events):
            def service(i):
                for when, what in events:
                    pl.when(i == when)(lambda what=what: (what(), None)[1])

            return service

        def suffix_early():
            pass_on(P_OWN)
            pass_on(P_SIB)
            start(ring(EARLY)[:K_ON])

        @scoped("svc_w")
        def suffix_late():
            pass_on(EARLY)
            start(ring(LATE)[:K_ON])
            for b in w_brings[:ON_UP]:
                b.wait_recv()
            start(w_sends[ON_UP:])
            start([w_share(UP), w_share(DOWN)])

        def early_suffix_here():
            sides_here(EARLY)
            far_here(EARLY)

        @scoped("svc_o")
        def early_o():
            swap(OE, True).wait_recv()
            start(o_sends[:ON_UP])
            o_keep(0).start()
            pass_on(LATE)

        @scoped("svc_o2")
        def early_o_on():
            for b in o_brings[:ON_UP]:
                b.wait_recv()
            start(o_sends[ON_UP:])
            for i in (ON_UP, ON_DOWN):
                w_brings[i].wait_recv()
                w_share(i).start()

        def late_suffix_here():
            sides_here(LATE)
            far_here(LATE)

        def trip(step):
            return lax.div(step - lead, unroll)

        e_done = lax.div(b5 + unroll - 1, unroll)
        trips = (n_main - lead) // unroll
        events = [
            (3, suffix_early),
            (trip(b2), lambda: [sides_here(P_OWN), sides_here(P_SIB)]),
            (trip(b3) - 2, suffix_late),
            (trip(b3), lambda: [far_here(P_OWN), far_here(P_SIB)]),
            (trip(b4), early_suffix_here),
            (e_done, lambda: finalize(0)),
            (e_done + 2, early_o),
            (e_done + 10, early_o_on),
            (trip(b8), late_suffix_here),
        ]
        if not exact:
            events.append((e_done + 4, sizes_meet))
        with jax.named_scope("run_main"):
            run(n_main, where, at_trip(events))

        pl.when(trip(b8) >= trips)(late_suffix_here)
        finalize(1)

        if exact:
            plain_out[0, 0] = 1
        else:
            for c in size_on():
                c.wait_recv()
            top = jnp.max(jnp.max(size_tp[...], axis=0), axis=1)
            fits = (scale * scale * top[0] * top[1] <= S_LIMIT**2) & (top[2] <= 2.0**V_LIMIT)
            plain_out[0, 0] = fits.astype(jnp.int32)
        with jax.named_scope("tail"):
            swap(OL, True).wait_recv()
            o_keep(1).start()
            for b in o_brings[ON_UP:] + w_theirs:
                b.wait_recv()
            for i in range(OL + 1):
                swap(i).wait_send()
            for item in (P_OWN, P_SIB, EARLY, LATE):
                for c in ring(item):
                    c.wait_send()
            for c in w_sends + [w_share(i) for i in range(4)] + o_sends:
                c.wait_send()
            if not exact:
                for c in size_copies() + size_on():
                    c.wait_send()
            o_keep(0).wait()
            o_keep(1).wait()

    n_state = 2 * side
    scratch = [
        pltpu.VMEM((d, n_proj), BF16),
        pltpu.VMEM((2, TILE, d), BF16),
        pltpu.VMEM((TILE, d), BF16),
        pltpu.VMEM((TILE, d), BF16),
        pltpu.VMEM((3, 2 * hd, side), BF16),
        pltpu.VMEM((send_pre, hd), BF16),
        pltpu.VMEM((send_pre + pre, hd), BF16),
        pltpu.VMEM((pre, 2 * hd), BF16),
        pltpu.VMEM((SUB, n_state), F32),
        pltpu.VMEM((hd, n_state), F32),
        pltpu.VMEM((deep, blk), BF16),
        pltpu.VMEM((deep, blk), BF16),
        pltpu.VMEM((2, blk, n_wide), BF16),
        pltpu.VMEM((2, blk, ratio * hd), BF16),
        pltpu.VMEM((groups, SUB, LANES), F32),
        pltpu.VMEM((tps, SUB, LANES), F32),
    ]
    if exact:
        scratch += [pltpu.VMEM((1, n_state), F32)]
        scratch += [pltpu.VMEM((deep, blk), F32)] * 2 + [pltpu.VMEM((SUB, blk), F32)] * 2 + [pltpu.VMEM((1, blk), F32)] * 2
    scratch += [dma(5), dma(2), dma(10), dma(10), dma(4, 6), dma(4, 6)] + [dma(4)] * 6 + [dma(groups)] * 2 + [dma(tps)] * 2
    shapes = [(rows, 2 * hd)] * 2 + [(blk, tps * n_wide)] * 2 + [(tps * w_rows, d_out)]
    return pl.pallas_call(
        kernel,
        in_specs=[HBM] * 3 + [VMEM] * 3 + [HBM] * 4,
        out_specs=[VMEM, VMEM, HBM, HBM, HBM, pl.BlockSpec(memory_space=pltpu.SMEM)],
        out_shape=[jax.ShapeDtypeStruct(s, BF16) for s in shapes] + [jax.ShapeDtypeStruct((1, 1), jnp.int32)],
        scratch_shapes=scratch,
        compiler_params=pltpu.CompilerParams(collective_id=2 + exact, has_side_effects=True, vmem_limit_bytes=VMEM_LIMIT),
        name="attention_exact" if exact else "attention",
    )(x_loc, kp2, vp2, cos_tab, sin_tab, norm_attn, w_query, w_key, w_value, w_out)


def mlp_call(x_loc, o_early, o_late, w_out, w_out_all, norm_mlp, w_gate, w_up, w_down, tps):
    rows, d = x_loc.shape
    blk, d_in = o_early.shape
    n_wide = d_in // tps
    ff = w_gate.shape[1]
    n_chunks = rows // TILE
    quarter = TILE // tps
    half = quarter // 2
    gate = WIDE // 2
    n_a, n_b, n_c = d // WIDE, ff // gate, d // WIDE
    per = n_a + n_b + n_c
    total = per * n_chunks
    slots = 3
    (FAR_R, FAR_L, NEAR_R, NEAR_L, SUM_R, SUM_L, OUT_R, OUT_L, ON_R, ON_L) = range(10)

    def kernel(x_hbm, oe_hbm, ol_in, wo_hbm, wall_hbm, g_ref, wg_hbm, wu_hbm, wd_hbm, out_hbm, ol_hbm,
               w_buf, o_buf, x_buf, y_buf, h_buf, act_buf, part, got1, got2, y_own, fin, w_sem, row_sem, c_s, c_r, c_sem, o_s, o_r):
        t = lax.axis_index("tp")
        right, left, far = [lax.rem(t + j, tps) for j in (1, tps - 1, 2)]

        def w_copies(kind, i, slot):
            def get(j, src, dst):
                return pltpu.make_async_copy(src, dst, w_sem.at[slot, j])

            if kind == 0:
                cols, out = span(i * WIDE, WIDE), []
                for j in range(tps):
                    at = span(lax.rem(t + j, tps) * n_wide, n_wide)
                    out.append(get(j, wo_hbm.at[:, cols] if j == 0 else wall_hbm.at[at, cols], w_buf.at[slot, at]))
                return out
            if kind == 1:
                at = span(i * gate, gate)
                return [get(j, w.at[:, at], w_buf.at[slot, :, pl.ds(j * gate, gate)]) for j, w in enumerate((wg_hbm, wu_hbm))]
            return [get(0, wd_hbm.at[:, span(i * WIDE, WIDE)], w_buf.at[slot, pl.ds(0, ff)])]

        def fetch(g):
            i, slot = lax.rem(g, per), lax.rem(g, slots)
            for kind, first, n in ((0, 0, n_a), (1, n_a, n_b), (2, n_a + n_b, n_c)):
                pl.when((g < total) & (i >= first) & (i < first + n))(lambda: start(w_copies(kind, i - first, slot)))

        def row_copies(c, slot, src):
            at = span(c * TILE, TILE)
            return [
                pltpu.make_async_copy(x_hbm.at[at], x_buf.at[slot], row_sem.at[0, slot]),
                pltpu.make_async_copy(src.at[span(lax.rem(c * TILE, blk), TILE)], o_buf.at[slot], row_sem.at[1, slot]),
            ]

        def start_rows(c, slot):
            pl.when(c < blk // TILE)(lambda: start(row_copies(c, slot, oe_hbm)))
            pl.when(c >= blk // TILE)(lambda: start(row_copies(c, slot, ol_hbm)))

        start(row_copies(0, 0, oe_hbm))
        fetch(0)
        fetch(1)
        greeted = [{"tp": who} for who in (right, left)]
        barrier = pltpu.get_barrier_semaphore()
        for who in greeted:
            pl.semaphore_signal(barrier, inc=1, device_id=who, device_id_type=MESH)
        pl.semaphore_wait(barrier, len(greeted))

        def ol_place(rank, first, n):
            return ol_hbm.at[pl.ds(first, n), span(rank * n_wide, n_wide)]

        o_sends, o_brings = gather_steps(ol_place, (o_s, o_r), (t, right, left, far, blk))
        start(o_sends[:ON_UP])

        def out_rows(c, q, first, n):
            return out_hbm.at[span(c * TILE + q * quarter + first, n, half)]

        def at_rows(q, first, n):
            return span(q * quarter + first, n, half)

        def moves(c):
            def go(i, src, dst):
                return remote(src, dst, (c_s.at[c], c_r.at[c]), i, {"tp": right if i % 2 == 0 else left})

            def mine(q, first):
                return part.at[c, at_rows(q, first, half)]

            top, low = pl.ds(0, half), pl.ds(half, half)
            sends = {
                FAR_R: (mine(far, 0), got1.at[c, 0]),
                FAR_L: (mine(far, half), got1.at[c, 1]),
                NEAR_R: (mine(right, half), got2.at[c, 0, low]),
                NEAR_L: (mine(left, 0), got2.at[c, 1, top]),
                SUM_R: (mine(right, 0), got2.at[c, 0, top]),
                SUM_L: (mine(left, half), got2.at[c, 1, low]),
                OUT_R: (fin.at[c], out_rows(c, t, 0, quarter)),
                OUT_L: (fin.at[c], out_rows(c, t, 0, quarter)),
                ON_R: (out_rows(c, left, 0, half), out_rows(c, left, 0, half)),
                ON_L: (out_rows(c, right, half, half), out_rows(c, right, half, half)),
            }
            brings = {
                OUT_R: (fin.at[c], out_rows(c, left, 0, quarter)),
                OUT_L: (fin.at[c], out_rows(c, right, 0, quarter)),
                ON_R: (out_rows(c, far, 0, half), out_rows(c, far, 0, half)),
                ON_L: (out_rows(c, far, half, half), out_rows(c, far, half, half)),
            }
            return [go(i, *s) for i, s in sends.items()], {i: go(i, *s) for i, s in brings.items()}

        def own_copy(c):
            return pltpu.make_async_copy(fin.at[c], out_rows(c, t, 0, quarter), c_sem.at[c])

        @scoped("middle")
        def middle(c):
            m = moves(c)[0]
            for way, q, first in ((0, right, 0), (1, left, half)):
                m[FAR_R + way].wait_recv()
                part[c, at_rows(q, first, half), :] += got1[c, way]
                m[SUM_R + way].start()

        @scoped("finish")
        def finish(c):
            m = moves(c)[0]
            for i in (NEAR_R, NEAR_L, SUM_R, SUM_L):
                m[i].wait_recv()
            fin[c] = (y_own[c] + (part[c, at_rows(t, 0, quarter), :] + (got2[c, 0] + got2[c, 1]))).astype(BF16)
            own_copy(c).start()
            start(m[OUT_R:ON_R])

        @scoped("forward")
        def forward(c):
            m, b = moves(c)
            for way in range(2):
                b[OUT_R + way].wait_recv()
                m[ON_R + way].start()

        @scoped("drain")
        def drain(c):
            m, b = moves(c)
            b[ON_R].wait_recv()
            b[ON_L].wait_recv()
            for s in m:
                s.wait_send()
            own_copy(c).wait()

        def tiles(n, base, kind, body):
            @scoped("tile_" + "abc"[kind])
            def one(i):
                g = base + i
                fetch(g + 2)
                slot = lax.rem(g, slots)
                for cp in w_copies(kind, i, slot):
                    cp.wait()
                body(i, slot)

            loop(n, one)

        def step(c):
            base = c * per
            row_slot = both(c)
            for cp in row_copies(0, row_slot, oe_hbm):
                cp.wait()

            def tile_a(i, slot):
                at = span(i * WIDE, WIDE)
                y_buf[:, at] = x_buf[row_slot, :, at].astype(F32) + jnp.dot(o_buf[row_slot], w_buf[slot], preferred_element_type=F32)

            tiles(n_a, base, 0, tile_a)
            y_own[c] = y_buf[span(t * quarter, quarter, quarter), :]

            def norm(i):
                at = span(i * NORM_ROWS, NORM_ROWS, NORM_ROWS)
                h_buf[at, :] = (rms(y_buf[at, :]) * g_ref[...].astype(F32)[None, :]).astype(BF16)

            loop(TILE // NORM_ROWS, norm)
            pl.when(c >= 1)(lambda: middle(c - 1))

            def tile_b(i, slot):
                pair = jnp.dot(h_buf[...], w_buf[slot], preferred_element_type=F32)
                act_buf[:, span(i * gate, gate)] = (jax.nn.silu(pair[:, :gate]) * pair[:, gate:]).astype(BF16)

            tiles(n_b, base + n_a, 1, tile_b)
            pl.when(c >= 2)(lambda: forward(c - 2))

            @pl.when(c == 0)
            def _():
                for b, s in zip(o_brings, o_sends[ON_UP:]):
                    b.wait_recv()
                    s.start()

            @pl.when(c == 1)
            def _():
                for b in o_brings[ON_UP:]:
                    b.wait_recv()

            pl.when(c + 1 < n_chunks)(lambda: start_rows(c + 1, 1 - row_slot))

            def tile_c(i, slot):
                part[c, :, span(i * WIDE, WIDE)] = jnp.dot(act_buf[...], w_buf[slot, 0:ff, :], preferred_element_type=F32)

            tiles(n_c, base + n_a + n_b, 2, tile_c)
            start(moves(c)[0][:SUM_R])
            pl.when(c >= 1)(lambda: finish(c - 1))

        loop(n_chunks, step)
        last = n_chunks - 1
        middle(last)
        forward(last - 1)
        finish(last)
        forward(last)
        loop(n_chunks, drain)
        for s in o_sends:
            s.wait_send()

    return pl.pallas_call(
        kernel,
        in_specs=[HBM] * 5 + [VMEM] + [HBM] * 3,
        out_specs=[HBM, HBM],
        out_shape=[jax.ShapeDtypeStruct((rows, d), BF16), jax.ShapeDtypeStruct(o_late.shape, BF16)],
        input_output_aliases={2: 1},
        scratch_shapes=[
            pltpu.VMEM((slots, d_in, WIDE), BF16),
            pltpu.VMEM((2, TILE, d_in), BF16),
            pltpu.VMEM((2, TILE, d), BF16),
            pltpu.VMEM((TILE, d), F32),
            pltpu.VMEM((TILE, d), BF16),
            pltpu.VMEM((TILE, ff), BF16),
            pltpu.VMEM((n_chunks, TILE, d), F32),
            pltpu.VMEM((n_chunks, 2, half, d), F32),
            pltpu.VMEM((n_chunks, 2, quarter, d), F32),
            pltpu.VMEM((n_chunks, quarter, d), F32),
            pltpu.VMEM((n_chunks, quarter, d), BF16),
            dma(slots, tps), dma(2, 2), dma(n_chunks, 10), dma(n_chunks, 10), dma(n_chunks), dma(4), dma(4),
        ],
        compiler_params=pltpu.CompilerParams(collective_id=4, has_side_effects=True, vmem_limit_bytes=VMEM_LIMIT),
        name="mlp",
    )(x_loc, o_early, o_late, w_out, w_out_all, norm_mlp, w_gate, w_up, w_down)


def angle_tables(owner, groups, blk, prefix_len, hd):
    lane = jnp.arange(hd, dtype=jnp.int32)
    early = lane < hd // 2
    block = jnp.where(early, owner, 2 * groups - 1 - owner)
    pos = prefix_len + block[None, :] * blk + jnp.arange(blk, dtype=jnp.int32)[:, None]
    inv_freq = ROPE_THETA ** (-jnp.arange(0, hd, 2, dtype=F32) / hd)
    angles = pos.astype(F32) * jnp.concatenate([inv_freq, inv_freq])[None, :]
    return jnp.cos(angles), jnp.sin(angles)


def solution(mesh):
    groups = mesh.shape["cp"]
    tps = mesh.shape["tp"]

    def local_layer(x_loc, kp_loc, vp_loc, norm_attn, w_query, w_key, w_value, w_out, norm_mlp, w_gate, w_up, w_down):
        rows = x_loc.shape[0]
        pre_dev, kv_loc, hd = kp_loc.shape
        flat = (pre_dev, kv_loc * hd)
        tables = angle_tables(lax.axis_index("cp"), groups, rows // 2, pre_dev * groups, hd)

        def attention(exact):
            return attention_call(
                exact, x_loc, kp_loc.reshape(flat), vp_loc.reshape(flat), *tables, norm_attn, w_query, w_key, w_value, w_out, groups, tps
            )

        k_new, v_new, o_early, o_late, w_out_all, plain = attention(False)
        o_early, o_late = lax.cond(plain[0, 0] == 1, lambda: (o_early, o_late), lambda: tuple(attention(True)[2:4]))
        x_out = mlp_call(x_loc, o_early, o_late, w_out, w_out_all, norm_mlp, w_gate, w_up, w_down, tps)[0]
        return x_out, k_new.reshape(rows, kv_loc, hd), v_new.reshape(rows, kv_loc, hd)

    row_spec = P(("dp", "cp"), None)
    kv_spec = P(("dp", "cp"), "tp", None)
    col_spec = P(None, "tp")
    row_split = P("tp", None)
    vec_spec = P(None)
    return jax.shard_map(
        local_layer,
        mesh=mesh,
        in_specs=(row_spec, kv_spec, kv_spec, vec_spec, col_spec, col_spec, col_spec, row_split, vec_spec, col_spec, col_spec, row_split),
        out_specs=(row_spec, kv_spec, kv_spec),
        check_vma=False,
    )
```

```python
import jax
import jax.numpy as jnp
from jax import lax
from jax.experimental import pallas as pl
from jax.experimental.pallas import tpu as pltpu
from jax.sharding import PartitionSpec as P

ROPE_THETA = 500000.0
NORM_EPS = 1e-5
LOG2E = 1.4426950408889634
F32 = jnp.float32
BF16 = jnp.bfloat16
MESH = pl.DeviceIdType.MESH
LANES = 128
SUB = 8
TILE = 256
NORM_ROWS = 32
WIDE = 512
VMEM_LIMIT = 67043328
S_LIMIT, V_LIMIT = 60.0, 40.0
HBM = pl.BlockSpec(memory_space=pl.ANY)
VMEM = pl.BlockSpec(memory_space=pltpu.VMEM)
(KP, VP, KE, VE, KL, VL, QE, QL, OE, OL) = range(10)
(K_RIGHT, V_RIGHT, K_LEFT, V_LEFT, K_ON, V_ON) = range(6)
(P_OWN, P_SIB, EARLY, LATE) = range(4)
(UP, DOWN, ON_UP, ON_DOWN) = range(4)
(FAR_R, FAR_L, NEAR_R, NEAR_L, SUM_R, SUM_L, OUT_R, OUT_L, ON_R, ON_L) = range(10)


def scoped(name):
    def deco(f):
        def g(*a):
            with jax.named_scope(name):
                return f(*a)

        return g

    return deco


def dma(*shape):
    return pltpu.SemaphoreType.DMA(shape)


def start(copies):
    for c in copies:
        c.start()


def span(at, size, unit=LANES):
    return pl.ds(pl.multiple_of(at, unit), size)


def both(v):
    return lax.rem(v, 2)


def fold_rows(values, op):
    rows, cols = values.shape
    return op(values.reshape(rows // SUB, SUB, cols), axis=0)


def rms(x):
    return x * lax.rsqrt(jnp.mean(x * x, axis=-1, keepdims=True) + NORM_EPS)


def loop(n, body):
    lax.fori_loop(0, n, lambda i, c: (body(i), c)[1], 0)


def remote(src, dst, sems, i, who):
    send, recv = sems
    return pltpu.make_async_remote_copy(src_ref=src, dst_ref=dst, send_sem=send.at[i], recv_sem=recv.at[i], device_id=who, device_id_type=MESH)


def gather_steps(at, sems, ranks, src=None):
    here, up, down, over, size = ranks
    half = size // 2
    to_up, to_down = {"tp": up}, {"tp": down}

    def move(i, rank, first, n, who, other=None):
        ref = at(rank, first, n)
        return remote(ref if other is None else other, ref, sems, i, who)

    sends = [
        move(UP, here, 0, size, to_up, src),
        move(DOWN, here, 0, size, to_down, src),
        move(ON_UP, down, 0, half, to_up),
        move(ON_DOWN, up, half, half, to_down),
    ]
    brings = [
        move(UP, down, 0, size, to_up),
        move(DOWN, up, 0, size, to_down),
        move(ON_UP, over, 0, half, to_up),
        move(ON_DOWN, over, half, half, to_down),
    ]
    return sends, brings


def layer_call(exact, x_loc, kp2, vp2, cos_tab, sin_tab, norm_attn, w_query, w_key, w_value, w_out, norm_mlp, w_gate, w_up, w_down, groups, tps):
    rows, d = x_loc.shape
    blk = rows // 2
    hd = kp2.shape[2]
    heads = w_query.shape[1] // hd
    ratio = heads // 2
    pre = kp2.shape[0]
    chips = groups // 2
    assert chips == tps == 4 and pre == rows and hd == LANES and ratio == 3
    deep = 2 * blk
    n_wide = heads * hd
    side = ratio * 2 * blk
    half_side = side // 2
    per_chip = 2 * pre
    suf = chips * per_chip
    send = suf + chips * 2 * rows
    send_pre = send + rows
    d_out = w_out.shape[1]
    w_half = (d_out - WIDE) // 2
    w_rows = w_out.shape[0]
    w_part = w_rows // groups
    scale = LOG2E * hd**-0.5
    n_proj = n_wide + 4 * hd
    d_in = tps * n_wide
    ff = w_gate.shape[1]
    n_chunks = rows // TILE
    quarter = TILE // tps
    half = quarter // 2
    gate = WIDE // 2
    n_a, n_b, n_c = d // WIDE, ff // gate, d // WIDE
    per = n_a + n_b + n_c
    total = per * n_chunks
    slots = 3

    def kernel(x_hbm, kp_hbm, vp_hbm, cos_ref, sin_ref, g_ref, wq_hbm, wk_hbm, wv_hbm, wo_hbm, g2_ref, wg_hbm, wu_hbm, wd_hbm,
               k_out, v_out, out_hbm, o_hbm, wall_hbm, wlast_hbm, plain_out,
               w_buf, x_buf, h_0, h_1, q3, keys, vals, kp_buf, vp_buf, l_ref, a_ref, o_st, o_snd, size_all, size_tp,
               o_buf, act_buf, part, got1, got2, y_own, fin, *rest):
        if exact:
            m_ref, *rest = rest
        l_sem, x_sem, sw_s, sw_r, x_s, x_r, w_s, w_r, d_s, d_r, o_s, o_r, z_s, z_r, y_s, y_r, e_s, e_r, t_sem, c_s, c_r, c_sem = rest
        me, t = lax.axis_index("cp"), lax.axis_index("tp")
        core, chip = both(me), lax.div(me, 2)
        sib = {"cp": me + 1 - 2 * core}
        x_right, x_left = {"cp": lax.rem(me + 2, groups)}, {"cp": lax.rem(me + groups - 2, groups)}
        up, down, over = [lax.rem(t + j, tps) for j in (1, tps - 1, 2)]

        def local(i, src, dst):
            return pltpu.make_async_copy(src, dst, l_sem.at[i])

        def x_copy(i):
            return pltpu.make_async_copy(x_hbm.at[span(i * TILE, TILE)], x_buf.at[both(i)], x_sem.at[both(i)])

        vp_copy = local(0, vp_hbm, vp_buf)
        kp_copy = local(1, kp_hbm, kp_buf)
        pair_w = 2 * hd

        def proj_w(pair):
            return pair * pair_w // WIDE, pl.ds(pair * pair_w % WIDE, pair_w)

        w_copies = []
        for pair in range(n_proj // pair_w):
            src, first = (wq_hbm, pair) if pair < ratio else ((wk_hbm, wv_hbm)[pair - ratio], 0)
            slot, lanes = proj_w(pair)
            w_copies.append(local(2 + pair, src.at[:, pl.ds(first * pair_w, pair_w)], w_buf.at[slot, :, lanes]))
        start([vp_copy, kp_copy, x_copy(0)] + w_copies + [x_copy(1)])

        greeted = [{"cp": lax.rem(me + j, groups)} for j in range(1, groups)] + [{"tp": lax.rem(t + j, tps)} for j in range(1, tps)]
        barrier = pltpu.get_barrier_semaphore()
        for who in greeted:
            pl.semaphore_signal(barrier, inc=1, device_id=who, device_id_type=MESH)

        def w_place(which):
            return lambda rank, first, size: wall_hbm.at[span(rank * w_rows + first, size), span(which * w_half, w_half)]

        w_ranks = (t, up, down, over, w_rows)
        w_sends, w_brings = gather_steps(w_place(core), (w_s, w_r), w_ranks, wo_hbm.at[:, span(core * w_half, w_half)])
        w_theirs = gather_steps(w_place(1 - core), (d_s, d_r), w_ranks)[1]

        def part_rows(who):
            return span(who * w_part, w_part, SUB)

        y_steps, x_steps, d_steps = range(tps - 1), range(tps - 1, 2 * (tps - 1)), range(2 * (tps - 1), 3 * tps - 2)

        def w_last(i, arriving=False):
            if i in y_steps:
                src = wo_hbm.at[part_rows(me), pl.ds(2 * w_half, WIDE)]
                return remote(src, wlast_hbm.at[y_steps[-1] - i, part_rows(me)], (e_s, e_r), i, {"tp": lax.rem(t + i + 1, tps)})
            back = 2 * (i - d_steps[0])
            if i in x_steps:
                back = 2 * (i - y_steps[-1])
                to = {"cp": lax.rem(me + back, groups)}
                owner = lax.rem(me + groups - back, groups) if arriving else me
            else:
                to, owner = sib, lax.rem(me + groups - back, groups)
                if arriving:
                    owner = owner + 1 - 2 * core
            ref = wlast_hbm.at[:, part_rows(owner)]
            return remote(ref, ref, (e_s, e_r), i, to)

        def w_last_round():
            for i in y_steps:
                w_last(i, True).wait_recv()
            start([w_last(i) for i in x_steps] + [w_last(d_steps[0])])

        @scoped("w_last_on")
        def w_last_on():
            for i in x_steps:
                w_last(i, True).wait_recv()
            start([w_last(i) for i in d_steps[1:]])

        @scoped("w_last_here")
        def w_last_here():
            for i in d_steps:
                w_last(i, True).wait_recv()

        def w_share(i):
            ref = w_brings[i].dst_ref
            return remote(ref, ref, (d_s, d_r), i, sib)

        def o_cols(which):
            return span(which * ratio * hd, ratio * hd)

        def swap(i, arriving=False):
            if i == KP:
                src, dst = keys.at[pl.ds(send_pre, pre)], keys.at[pl.ds(pre, pre)]
            elif i == VP:
                src, dst = vals.at[pl.ds(send_pre, pre)], vals.at[pl.ds(pre, pre)]
            elif i in (KE, VE, KL, VL):
                buf, late = keys if i in (KE, KL) else vals, i in (KL, VL)
                src, dst = buf.at[pl.ds(send + late * blk, blk)], buf.at[pl.ds(suf + late * deep + blk, blk)]
            elif i in (QE, QL):
                at = pl.ds((i - QE) * half_side, half_side)
                src, dst = q3.at[2, :, at], q3.at[1, :, at]
            else:
                src, dst = o_snd.at[i - OE], o_st.at[i - OE, :, o_cols(1 - core if arriving else core)]
            return remote(src, dst, (sw_s, sw_r), i, sib)

        def region(item, slot):
            if item in (P_OWN, P_SIB):
                return pl.ds(slot * per_chip + item * pre, pre)
            return pl.ds(suf + (2 * slot + item - EARLY) * deep, deep)

        def ring(item):
            plan = {K_RIGHT: (keys, 0, 1, x_right), V_RIGHT: (vals, 0, 1, x_right), K_LEFT: (keys, 0, 3, x_left), V_LEFT: (vals, 0, 3, x_left),
                    K_ON: (keys, 1, 2, x_right), V_ON: (vals, 3, 2, x_left)}
            return [remote(buf.at[region(item, a)], buf.at[region(item, b)], (x_s.at[item], x_r.at[item]), i, who) for i, (buf, a, b, who) in plan.items()]

        @scoped("ring_on")
        def pass_on(item):
            got = ring(item)
            got[K_RIGHT].wait_recv()
            got[K_ON].start()
            got[V_LEFT].wait_recv()
            got[V_ON].start()

        @scoped("wait_sides")
        def sides_here(item):
            got = ring(item)
            got[V_RIGHT].wait_recv()
            got[K_LEFT].wait_recv()

        @scoped("wait_far")
        def far_here(item):
            got = ring(item)
            got[K_ON].wait_recv()
            got[V_ON].wait_recv()

        h_bufs = (h_0, h_1)

        def norm(i, slot):
            g = g_ref[...].astype(F32)[None, :]
            for r in range(0, TILE, NORM_ROWS):
                h_bufs[slot][r : r + NORM_ROWS, :] = (rms(x_buf[slot, r : r + NORM_ROWS, :].astype(F32)) * g).astype(BF16)

        def project(i, slot):
            h_tile = h_bufs[slot]
            late, sub = lax.div(i, blk // TILE), lax.rem(i, blk // TILE)
            at_rows = span(i * TILE, TILE)
            tab = span(sub * TILE, TILE)
            first = lax.broadcasted_iota(jnp.int32, (TILE, hd), 1) < hd // 2

            def table(ref):
                v = ref[tab, :]
                w = pltpu.roll(v, hd // 2, 1)
                return jnp.where(first == (late == 0), v, w)

            cos, sin = table(cos_ref), table(sin_ref)
            sin = jnp.where(first, -sin, sin)

            def rope(v):
                return v * cos + pltpu.roll(v, hd // 2, 1) * sin

            for pair in range(n_proj // pair_w):
                slot, w_lanes = proj_w(pair)
                out = jnp.dot(h_tile[...], w_buf[slot, :, w_lanes], preferred_element_type=F32)
                heads_new = []
                for hh in range(2):
                    v = out[:, hh * hd : (hh + 1) * hd]
                    head = 2 * pair + hh
                    at = jnp.where(core == hh, suf + late * deep, send + late * blk) + sub * TILE
                    if head < heads:
                        q_t = rope(v).astype(BF16).astype(F32).T
                        if not exact:
                            n2 = jnp.max(jnp.sum(fold_rows(q_t * q_t, jnp.sum), axis=0, keepdims=True), axis=1, keepdims=True)
                            note(0, jnp.broadcast_to(n2, (1, LANES)))
                        q_t = q_t * scale
                        hi = q_t.astype(BF16)
                        idx = jnp.where(core == head // ratio, 0, 2)
                        col = span(late * half_side + (head % ratio) * blk + sub * TILE, TILE)
                        q3[idx, pl.ds(0, hd), col] = hi
                        q3[idx, pl.ds(hd, hd), col] = (q_t - hi.astype(F32)).astype(BF16)
                    elif head < heads + 2:
                        k = rope(v).astype(BF16)
                        keys[span(at, TILE), :] = k
                        heads_new.append(k)
                        note_rows(1, k.astype(F32))
                    else:
                        v = v.astype(BF16)
                        heads_new.append(v)
                        v_t = v.astype(F32).T
                        note_size(2, v.astype(F32))
                        for b in range(0, TILE, LANES):
                            vals[span(at + b, LANES), :] = v_t[:, b : b + LANES].astype(BF16)
                if heads_new:
                    (kp_buf, vp_buf)[pair - ratio][at_rows] = jnp.concatenate(heads_new, axis=1).reshape(TILE, 2, hd)

        kp_copy.wait()
        vp_copy.wait()
        if not exact:
            size_all[0] = jnp.zeros(size_all.shape[1:], F32)

        def note(i, v):
            if not exact:
                size_all[0, i : i + 1, :] = jnp.maximum(size_all[0, i : i + 1, :], v)

        def note_rows(i, v):
            if not exact:
                n2 = jnp.sum(v * v, axis=1, keepdims=True)
                note(i, jnp.broadcast_to(jnp.max(n2, axis=0, keepdims=True), (1, LANES)))

        def note_size(i, v):
            if not exact:
                note(i, jnp.max(fold_rows(jnp.abs(v), jnp.max), axis=0, keepdims=True))

        def split_prefix(b):
            rows_b = span(b * LANES, LANES)
            k, v = [buf[rows_b].reshape(LANES, 2 * hd) for buf in (kp_buf, vp_buf)]
            for j in range(2):
                at = span(jnp.where(core == j, 0, send_pre) + b * LANES, LANES)
                k_j, v_j = k[:, j * hd : (j + 1) * hd], v[:, j * hd : (j + 1) * hd].astype(F32)
                keys[at, :] = k_j
                vals[at, :] = v_j.T.astype(BF16)
                note_rows(1, k_j.astype(F32))
                note_size(2, v_j)

        loop(pre // LANES, split_prefix)
        x_copy(0).wait()
        norm(0, 0)
        pl.semaphore_wait(barrier, len(greeted))
        start([swap(KP), swap(VP)] + ring(P_OWN)[:K_ON] + [w_last(i) for i in y_steps] + w_sends[:ON_UP])
        with jax.named_scope("w_wait"):
            for c in w_copies:
                c.wait()

        n_tiles = rows // TILE

        @scoped("project")
        def two_tiles(j):
            i = 2 * j
            x_copy(i + 1).wait()

            @pl.when(i + 2 < n_tiles)
            def _():
                x_copy(i + 2).start()

            norm(i + 1, 1)
            project(i, 0)

            @pl.when(j == 0)
            def _():
                swap(KP).wait_recv()
                swap(VP).wait_recv()
                start(ring(P_SIB)[:K_ON])

            @pl.when(i + 2 < n_tiles)
            def _():
                x_copy(i + 3).start()
                x_copy(i + 2).wait()

            norm(i + 2, 0)
            project(i + 1, 1)

            @pl.when(j == 0)
            def _():
                start([swap(i) for i in (KE, VE, QE)])

        loop(n_tiles // 2, two_tiles)
        start([swap(i) for i in (KL, VL, QL)])
        new_copies = [local(4, kp_buf, k_out), local(5, vp_buf, v_out)]
        start(new_copies)

        def size_copies():
            out = []
            for j in range(1, groups):
                out.append(remote(size_all.at[0], size_all.at[j], (z_s, z_r), j, {"cp": lax.rem(me + j, groups)}))
            return out

        def size_on():
            return [remote(size_tp.at[0], size_tp.at[j], (y_s, y_r), j, {"tp": lax.rem(t + j, tps)}) for j in range(1, tps)]

        def sizes_meet():
            for c in size_copies():
                c.wait_recv()
            size_tp[0] = jnp.max(size_all[...], axis=0)
            start(size_on())

        if not exact:
            start(size_copies())
        if exact:
            m_ref[...] = jnp.full_like(m_ref, -jnp.inf)
        l_ref[...] = jnp.zeros_like(l_ref)
        a_ref[...] = jnp.zeros_like(a_ref)
        with jax.named_scope("swap_wait"):
            for i in range(KE, OE):
                swap(i).wait_recv()

        p_bufs = (o_buf, act_buf)

        def beside(r):
            return pl.ds(r // TILE * blk, blk)

        lead = 0 if exact else 1
        main_unroll = 1 if exact else 4

        def state_at(step):
            who, late, head = step[:3]
            return span(who * side + late * half_side + head * blk, blk)

        def product(step, r, n, shifts):
            who, late, head, key = step
            k = keys[span(key + r, n), :]
            s = jnp.dot(jnp.concatenate([k, k], axis=1), q3[who, :, span(late * half_side + head * blk, blk)], preferred_element_type=F32)
            if shifts is not None:
                row = lax.broadcasted_iota(jnp.int32, s.shape, 0) + r % blk
                col = lax.broadcasted_iota(jnp.int32, s.shape, 1) + shifts[r // blk]
                s = jnp.where(row <= col, s, -jnp.inf)
            return s

        def weights(step, slot, shifts):
            total = None
            for r in range(0, deep, TILE):
                p = jnp.exp2(product(step, r, TILE, shifts))
                p_bufs[slot][:, beside(r)] = p.astype(BF16)
                t8 = fold_rows(p, jnp.sum)
                total = t8 if total is None else total + t8
            l_ref[:, state_at(step)] += total

        def values(step, slot):
            v = jnp.concatenate([vals[span(step[3] + b, LANES), :] for b in range(0, deep, LANES)], axis=1)
            p = jnp.concatenate([p_bufs[slot][:, beside(r)] for r in range(0, deep, TILE)], axis=0)
            a_ref[:, state_at(step)] += jnp.dot(v, p, preferred_element_type=F32)

        def exact_step(step, shifts):
            cols = state_at(step)
            top = m_old = m_ref[:, cols]
            for r in range(0, deep, TILE):
                s = product(step, r, TILE, shifts)
                part[0, :, beside(r)] = s
                top = jnp.maximum(top, jnp.max(s, axis=0, keepdims=True))
            corr = jnp.exp2(m_old - top)
            m_ref[:, cols] = top
            total = l_ref[:, cols] * corr
            for r in range(0, deep, TILE):
                p = jnp.exp2(part[0, :, beside(r)] - top)
                o_buf[:, beside(r)] = p.astype(BF16)
                total += fold_rows(p, jnp.sum)
            l_ref[:, cols] = total
            a_ref[:, cols] = a_ref[:, cols] * corr
            values(step, 0)

        def run(n_steps, unroll, where, service, mask=None):
            def shifts(step):
                return None if mask is None else mask(step)

            def ahead(u, slot):
                weights(where(u), slot, shifts(where(u)))

            if not exact:
                ahead(0, 0)

            @scoped("body")
            def body(i):
                service(i)
                for j in range(unroll):
                    u = unroll * i + j
                    if exact:
                        exact_step(where(u), shifts(where(u)))
                    else:
                        ahead(u + 1, (j + 1) % 2)
                        values(where(u), j % 2)

            trips = (n_steps - lead) // unroll
            loop(trips, body)
            for u in range(unroll * trips, n_steps):
                if u + 1 < n_steps:
                    ahead(u + 1, (u + 1) % 2)
                values(where(u), u % 2)

        def own_where(u):
            who, rest = lax.div(u, 2 * ratio), lax.rem(u, 2 * ratio)
            late, head = lax.div(rest, ratio), lax.rem(rest, ratio)
            return who, late, head, suf + late * deep

        def own_mask(step):
            who, late = step[:2]
            q_core = jnp.where(who == 0, core, 1 - core)
            seen = jnp.where(late == 0, q_core, 1 - q_core)
            other = (2 * seen - 1) * blk
            return jnp.where(who == 0, 0, other), jnp.where(who == 0, other, 0)

        with jax.named_scope("run_own"):
            run(4 * ratio, 1 if exact else 2, own_where, lambda i: None, own_mask)

        qt = 2 * ratio
        pc = per_chip // deep
        n_rem = chips - 1
        n_near = jnp.minimum(chip, 1) + lax.div(chip, n_rem)
        b1 = 2 * qt * pc
        b2 = b1 + qt
        b4 = b2 + n_rem * qt * pc
        b5 = b4 + qt * n_near
        b6 = b5 + qt * pc
        b7 = b6 + qt * (chip - n_near)
        b8 = b7 + (n_rem - 1) * qt * pc
        b9 = b8 + qt * n_rem
        n_main = b4 + n_rem * qt * pc + 2 * qt * n_rem

        def where(u):
            def prefix(j, skip=0):
                i, r = lax.div(j, qt * pc) + skip, lax.rem(j, qt * pc)
                return lax.div(r, pc), far_last(i) * per_chip + lax.rem(r, pc) * deep

            def far_last(i):
                return jnp.where(i == 0, 1, jnp.where(i == 1, n_rem, 2))

            def suffix(j, back):
                return lax.rem(j, qt), suf + back * 2 * deep

            tile = lax.div(u, pc)
            late = lax.div(tile, qt)
            q_i, key = lax.rem(tile, qt), lax.rem(u, pc) * deep
            j9 = suffix(u - b9, far_last(jnp.minimum(chip, 1) + lax.div(u - b9, qt)))
            for first, is_late, (q_n, key_n) in (
                (b1, 1, (u - b1, suf)),
                (b2, 0, prefix(u - b2)),
                (b4, 0, suffix(u - b4, far_last(lax.div(u - b4, qt)))),
                (b5, 1, prefix(u - b5)),
                (b6, 0, suffix(u - b6, 2)),
                (b7, 1, prefix(u - b7, 1)),
                (b8, 1, (lax.div(u - b8, n_rem), suf + (1 + lax.rem(u - b8, n_rem)) * 2 * deep)),
                (b9, 1, (j9[0], j9[1] + deep)),
            ):
                here = u >= first
                late, q_i, key = [jnp.where(here, a, b) for a, b in ((is_late, late), (q_n, q_i), (key_n, key))]
            return lax.div(q_i, ratio), late, lax.rem(q_i, ratio), key

        @scoped("finalize")
        def finalize(h):
            def one(u):
                who, head = lax.div(u, ratio), lax.rem(u, ratio)
                at = state_at((who, h, head))
                inv = 1.0 / jnp.sum(l_ref[:, at], axis=0, keepdims=True)
                o = (a_ref[:, at] * inv).T.astype(BF16)

                @pl.when(who == 0)
                def _():
                    o_st[h, :, span(core * ratio * hd + head * hd, hd)] = o

                @pl.when(who == 1)
                def _():
                    o_snd[h, :, span(head * hd, hd)] = o

            loop(2 * ratio, one)
            swap(OE + h).start()

        gathers, o_keeps = [], []
        for i, (h, first, n) in enumerate(((0, 0, TILE), (0, TILE, blk - TILE), (1, 0, blk))):
            place = lambda rank, at, size, base=h * blk + first: o_hbm.at[pl.ds(base + at, size), span(rank * n_wide, n_wide)]
            src = o_st.at[h, pl.ds(first, n)]
            gathers.append(gather_steps(place, (o_s.at[i], o_r.at[i]), (t, up, down, over, n), src))
            o_keeps.append(local(i, src, place(t, 0, n)))

        def gather_on(i):
            sends, brings = gathers[i]
            for b, s in zip(brings, sends[ON_UP:]):
                b.wait_recv()
                s.start()

        def gathered(i):
            for b in gathers[i][1][ON_UP:]:
                b.wait_recv()
            o_keeps[i].wait()

        def tile_copies(kind, i, slot):
            def get(j, src, dst):
                return pltpu.make_async_copy(src, dst, t_sem.at[slot, j])

            if kind in (0, 3):
                cols, out = span(i * WIDE, WIDE), []
                for j in range(tps):
                    rank = lax.rem(t + j, tps)
                    at = span(rank * n_wide, n_wide)
                    src = wo_hbm.at[:, cols] if j == 0 else wlast_hbm.at[j - 1] if kind == 3 else wall_hbm.at[at, cols]
                    out.append(get(j, src, w_buf.at[slot, at]))
                return out
            if kind == 1:
                at = span(i * gate, gate)
                return [get(j, w.at[:, at], w_buf.at[slot, :, pl.ds(j * gate, gate)]) for j, w in enumerate((wg_hbm, wu_hbm))]
            return [get(0, wd_hbm.at[:, span(i * WIDE, WIDE)], w_buf.at[slot, pl.ds(0, ff)])]

        def fetch(g):
            i, slot = lax.rem(g, per), lax.rem(g, slots)
            last_a = n_a - 1
            pl.when(g == 3)(w_last_on)
            pl.when(g == last_a)(w_last_here)
            for kind, first, n in ((0, 0, last_a), (3, last_a, 1), (1, n_a, n_b), (2, n_a + n_b, n_c)):
                pl.when((g < total) & (i >= first) & (i < first + n))(lambda: start(tile_copies(kind, last_a if kind == 3 else i - first, slot)))

        def mlp_x(c):
            return pltpu.make_async_copy(x_hbm.at[span(c * TILE, TILE)], x_buf.at[both(c)], x_sem.at[both(c)])

        def start_x(c):
            mlp_x(c).start()

        def o_rows(c):
            return local(3, o_hbm.at[span(c * TILE, TILE)], o_buf)

        def out_rows(c, q, first, n):
            return out_hbm.at[span(c * TILE + q * quarter + first, n, half)]

        def at_rows(q, first, n):
            return span(q * quarter + first, n, half)

        def moves(c):
            def go(i, src, dst):
                return remote(src, dst, (c_s.at[c], c_r.at[c]), i, {"tp": up if i % 2 == 0 else down})

            def mine(q, first):
                return part.at[both(c), at_rows(q, first, half)]

            top, low = pl.ds(0, half), pl.ds(half, half)
            sends = {
                FAR_R: (mine(over, 0), got1.at[c, 0]),
                FAR_L: (mine(over, half), got1.at[c, 1]),
                NEAR_R: (mine(up, half), got2.at[c, 0, low]),
                NEAR_L: (mine(down, 0), got2.at[c, 1, top]),
                SUM_R: (mine(up, 0), got2.at[c, 0, top]),
                SUM_L: (mine(down, half), got2.at[c, 1, low]),
                OUT_R: (fin.at[c], out_rows(c, t, 0, quarter)),
                OUT_L: (fin.at[c], out_rows(c, t, 0, quarter)),
                ON_R: (out_rows(c, down, 0, half), out_rows(c, down, 0, half)),
                ON_L: (out_rows(c, up, half, half), out_rows(c, up, half, half)),
            }
            brings = {
                OUT_R: (fin.at[c], out_rows(c, down, 0, quarter)),
                OUT_L: (fin.at[c], out_rows(c, up, 0, quarter)),
                ON_R: (out_rows(c, over, 0, half), out_rows(c, over, 0, half)),
                ON_L: (out_rows(c, over, half, half), out_rows(c, over, half, half)),
            }
            return [go(i, *s) for i, s in sends.items()], {i: go(i, *s) for i, s in brings.items()}

        def own_copy(c):
            return pltpu.make_async_copy(fin.at[c], out_rows(c, t, 0, quarter), c_sem.at[c])

        @scoped("middle")
        def middle(c):
            m = moves(c)[0]
            for way, q, first in ((0, up, 0), (1, down, half)):
                m[FAR_R + way].wait_recv()
                part[both(c), at_rows(q, first, half), :] += got1[c, way]
                m[SUM_R + way].start()

        @scoped("finish")
        def finish(c):
            m = moves(c)[0]
            for i in (NEAR_R, NEAR_L, SUM_R, SUM_L):
                m[i].wait_recv()
            fin[c] = (y_own[both(c)] + (part[both(c), at_rows(t, 0, quarter), :] + (got2[c, 0] + got2[c, 1]))).astype(BF16)
            own_copy(c).start()
            start(m[OUT_R:ON_R])

        @scoped("forward")
        def forward(c):
            m, b = moves(c)
            for way in range(2):
                b[OUT_R + way].wait_recv()
                m[ON_R + way].start()

        @scoped("drain")
        def drain(c):
            m, b = moves(c)
            b[ON_R].wait_recv()
            b[ON_L].wait_recv()
            for s in m[OUT_R:]:
                s.wait_send()
            own_copy(c).wait()

        def release(c):
            for s in moves(c)[0][:OUT_R]:
                s.wait_send()

        def tiles(n, base, kind, body):
            @scoped("tile_" + "abc"[kind])
            def one(i):
                g = base + i
                fetch(g + 2)
                slot = lax.rem(g, slots)
                at = jnp.minimum(i, n_a - 2) if kind == 0 else i
                for cp in tile_copies(kind, at, slot):
                    cp.wait()
                body(i, slot)

            loop(n, one)

        def chunk_step(c):
            base, slot_c = c * per, both(c)
            for i in range(3):
                pl.when(c == i)(lambda i=i: gathered(i))
            o_rows(c).start()
            pl.when(c >= 2)(lambda: release(c - 2))
            mlp_x(c).wait()
            pl.when(c + 1 < n_chunks)(lambda: start_x(c + 1))
            o_rows(c).wait()

            def tile_a(i, slot):
                at = span(i * WIDE, WIDE)
                part[slot_c, :, at] = x_buf[slot_c, :, at].astype(F32) + jnp.dot(o_buf[...], w_buf[slot], preferred_element_type=F32)

            tiles(n_a, base, 0, tile_a)
            y_own[both(c)] = part[slot_c, span(t * quarter, quarter, quarter), :]

            def norm2(i):
                at = span(i * NORM_ROWS, NORM_ROWS, NORM_ROWS)
                h_0[at, :] = (rms(part[slot_c, at, :]) * g2_ref[...].astype(F32)[None, :]).astype(BF16)

            loop(TILE // NORM_ROWS, norm2)
            pl.when(c == 0)(lambda: gather_on(1))
            pl.when(c >= 1)(lambda: middle(c - 1))

            def tile_b(i, slot):
                pair = jnp.dot(h_0[...], w_buf[slot], preferred_element_type=F32)
                act_buf[:, span(i * gate, gate)] = (jax.nn.silu(pair[:, :gate]) * pair[:, gate:]).astype(BF16)

            tiles(n_b, base + n_a, 1, tile_b)
            pl.when(c >= 2)(lambda: forward(c - 2))

            def tile_c(i, slot):
                part[slot_c, :, span(i * WIDE, WIDE)] = jnp.dot(act_buf[...], w_buf[slot, 0:ff, :], preferred_element_type=F32)

            tiles(n_c, base + n_a + n_b, 2, tile_c)
            start(moves(c)[0][:SUM_R])
            pl.when(c == 0)(lambda: gather_on(2))
            pl.when(c >= 1)(lambda: finish(c - 1))

        def at_trip(events):
            def service(i):
                for when, what in events:
                    pl.when(i == when)(lambda what=what: (what(), None)[1])

            return service

        def suffix_early():
            pass_on(P_OWN)
            pass_on(P_SIB)
            start(ring(EARLY)[:K_ON])

        @scoped("w_on")
        def w_on():
            for b, c in zip(w_brings, w_sends[ON_UP:]):
                b.wait_recv()
                c.start()
            start([w_share(UP), w_share(DOWN)])

        def suffix_late():
            pass_on(EARLY)
            start(ring(LATE)[:K_ON])

        @scoped("early_o")
        def early_o():
            swap(OE, True).wait_recv()
            start(gathers[0][0][:ON_UP] + o_keeps[:2])

        @scoped("w_rest")
        def w_rest():
            for i in (ON_UP, ON_DOWN):
                w_brings[i].wait_recv()
                w_share(i).start()

        def trip(step):
            return lax.div(step - lead, main_unroll)

        e_done = lax.div(b7 + main_unroll - 1, main_unroll)
        trips = (n_main - lead) // main_unroll
        events = [
            (trip(qt + 4), suffix_early),
            (trip(b2), lambda: [sides_here(P_OWN), sides_here(P_SIB)]),
            (trip(b4 - qt * pc), lambda: [far_here(P_OWN), far_here(P_SIB)]),
            (trip(b4 - 2 * qt), w_on),
            (trip(b4 - 4), suffix_late),
            (trip(b4), lambda: sides_here(EARLY)),
            (trip(jnp.where(chip < 2, b8, b6)), lambda: far_here(EARLY)),
            (e_done, lambda: finalize(0)),
            (e_done + 1, early_o),
            (trip(n_main - 32), lambda: [pass_on(LATE), w_last_round()]),
            (trip(b9), lambda: sides_here(LATE)),
            (trip(n_main - 20), w_rest),
        ]
        events.append((trip(n_main - 16), lambda: [gather_on(0), start(gathers[1][0][:ON_UP])]))
        far_late = trip(jnp.where(chip < 2, b9 + qt * (2 - chip), n_main))
        events.append((far_late, lambda: far_here(LATE)))
        if not exact:
            events.append((e_done + 2, sizes_meet))
        with jax.named_scope("run_main"):
            run(n_main, main_unroll, where, at_trip(events))

        pl.when(trip(b9) >= trips)(lambda: sides_here(LATE))
        pl.when(far_late >= trips)(lambda: far_here(LATE))
        with jax.named_scope("w_theirs"):
            for b in w_theirs:
                b.wait_recv()
        fetch(0)
        fetch(1)
        start_x(0)
        finalize(1)
        with jax.named_scope("o_on"):
            swap(OL, True).wait_recv()
            start(gathers[2][0][:ON_UP] + o_keeps[2:])
        loop(n_chunks, chunk_step)
        last = n_chunks - 1
        middle(last)
        forward(last - 1)
        finish(last)
        forward(last)
        if exact:
            plain_out[0, 0] = 1
        else:
            for c in size_on():
                c.wait_recv()
            top = jnp.max(jnp.max(size_tp[...], axis=0), axis=1)
            fits = (scale * scale * top[0] * top[1] <= S_LIMIT**2) & (top[2] <= 2.0**V_LIMIT)
            plain_out[0, 0] = fits.astype(jnp.int32)
        with jax.named_scope("tail"):
            for c in new_copies:
                c.wait()
            loop(n_chunks, drain)
            release(last - 1)
            release(last)
            for i in range(OL + 1):
                swap(i).wait_send()
            for item in (P_OWN, P_SIB, EARLY, LATE):
                for c in ring(item):
                    c.wait_send()
            for c in w_sends + [w_share(i) for i in range(4)] + [w_last(i) for i in range(3 * tps - 2)] + sum([g[0] for g in gathers], []):
                c.wait_send()
            if not exact:
                for c in size_copies() + size_on():
                    c.wait_send()

    n_state = 2 * side
    scratch = [
        pltpu.VMEM(shape, BF16)
        for shape in (
            (slots, d_in, WIDE), (2, TILE, d), (TILE, d), (TILE, d), (3, 2 * hd, side), (send_pre + pre, hd), (send_pre + pre, hd), (pre, 2, hd), (pre, 2, hd)
        )
    ]
    scratch += [pltpu.VMEM((SUB, n_state), F32), pltpu.VMEM((hd, n_state), F32)]
    scratch += [pltpu.VMEM(shape, BF16) for shape in ((2, blk, n_wide), (2, blk, ratio * hd))]
    scratch += [pltpu.VMEM((groups, SUB, LANES), F32), pltpu.VMEM((tps, SUB, LANES), F32)]
    scratch += [pltpu.VMEM((TILE, d_in), BF16), pltpu.VMEM((TILE, ff), BF16)]
    scratch += [pltpu.VMEM(shape, F32) for shape in ((2, TILE, d), (n_chunks, 2, half, d), (n_chunks, 2, quarter, d), (2, quarter, d))]
    scratch += [pltpu.VMEM((n_chunks, quarter, d), BF16)]
    if exact:
        scratch += [pltpu.VMEM((1, n_state), F32)]
    scratch += [dma(*n) for n in ((7,), (2,), (10,), (10,), (4, 6), (4, 6), (4,), (4,), (4,), (4,), (3, 4), (3, 4))]
    scratch += [dma(groups)] * 2 + [dma(tps)] * 2 + [dma(3 * tps - 2)] * 2 + [dma(slots, tps), dma(n_chunks, 10), dma(n_chunks, 10), dma(n_chunks)]
    shapes = [(rows, 2, hd)] * 2 + [(rows, d), (rows, d_in), (d_in, 2 * w_half), (tps - 1, w_rows, WIDE)]
    return pl.pallas_call(
        kernel,
        in_specs=[HBM] * 3 + [VMEM] * 3 + [HBM] * 4 + [VMEM] + [HBM] * 3,
        out_specs=[HBM] * 6 + [pl.BlockSpec(memory_space=pltpu.SMEM)],
        out_shape=[jax.ShapeDtypeStruct(s, BF16) for s in shapes] + [jax.ShapeDtypeStruct((1, 1), jnp.int32)],
        scratch_shapes=scratch,
        compiler_params=pltpu.CompilerParams(collective_id=2 + exact, has_side_effects=True, vmem_limit_bytes=VMEM_LIMIT),
        name="layer_exact" if exact else "layer",
    )(x_loc, kp2, vp2, cos_tab, sin_tab, norm_attn, w_query, w_key, w_value, w_out, norm_mlp, w_gate, w_up, w_down)


def angle_tables(owner, groups, blk, prefix_len, hd):
    lane = jnp.arange(hd, dtype=jnp.int32)
    early = lane < hd // 2
    block = jnp.where(early, owner, 2 * groups - 1 - owner)
    pos = prefix_len + block[None, :] * blk + jnp.arange(blk, dtype=jnp.int32)[:, None]
    inv_freq = ROPE_THETA ** (-jnp.arange(0, hd, 2, dtype=F32) / hd)
    angles = pos.astype(F32) * jnp.concatenate([inv_freq, inv_freq])[None, :]
    return jnp.cos(angles), jnp.sin(angles)


def solution(mesh):
    groups = mesh.shape["cp"]
    tps = mesh.shape["tp"]

    def local_layer(x_loc, kp_loc, vp_loc, norm_attn, w_query, w_key, w_value, w_out, norm_mlp, w_gate, w_up, w_down):
        rows = x_loc.shape[0]
        pre_dev, kv_loc, hd = kp_loc.shape
        tables = angle_tables(lax.axis_index("cp"), groups, rows // 2, pre_dev * groups, hd)

        def layer(exact):
            return layer_call(
                exact, x_loc, kp_loc, vp_loc, *tables, norm_attn, w_query, w_key, w_value, w_out, norm_mlp, w_gate, w_up, w_down, groups, tps
            )

        k_new, v_new, x_out, _, _, _, plain = layer(False)
        x_out = lax.cond(plain[0, 0] == 1, lambda: x_out, lambda: layer(True)[2])
        return x_out, k_new, v_new

    row_spec = P(("dp", "cp"), None)
    kv_spec = P(("dp", "cp"), "tp", None)
    col_spec = P(None, "tp")
    row_split = P("tp", None)
    vec_spec = P(None)
    return jax.shard_map(
        local_layer,
        mesh=mesh,
        in_specs=(row_spec, kv_spec, kv_spec, vec_spec, col_spec, col_spec, col_spec, row_split, vec_spec, col_spec, col_spec, row_split),
        out_specs=(row_spec, kv_spec, kv_spec),
        check_vma=False,
    )
```

```python
import jax
import jax.numpy as jnp
from jax import lax
from jax.experimental import pallas as pl
from jax.experimental.pallas import tpu as pltpu
from jax.sharding import PartitionSpec as P

ROPE_THETA = 500000.0
NORM_EPS = 1e-5
LOG2E = 1.4426950408889634
F32 = jnp.float32
BF16 = jnp.bfloat16
MESH = pl.DeviceIdType.MESH
LANES = 128
PAIR = 2
SUB = 8
TILE = 256
NORM_ROWS = 32
WIDE = 512
VMEM_LIMIT = 67043328
S_LIMIT, V_LIMIT = 60.0, 40.0
HBM = pl.BlockSpec(memory_space=pl.ANY)
VMEM = pl.BlockSpec(memory_space=pltpu.VMEM)
(KP, VP, KE, VE, KL, VL, QE, QL, OE, OL) = range(10)
(K_RIGHT, V_RIGHT, K_LEFT, V_LEFT, K_ON, V_ON) = range(6)
(P_OWN, P_SIB, EARLY, LATE) = range(4)
(UP, DOWN, ON_UP, ON_DOWN) = range(4)
(FAR_R, FAR_L, NEAR_R, NEAR_L, SUM_R, SUM_L, OUT_R, OUT_L, ON_R, ON_L) = range(10)


def scoped(name):
    def deco(f):
        def g(*a):
            with jax.named_scope(name):
                return f(*a)

        return g

    return deco


def dma(*shape):
    return pltpu.SemaphoreType.DMA(shape)


def start(copies):
    for c in copies:
        c.start()


def span(at, size, unit=LANES):
    return pl.ds(pl.multiple_of(at, unit), size)


def both(v):
    return lax.rem(v, 2)


def fold_rows(values, op):
    rows, cols = values.shape
    return op(values.reshape(rows // SUB, SUB, cols), axis=0)


def rms(x):
    return x * lax.rsqrt(jnp.mean(x * x, axis=-1, keepdims=True) + NORM_EPS)


def loop(n, body):
    lax.fori_loop(0, n, lambda i, c: (body(i), c)[1], 0)


def remote(src, dst, sems, i, who):
    send, recv = sems
    return pltpu.make_async_remote_copy(src_ref=src, dst_ref=dst, send_sem=send.at[i], recv_sem=recv.at[i], device_id=who, device_id_type=MESH)


def gather_steps(at, sems, ranks, src=None):
    here, up, down, over, size = ranks
    half = size // PAIR
    to_up, to_down = {"tp": up}, {"tp": down}

    def move(i, rank, first, n, who, other=None):
        ref = at(rank, first, n)
        return remote(ref if other is None else other, ref, sems, i, who)

    sends = [
        move(UP, here, 0, size, to_up, src),
        move(DOWN, here, 0, size, to_down, src),
        move(ON_UP, down, 0, half, to_up),
        move(ON_DOWN, up, half, half, to_down),
    ]
    brings = [
        move(UP, down, 0, size, to_up),
        move(DOWN, up, 0, size, to_down),
        move(ON_UP, over, 0, half, to_up),
        move(ON_DOWN, over, half, half, to_down),
    ]
    return sends, brings


def layer_call(exact, x_loc, kp2, vp2, cos_tab, sin_tab, norm_attn, w_query, w_key, w_value, w_out, norm_mlp, w_gate, w_up, w_down, groups, tps):
    rows, d = x_loc.shape
    blk = rows // PAIR
    hd = kp2.shape[2]
    heads = w_query.shape[1] // hd
    ratio = heads // PAIR
    pre = kp2.shape[0]
    chips = groups // PAIR
    assert chips == tps == 4 and pre == rows and hd == LANES and ratio == 3
    deep = PAIR * blk
    n_wide = heads * hd
    side = ratio * PAIR * blk
    half_side = side // PAIR
    per_chip = PAIR * pre
    suf = chips * per_chip
    send = suf + chips * PAIR * rows
    send_pre = send + rows
    d_out = w_out.shape[1]
    w_half = (d_out - WIDE) // PAIR
    w_rows = w_out.shape[0]
    w_part = w_rows // groups
    scale = LOG2E * hd**-0.5
    n_proj = n_wide + 4 * hd
    d_in = tps * n_wide
    ff = w_gate.shape[1]
    n_chunks = rows // TILE
    quarter = TILE // tps
    half = quarter // PAIR
    gate = WIDE // PAIR
    n_a, n_b, n_c = d // WIDE, ff // gate, d // WIDE
    per = n_a + n_b + n_c
    total = per * n_chunks
    slots = 4

    def kernel(x_hbm, kp_hbm, vp_hbm, cos_ref, sin_ref, g_ref, wq_hbm, wk_hbm, wv_hbm, wo_hbm, g2_ref, wg_hbm, wu_hbm, wd_hbm,
               k_out, v_out, out_hbm, o_hbm, wall_hbm, wlast_hbm, plain_out,
               w_buf, x_buf, h_0, h_1, q3, keys, vals, kp_buf, vp_buf, l_ref, a_ref, o_st, o_snd, size_all, size_tp,
               o_buf, act_buf, part, got1, got2, y_own, fin, flag, *rest):
        if exact:
            m_ref, *rest = rest
        l_sem, x_sem, sw_s, sw_r, x_s, x_r, w_s, w_r, d_s, d_r, o_s, o_r, z_s, z_r, y_s, y_r, e_s, e_r, t_sem, c_s, c_r, c_sem = rest
        me, t = lax.axis_index("cp"), lax.axis_index("tp")
        core, chip = both(me), lax.div(me, 2)
        sib = {"cp": me + 1 - PAIR * core}
        x_right, x_left = {"cp": lax.rem(me + 2, groups)}, {"cp": lax.rem(me + groups - 2, groups)}
        up, down, over = [lax.rem(t + j, tps) for j in (1, tps - 1, 2)]

        def local(i, src, dst):
            return pltpu.make_async_copy(src, dst, l_sem.at[i])

        def x_copy(i):
            return pltpu.make_async_copy(x_hbm.at[span(i * TILE, TILE)], x_buf.at[both(i)], x_sem.at[both(i)])

        vp_copy = local(0, vp_hbm, vp_buf)
        kp_copy = local(1, kp_hbm, kp_buf)
        pair_w = PAIR * hd

        def proj_w(pair):
            return pair * pair_w // WIDE, pl.ds(pair * pair_w % WIDE, pair_w)

        w_copies = []
        for pair in range(n_proj // pair_w):
            src, first = (wq_hbm, pair) if pair < ratio else ((wk_hbm, wv_hbm)[pair - ratio], 0)
            slot, lanes = proj_w(pair)
            w_copies.append(local(2 + pair, src.at[:, pl.ds(first * pair_w, pair_w)], w_buf.at[slot, :, lanes]))
        start([vp_copy, kp_copy, x_copy(0)] + w_copies + [x_copy(1)])

        greeted = [{"cp": lax.rem(me + j, groups)} for j in range(1, groups)] + [{"tp": lax.rem(t + j, tps)} for j in range(1, tps)]
        barrier = pltpu.get_barrier_semaphore()
        for who in greeted:
            pl.semaphore_signal(barrier, inc=1, device_id=who, device_id_type=MESH)

        def w_place(which):
            return lambda rank, first, size: wall_hbm.at[span(rank * w_rows + first, size), span(which * w_half, w_half)]

        w_ranks = (t, up, down, over, w_rows)
        w_sends, w_brings = gather_steps(w_place(core), (w_s, w_r), w_ranks, wo_hbm.at[:, span(core * w_half, w_half)])
        w_theirs = gather_steps(w_place(1 - core), (d_s, d_r), w_ranks)[1]

        def part_rows(who):
            return span(who * w_part, w_part, SUB)

        y_steps, x_steps, d_steps = range(tps - 1), range(tps - 1, PAIR * (tps - 1)), range(PAIR * (tps - 1), 3 * tps - 2)

        def w_last(i, arriving=False):
            if i in y_steps:
                src = wo_hbm.at[part_rows(me), pl.ds(PAIR * w_half, WIDE)]
                return remote(src, wlast_hbm.at[y_steps[-1] - i, part_rows(me)], (e_s, e_r), i, {"tp": lax.rem(t + i + 1, tps)})
            back = PAIR * (i - d_steps[0])
            if i in x_steps:
                back = PAIR * (i - y_steps[-1])
                to = {"cp": lax.rem(me + back, groups)}
                owner = lax.rem(me + groups - back, groups) if arriving else me
            else:
                to, owner = sib, lax.rem(me + groups - back, groups)
                if arriving:
                    owner = owner + 1 - PAIR * core
            ref = wlast_hbm.at[:, part_rows(owner)]
            return remote(ref, ref, (e_s, e_r), i, to)

        def w_last_round():
            for i in y_steps:
                w_last(i, True).wait_recv()
            start([w_last(i) for i in x_steps] + [w_last(d_steps[0])])

        @scoped("w_last_on")
        def w_last_on():
            for i in x_steps:
                w_last(i, True).wait_recv()
            start([w_last(i) for i in d_steps[1:]])

        @scoped("w_last_here")
        def w_last_here():
            for i in d_steps:
                w_last(i, True).wait_recv()

        def w_share(i):
            ref = w_brings[i].dst_ref
            return remote(ref, ref, (d_s, d_r), i, sib)

        def o_cols(which):
            return span(which * ratio * hd, ratio * hd)

        def swap(i, arriving=False):
            if i == KP:
                src, dst = keys.at[pl.ds(send_pre, pre)], keys.at[pl.ds(pre, pre)]
            elif i == VP:
                src, dst = vals.at[pl.ds(send_pre, pre)], vals.at[pl.ds(pre, pre)]
            elif i in (KE, VE, KL, VL):
                buf, late = keys if i in (KE, KL) else vals, i in (KL, VL)
                src, dst = buf.at[pl.ds(send + late * blk, blk)], buf.at[pl.ds(suf + late * deep + blk, blk)]
            elif i in (QE, QL):
                at = pl.ds((i - QE) * half_side, half_side)
                src, dst = q3.at[2, :, at], q3.at[1, :, at]
            else:
                src, dst = o_snd.at[i - OE], o_st.at[i - OE, :, o_cols(1 - core if arriving else core)]
            return remote(src, dst, (sw_s, sw_r), i, sib)

        def region(item, slot):
            if item in (P_OWN, P_SIB):
                return pl.ds(slot * per_chip + item * pre, pre)
            return pl.ds(suf + (PAIR * slot + item - EARLY) * deep, deep)

        def ring(item):
            plan = {K_RIGHT: (keys, 0, 1, x_right), V_RIGHT: (vals, 0, 1, x_right), K_LEFT: (keys, 0, 3, x_left), V_LEFT: (vals, 0, 3, x_left),
                    K_ON: (keys, 1, 2, x_right), V_ON: (vals, 3, 2, x_left)}
            return [remote(buf.at[region(item, a)], buf.at[region(item, b)], (x_s.at[item], x_r.at[item]), i, who) for i, (buf, a, b, who) in plan.items()]

        @scoped("ring_on")
        def pass_on(item):
            got = ring(item)
            got[K_RIGHT].wait_recv()
            got[K_ON].start()
            got[V_LEFT].wait_recv()
            got[V_ON].start()

        @scoped("wait_sides")
        def sides_here(item):
            got = ring(item)
            got[V_RIGHT].wait_recv()
            got[K_LEFT].wait_recv()

        @scoped("wait_far")
        def far_here(item):
            got = ring(item)
            got[K_ON].wait_recv()
            got[V_ON].wait_recv()

        h_bufs = (h_0, h_1)

        def norm(i, slot):
            g = g_ref[...].astype(F32)[None, :]
            for r in range(0, TILE, NORM_ROWS):
                h_bufs[slot][r : r + NORM_ROWS, :] = (rms(x_buf[slot, r : r + NORM_ROWS, :].astype(F32)) * g).astype(BF16)

        def project(i, slot):
            h_tile = h_bufs[slot]
            late, sub = lax.div(i, blk // TILE), lax.rem(i, blk // TILE)
            at_rows = span(i * TILE, TILE)
            tab = span(sub * TILE, TILE)
            first = lax.broadcasted_iota(jnp.int32, (TILE, hd), 1) < hd // PAIR

            def table(ref):
                v = ref[tab, :]
                w = pltpu.roll(v, hd // PAIR, 1)
                return jnp.where(first == (late == 0), v, w)

            cos, sin = table(cos_ref), table(sin_ref)
            sin = jnp.where(first, -sin, sin)

            def rope(v):
                return v * cos + pltpu.roll(v, hd // PAIR, 1) * sin

            for pair in range(n_proj // pair_w):
                slot, w_lanes = proj_w(pair)
                out = jnp.dot(h_tile[...], w_buf[slot, :, w_lanes], preferred_element_type=F32)
                heads_new = []
                for hh in range(PAIR):
                    v = out[:, hh * hd : (hh + 1) * hd]
                    head = PAIR * pair + hh
                    at = jnp.where(core == hh, suf + late * deep, send + late * blk) + sub * TILE
                    if head < heads:
                        q_t = rope(v).astype(BF16).astype(F32).T
                        if not exact:
                            n2 = jnp.max(jnp.sum(fold_rows(q_t * q_t, jnp.sum), axis=0, keepdims=True), axis=1, keepdims=True)
                            note(0, jnp.broadcast_to(n2, (1, LANES)))
                        q_t = q_t * scale
                        hi = q_t.astype(BF16)
                        idx = jnp.where(core == head // ratio, 0, 2)
                        col = span(late * half_side + (head % ratio) * blk + sub * TILE, TILE)
                        q3[idx, pl.ds(0, hd), col] = hi
                        q3[idx, pl.ds(hd, hd), col] = (q_t - hi.astype(F32)).astype(BF16)
                    elif head < heads + 2:
                        k = rope(v).astype(BF16)
                        keys[span(at, TILE), :] = k
                        heads_new.append(k)
                        note_rows(1, k.astype(F32))
                    else:
                        v = v.astype(BF16)
                        heads_new.append(v)
                        v_t = v.astype(F32).T
                        note_size(2, v.astype(F32))
                        for b in range(0, TILE, LANES):
                            vals[span(at + b, LANES), :] = v_t[:, b : b + LANES].astype(BF16)
                if heads_new:
                    (kp_buf, vp_buf)[pair - ratio][at_rows] = jnp.concatenate(heads_new, axis=1).reshape(TILE, 2, hd)

        kp_copy.wait()
        vp_copy.wait()
        if not exact:
            size_all[0] = jnp.zeros(size_all.shape[1:], F32)

        def note(i, v):
            if not exact:
                size_all[0, i : i + 1, :] = jnp.maximum(size_all[0, i : i + 1, :], v)

        def note_rows(i, v):
            if not exact:
                n2 = jnp.sum(v * v, axis=1, keepdims=True)
                note(i, jnp.broadcast_to(jnp.max(n2, axis=0, keepdims=True), (1, LANES)))

        def note_size(i, v):
            if not exact:
                note(i, jnp.max(fold_rows(jnp.abs(v), jnp.max), axis=0, keepdims=True))

        def split_prefix(b):
            rows_b = span(b * LANES, LANES)
            k, v = [buf[rows_b].reshape(LANES, PAIR * hd) for buf in (kp_buf, vp_buf)]
            for j in range(PAIR):
                at = span(jnp.where(core == j, 0, send_pre) + b * LANES, LANES)
                k_j, v_j = k[:, j * hd : (j + 1) * hd], v[:, j * hd : (j + 1) * hd].astype(F32)
                keys[at, :] = k_j
                vals[at, :] = v_j.T.astype(BF16)
                note_rows(1, k_j.astype(F32))
                note_size(2, v_j)

        loop(pre // LANES, split_prefix)
        with jax.named_scope("barrier"):
            pl.semaphore_wait(barrier, len(greeted))
        start([swap(KP), swap(VP)] + ring(P_OWN)[:K_ON] + [w_last(i) for i in y_steps] + w_sends[:ON_UP])
        with jax.named_scope("x_wait"):
            x_copy(0).wait()
        norm(0, 0)
        with jax.named_scope("w_wait"):
            for c in w_copies:
                c.wait()

        n_tiles = rows // TILE

        @scoped("project")
        def two_tiles(j):
            i = PAIR * j
            x_copy(i + 1).wait()

            @pl.when(i + 2 < n_tiles)
            def _():
                x_copy(i + 2).start()

            norm(i + 1, 1)
            project(i, 0)

            @pl.when(j == 0)
            def _():
                swap(KP).wait_recv()
                swap(VP).wait_recv()
                start(ring(P_SIB)[:K_ON])

            @pl.when(i + 2 < n_tiles)
            def _():
                x_copy(i + 3).start()
                x_copy(i + 2).wait()

            norm(i + 2, 0)
            project(i + 1, 1)

            @pl.when(j == 0)
            def _():
                start([swap(i) for i in (KE, VE, QE)])

        loop(n_tiles // PAIR, two_tiles)
        start([swap(i) for i in (KL, VL, QL)])
        new_copies = [local(4, kp_buf, k_out), local(5, vp_buf, v_out)]
        start(new_copies)

        def size_copies():
            out = []
            for j in range(1, groups):
                out.append(remote(size_all.at[0], size_all.at[j], (z_s, z_r), j, {"cp": lax.rem(me + j, groups)}))
            return out

        def size_on():
            return [remote(size_tp.at[0], size_tp.at[j], (y_s, y_r), j, {"tp": lax.rem(t + j, tps)}) for j in range(1, tps)]

        flag_copy = local(6, flag, plain_out)

        def sizes_known():
            for c in size_on():
                c.wait_recv()
            top = jnp.max(jnp.max(size_tp[...], axis=0), axis=1)
            fits = (scale * scale * top[0] * top[1] <= S_LIMIT**2) & (top[2] <= 2.0**V_LIMIT)
            flag[0, 0] = fits.astype(jnp.int32)
            flag_copy.start()

        def sizes_meet():
            for c in size_copies():
                c.wait_recv()
            size_tp[0] = jnp.max(size_all[...], axis=0)
            start(size_on())

        if not exact:
            start(size_copies())
        if exact:
            flag[0, 0] = 1
            flag_copy.start()
            m_ref[...] = jnp.full_like(m_ref, -jnp.inf)
        l_ref[...] = jnp.zeros_like(l_ref)
        a_ref[...] = jnp.zeros_like(a_ref)
        with jax.named_scope("swap_wait"):
            for i in range(KE, OE):
                swap(i).wait_recv()

        p_bufs = (o_buf, act_buf)

        def beside(r):
            return pl.ds(r // TILE * blk, blk)

        lead = 0 if exact else 1
        main_unroll = 1 if exact else 4

        def state_at(step):
            who, late, head = step[:3]
            return span(who * side + late * half_side + head * blk, blk)

        def product(step, r, n, shifts):
            who, late, head, key = step
            k = keys[span(key + r, n), :]
            s = jnp.dot(jnp.concatenate([k, k], axis=1), q3[who, :, span(late * half_side + head * blk, blk)], preferred_element_type=F32)
            if shifts is not None:
                row = lax.broadcasted_iota(jnp.int32, s.shape, 0) + r % blk
                col = lax.broadcasted_iota(jnp.int32, s.shape, 1) + shifts[r // blk]
                s = jnp.where(row <= col, s, -jnp.inf)
            return s

        def weights(step, slot, shifts):
            total = None
            for r in range(0, deep, TILE):
                p = jnp.exp2(product(step, r, TILE, shifts))
                p_bufs[slot][:, beside(r)] = p.astype(BF16)
                t8 = fold_rows(p, jnp.sum)
                total = t8 if total is None else total + t8
            l_ref[:, state_at(step)] += total

        def values(step, slot):
            v = jnp.concatenate([vals[span(step[3] + b, LANES), :] for b in range(0, deep, LANES)], axis=1)
            p = jnp.concatenate([p_bufs[slot][:, beside(r)] for r in range(0, deep, TILE)], axis=0)
            a_ref[:, state_at(step)] += jnp.dot(v, p, preferred_element_type=F32)

        def exact_step(step, shifts):
            cols = state_at(step)
            top = m_old = m_ref[:, cols]
            for r in range(0, deep, TILE):
                s = product(step, r, TILE, shifts)
                part[0, :, beside(r)] = s
                top = jnp.maximum(top, jnp.max(s, axis=0, keepdims=True))
            corr = jnp.exp2(m_old - top)
            m_ref[:, cols] = top
            total = l_ref[:, cols] * corr
            for r in range(0, deep, TILE):
                p = jnp.exp2(part[0, :, beside(r)] - top)
                o_buf[:, beside(r)] = p.astype(BF16)
                total += fold_rows(p, jnp.sum)
            l_ref[:, cols] = total
            a_ref[:, cols] = a_ref[:, cols] * corr
            values(step, 0)

        def run(n_steps, unroll, where, service, mask=None):
            def shifts(step):
                return None if mask is None else mask(step)

            def ahead(u, slot):
                weights(where(u), slot, shifts(where(u)))

            if not exact:
                ahead(0, 0)

            @scoped("body")
            def body(i):
                service(i)
                for j in range(unroll):
                    u = unroll * i + j
                    if exact:
                        exact_step(where(u), shifts(where(u)))
                    else:
                        ahead(u + 1, (j + 1) % 2)
                        values(where(u), j % 2)

            trips = (n_steps - lead) // unroll
            loop(trips, body)
            for u in range(unroll * trips, n_steps):
                if u + 1 < n_steps:
                    ahead(u + 1, (u + 1) % 2)
                values(where(u), u % 2)

        def own_where(u):
            who, rest = lax.div(u, PAIR * ratio), lax.rem(u, PAIR * ratio)
            late, head = lax.div(rest, ratio), lax.rem(rest, ratio)
            return who, late, head, suf + late * deep

        def own_mask(step):
            who, late = step[:2]
            q_core = jnp.where(who == 0, core, 1 - core)
            seen = jnp.where(late == 0, q_core, 1 - q_core)
            other = (PAIR * seen - 1) * blk
            return jnp.where(who == 0, 0, other), jnp.where(who == 0, other, 0)

        with jax.named_scope("run_own"):
            run(4 * ratio, 1 if exact else 2, own_where, lambda i: None, own_mask)

        qt = PAIR * ratio
        pc = per_chip // deep
        n_rem = chips - 1
        n_near = jnp.minimum(chip, 1) + lax.div(chip, n_rem)
        b1 = PAIR * qt * pc
        b2 = b1 + qt
        b4 = b2 + n_rem * qt * pc
        b5 = b4 + qt * n_near
        b6 = b5 + qt
        b7 = b6 + qt * (chip - n_near)
        b8 = b7 + n_rem * qt * pc - qt
        b9 = b8 + qt * n_rem
        n_main = b4 + n_rem * qt * pc + PAIR * qt * n_rem

        def where(u):
            def prefix(j):
                i, r = lax.div(j, qt * pc), lax.rem(j, qt * pc)
                return lax.div(r, pc), far_last(i) * per_chip + lax.rem(r, pc) * deep

            def far_last(i):
                return jnp.where(i == 0, 1, jnp.where(i == 1, n_rem, 2))

            def suffix(j, back):
                return lax.rem(j, qt), suf + back * PAIR * deep

            tile = lax.div(u, pc)
            late = lax.div(tile, qt)
            q_i, key = lax.rem(tile, qt), lax.rem(u, pc) * deep
            j9 = suffix(u - b9, far_last(jnp.minimum(chip, 1) + lax.div(u - b9, qt)))
            for first, is_late, (q_n, key_n) in (
                (b1, 1, (u - b1, suf)),
                (b2, 0, prefix(u - b2)),
                (b4, 0, suffix(u - b4, far_last(lax.div(u - b4, qt)))),
                (b5, 1, prefix(u - b5)),
                (b6, 0, suffix(u - b6, 2)),
                (b7, 1, prefix(u - b7 + qt)),
                (b8, 1, (lax.div(u - b8, n_rem), suf + (1 + lax.rem(u - b8, n_rem)) * PAIR * deep)),
                (b9, 1, (j9[0], j9[1] + deep)),
            ):
                here = u >= first
                late, q_i, key = [jnp.where(here, a, b) for a, b in ((is_late, late), (q_n, q_i), (key_n, key))]
            return lax.div(q_i, ratio), late, lax.rem(q_i, ratio), key

        @scoped("finalize")
        def finalize(h):
            for who in range(PAIR):
                for head in range(ratio):
                    at = state_at((who, h, head))
                    inv = 1.0 / jnp.sum(l_ref[:, at], axis=0, keepdims=True)
                    o = (a_ref[:, at] * inv).T.astype(BF16)
                    if who == 0:
                        o_st[h, :, span(core * ratio * hd + head * hd, hd)] = o
                    else:
                        o_snd[h, :, span(head * hd, hd)] = o
            swap(OE + h).start()

        gathers, o_keeps = [], []
        for i, (h, first, n) in enumerate(((0, 0, TILE), (0, TILE, blk - TILE), (1, 0, blk))):
            place = lambda rank, at, size, base=h * blk + first: o_hbm.at[pl.ds(base + at, size), span(rank * n_wide, n_wide)]
            src = o_st.at[h, pl.ds(first, n)]
            gathers.append(gather_steps(place, (o_s.at[i], o_r.at[i]), (t, up, down, over, n), src))
            o_keeps.append(local(i, src, place(t, 0, n)))

        def gather_on(i):
            sends, brings = gathers[i]
            for b, s in zip(brings, sends[ON_UP:]):
                b.wait_recv()
                s.start()

        def gathered(i):
            for b in gathers[i][1][ON_UP:]:
                b.wait_recv()
            o_keeps[i].wait()

        def tile_copies(kind, i, slot):
            def get(j, src, dst):
                return pltpu.make_async_copy(src, dst, t_sem.at[slot, j])

            if kind in (0, 3):
                cols, out = span(i * WIDE, WIDE), []
                for j in range(tps):
                    rank = lax.rem(t + j, tps)
                    at = span(rank * n_wide, n_wide)
                    src = wo_hbm.at[:, cols] if j == 0 else wlast_hbm.at[j - 1] if kind == 3 else wall_hbm.at[at, cols]
                    out.append(get(j, src, w_buf.at[slot, at]))
                return out
            if kind == 1:
                at = span(i * gate, gate)
                return [get(j, w.at[:, at], w_buf.at[slot, :, pl.ds(j * gate, gate)]) for j, w in enumerate((wg_hbm, wu_hbm))]
            return [get(0, wd_hbm.at[:, span(i * WIDE, WIDE)], w_buf.at[slot, pl.ds(0, ff)])]

        def after_first():
            swap(OL, True).wait_recv()
            start(gathers[2][0][:ON_UP] + o_keeps[2:])
            w_last_on()

        def fetch(g):
            i, slot = lax.rem(g, per), lax.rem(g, slots)
            last_a = n_a - 1
            pl.when(g == slots)(after_first)
            pl.when(g == last_a)(w_last_here)
            for kind, first, n in ((0, 0, last_a), (3, last_a, 1), (1, n_a, n_b), (2, n_a + n_b, n_c)):
                pl.when((g < total) & (i >= first) & (i < first + n))(lambda: start(tile_copies(kind, last_a if kind == 3 else i - first, slot)))

        def mlp_x(c):
            return pltpu.make_async_copy(x_hbm.at[span(c * TILE, TILE)], x_buf.at[both(c)], x_sem.at[both(c)])

        def start_x(c):
            mlp_x(c).start()

        def o_rows(c):
            return local(3, o_hbm.at[span(c * TILE, TILE)], o_buf)

        def cols_of(cut):
            return span(cut * d // PAIR, d // PAIR)

        def moves(c, cut):
            cols, slot = cols_of(cut), both(c)

            def go(i, src, dst):
                return remote(src, dst, (c_s.at[c, cut], c_r.at[c, cut]), i, {"tp": up if i % 2 == 0 else down})

            def mine(q, first):
                return part.at[slot, span(q * quarter + first, half, half), cols]

            def out(q, first, n):
                return out_hbm.at[span(c * TILE + q * quarter + first, n, half), cols]

            def sums(way, first):
                return got2.at[slot, way, pl.ds(first, half), cols]

            done = fin.at[c, :, cols]
            sends = {
                FAR_R: (mine(over, 0), got1.at[slot, 0, :, cols]),
                FAR_L: (mine(over, half), got1.at[slot, 1, :, cols]),
                NEAR_R: (mine(up, half), sums(0, half)),
                NEAR_L: (mine(down, 0), sums(1, 0)),
                SUM_R: (mine(up, 0), sums(0, 0)),
                SUM_L: (mine(down, half), sums(1, half)),
                OUT_R: (done, out(t, 0, quarter)),
                OUT_L: (done, out(t, 0, quarter)),
                ON_R: (out(down, 0, half), out(down, 0, half)),
                ON_L: (out(up, half, half), out(up, half, half)),
            }
            brings = {
                OUT_R: (done, out(down, 0, quarter)),
                OUT_L: (done, out(up, 0, quarter)),
                ON_R: (out(over, 0, half), out(over, 0, half)),
                ON_L: (out(over, half, half), out(over, half, half)),
            }
            own = pltpu.make_async_copy(done, out(t, 0, quarter), c_sem.at[c, cut])
            return [go(i, *m) for i, m in sends.items()], {i: go(i, *m) for i, m in brings.items()}, own

        def cuts(name):
            def deco(f):
                return scoped(name)(lambda c: loop(2, lambda cut: f(c, cut)))

            return deco

        @cuts("middle")
        def middle(c, cut):
            m = moves(c, cut)[0]
            for way, q, first in ((0, up, 0), (1, down, half)):
                m[FAR_R + way].wait_recv()
                part[both(c), span(q * quarter + first, half, half), cols_of(cut)] += got1[both(c), way, :, cols_of(cut)]
                m[SUM_R + way].start()

        @cuts("finish")
        def finish(c, cut):
            m, _, own = moves(c, cut)
            for i in (NEAR_R, NEAR_L, SUM_R, SUM_L):
                m[i].wait_recv()
            cols, slot = cols_of(cut), both(c)
            rest = got2[slot, 0, :, cols] + got2[slot, 1, :, cols]
            fin[c, :, cols] = (y_own[slot, :, cols] + (part[slot, span(t * quarter, quarter, quarter), cols] + rest)).astype(BF16)
            own.start()
            start(m[OUT_R:ON_R])

        @cuts("forward")
        def forward(c, cut):
            m, b, _ = moves(c, cut)
            for way in range(PAIR):
                b[OUT_R + way].wait_recv()
                m[ON_R + way].start()

        @cuts("drain")
        def drain(c, cut):
            m, b, own = moves(c, cut)
            b[ON_R].wait_recv()
            b[ON_L].wait_recv()
            for s in m[OUT_R:]:
                s.wait_send()
            own.wait()

        @cuts("release")
        def release(c, cut):
            for s in moves(c, cut)[0][:OUT_R]:
                s.wait_send()

        def tiles(n, base, kind, body):
            @scoped("tile_" + "abc"[kind])
            def one(i):
                g = base + i
                fetch(g + slots - 1)
                slot = lax.rem(g, slots)
                at = jnp.minimum(i, n_a - 2) if kind == 0 else i
                for cp in tile_copies(kind, at, slot):
                    cp.wait()
                body(i, slot)

            loop(n, one)

        def chunk_step(c):
            base, slot_c = c * per, both(c)
            for i in (1, 2):
                pl.when(c == i)(lambda i=i: gathered(i))
            pl.when(c >= 1)(lambda: o_rows(c).start())
            pl.when(c >= 2)(lambda: release(c - 2))
            mlp_x(c).wait()
            pl.when(c + 1 < n_chunks)(lambda: start_x(c + 1))
            o_rows(c).wait()

            def tile_a(i, slot):
                at = span(i * WIDE, WIDE)
                part[slot_c, :, at] = x_buf[slot_c, :, at].astype(F32) + jnp.dot(o_buf[...], w_buf[slot], preferred_element_type=F32)

            tiles(n_a, base, 0, tile_a)
            y_own[both(c)] = part[slot_c, span(t * quarter, quarter, quarter), :]

            def norm2(i):
                at = span(i * NORM_ROWS, NORM_ROWS, NORM_ROWS)
                h_0[at, :] = (rms(part[slot_c, at, :]) * g2_ref[...].astype(F32)[None, :]).astype(BF16)

            loop(TILE // NORM_ROWS, norm2)
            pl.when(c == 0)(lambda: gather_on(1))
            pl.when(c >= 1)(lambda: middle(c - 1))

            def tile_b(i, slot):
                pair = jnp.dot(h_0[...], w_buf[slot], preferred_element_type=F32)
                act_buf[:, span(i * gate, gate)] = (jax.nn.silu(pair[:, :gate]) * pair[:, gate:]).astype(BF16)

            tiles(n_b, base + n_a, 1, tile_b)
            pl.when(c >= 2)(lambda: forward(c - 2))

            def tile_c(i, slot):
                part[slot_c, :, span(i * WIDE, WIDE)] = jnp.dot(act_buf[...], w_buf[slot, 0:ff, :], preferred_element_type=F32)
                for cut in range(PAIR):
                    pl.when(i == (cut + 1) * n_c // PAIR - 1)(lambda cut=cut: start(moves(c, cut)[0][:SUM_R]))

            tiles(n_c, base + n_a + n_b, 2, tile_c)
            pl.when(c == 0)(lambda: gather_on(2))
            if not exact:
                pl.when(c == 1)(sizes_known)
            pl.when(c >= 1)(lambda: finish(c - 1))

        def at_trip(events):
            def service(i):
                for when, what in events:
                    pl.when(i == when)(lambda what=what: (what(), None)[1])

            return service

        def suffix_early():
            pass_on(P_OWN)
            pass_on(P_SIB)
            start(ring(EARLY)[:K_ON])

        @scoped("w_on")
        def w_on():
            for b, c in zip(w_brings, w_sends[ON_UP:]):
                b.wait_recv()
                c.start()
            start([w_share(UP), w_share(DOWN)])

        def suffix_late():
            pass_on(EARLY)
            start(ring(LATE)[:K_ON])

        @scoped("early_o")
        def early_o():
            swap(OE, True).wait_recv()
            start(gathers[0][0][:ON_UP] + o_keeps[:2])

        @scoped("w_rest")
        def w_rest():
            for i in (ON_UP, ON_DOWN):
                w_brings[i].wait_recv()
                w_share(i).start()

        @scoped("first_tiles")
        def first_tiles():
            for b in w_theirs:
                b.wait_recv()
            start_x(0)
            for g in range(slots - 1):
                fetch(g)

        def trip(step):
            return lax.div(step - lead, main_unroll)

        e_done = lax.div(b7 + main_unroll - 1, main_unroll)
        trips = (n_main - lead) // main_unroll
        events = [
            (trip(qt + 4), suffix_early),
            (trip(b2), lambda: [sides_here(P_OWN), sides_here(P_SIB)]),
            (trip(b4 - qt * pc), lambda: [far_here(P_OWN), far_here(P_SIB)]),
            (trip(b4 - qt), w_on),
            (trip(b4 - 4), suffix_late),
            (trip(b4), lambda: sides_here(EARLY)),
            (trip(jnp.where(chip < 2, b8, b6)), lambda: far_here(EARLY)),
            (e_done, lambda: finalize(0)),
            (e_done + 1, early_o),
            (trip(n_main - 40), lambda: [pass_on(LATE), w_last_round()]),
            (trip(b9), lambda: sides_here(LATE)),
            (trip(n_main - 20), w_rest),
            (trip(n_main - 8), first_tiles),
        ]
        events.append((trip(n_main - 20), lambda: [gather_on(0), start(gathers[1][0][:ON_UP])]))
        far_late = trip(jnp.where(chip < 2, b9 + qt * (2 - chip), n_main))
        events.append((far_late, lambda: far_here(LATE)))
        if not exact:
            events.append((e_done + 2, sizes_meet))
        with jax.named_scope("run_main"):
            run(n_main, main_unroll, where, at_trip(events))

        pl.when(trip(b9) >= trips)(lambda: sides_here(LATE))
        pl.when(far_late >= trips)(lambda: far_here(LATE))
        with jax.named_scope("gathered"):
            gathered(0)
        o_rows(0).start()
        finalize(1)
        loop(n_chunks, chunk_step)
        last = n_chunks - 1
        middle(last)
        forward(last - 1)
        finish(last)
        forward(last)
        with jax.named_scope("tail"):
            for c in new_copies + [flag_copy]:
                c.wait()
            loop(n_chunks, drain)
            release(last - 1)
            release(last)
            for i in range(OL + 1):
                swap(i).wait_send()
            for item in (P_OWN, P_SIB, EARLY, LATE):
                for c in ring(item):
                    c.wait_send()
            for c in w_sends + [w_share(i) for i in range(4)] + [w_last(i) for i in range(3 * tps - 2)] + sum([g[0] for g in gathers], []):
                c.wait_send()
            if not exact:
                for c in size_copies() + size_on():
                    c.wait_send()

    n_state = PAIR * side
    scratch = [
        pltpu.VMEM(shape, BF16)
        for shape in (
            (slots, d_in, WIDE), (2, TILE, d), (TILE, d), (TILE, d), (3, PAIR * hd, side), (send_pre + pre, hd), (send_pre + pre, hd), (pre, 2, hd), (pre, 2, hd)
        )
    ]
    scratch += [pltpu.VMEM((SUB, n_state), F32), pltpu.VMEM((hd, n_state), F32)]
    scratch += [pltpu.VMEM(shape, BF16) for shape in ((2, blk, n_wide), (2, blk, ratio * hd))]
    scratch += [pltpu.VMEM((groups, SUB, LANES), F32), pltpu.VMEM((tps, SUB, LANES), F32)]
    scratch += [pltpu.VMEM((TILE, d_in), BF16), pltpu.VMEM((TILE, ff), BF16)]
    scratch += [pltpu.VMEM(shape, F32) for shape in ((2, TILE, d), (2, 2, half, d), (2, 2, quarter, d), (2, quarter, d))]
    scratch += [pltpu.VMEM((n_chunks, quarter, d), BF16), pltpu.SMEM((1, 1), jnp.int32)]
    if exact:
        scratch += [pltpu.VMEM((1, n_state), F32)]
    scratch += [dma(*n) for n in ((7,), (2,), (10,), (10,), (4, 6), (4, 6), (4,), (4,), (4,), (4,), (3, 4), (3, 4))]
    scratch += [dma(groups)] * 2 + [dma(tps)] * 2 + [dma(3 * tps - 2)] * 2 + [dma(slots, tps), dma(n_chunks, 2, 10), dma(n_chunks, 2, 10), dma(n_chunks, 2)]
    shapes = [(rows, 2, hd)] * 2 + [(rows, d), (rows, d_in), (d_in, PAIR * w_half), (tps - 1, w_rows, WIDE)]
    return pl.pallas_call(
        kernel,
        in_specs=[HBM] * 3 + [VMEM] * 3 + [HBM] * 4 + [VMEM] + [HBM] * 3,
        out_specs=[HBM] * 7,
        out_shape=[jax.ShapeDtypeStruct(s, BF16) for s in shapes] + [jax.ShapeDtypeStruct((1, 1), jnp.int32)],
        scratch_shapes=scratch,
        compiler_params=pltpu.CompilerParams(collective_id=2 + exact, has_side_effects=True, vmem_limit_bytes=VMEM_LIMIT),
        name="layer_exact" if exact else "layer",
    )(x_loc, kp2, vp2, cos_tab, sin_tab, norm_attn, w_query, w_key, w_value, w_out, norm_mlp, w_gate, w_up, w_down)


def emit_call(x_out, k_new, v_new):
    step = x_out.shape[0] // SUB

    def kernel(x_hbm, k_hbm, v_hbm, x_to, k_to, v_to, x_buf, k_buf, v_buf, r_sem, w_sem):
        moves = [[ref.at[pl.ds(i * step, step)] for ref in (x_hbm, x_buf, x_to)] for i in range(SUB)]
        moves += [(k_hbm, k_buf, k_to), (v_hbm, v_buf, v_to)]
        reads = [pltpu.make_async_copy(src, buf, r_sem.at[i]) for i, (src, buf, _) in enumerate(moves)]
        writes = [pltpu.make_async_copy(buf, dst, w_sem.at[i]) for i, (_, buf, dst) in enumerate(moves)]
        start(reads)
        for r, w in zip(reads, writes):
            r.wait()
            w.start()
        for w in writes:
            w.wait()

    arrays = (x_out, k_new, v_new)
    return pl.pallas_call(
        kernel,
        in_specs=[HBM] * len(arrays),
        out_specs=[HBM] * len(arrays),
        out_shape=[jax.ShapeDtypeStruct(a.shape, a.dtype) for a in arrays],
        scratch_shapes=[pltpu.VMEM(a.shape, a.dtype) for a in arrays] + [dma(SUB + len(arrays))] * 2,
        name="emit",
    )(*arrays)


def angle_tables(owner, groups, blk, prefix_len, hd):
    lane = jnp.arange(hd, dtype=jnp.int32)
    early = lane < hd // PAIR
    block = jnp.where(early, owner, PAIR * groups - 1 - owner)
    pos = prefix_len + block[None, :] * blk + jnp.arange(blk, dtype=jnp.int32)[:, None]
    inv_freq = ROPE_THETA ** (-jnp.arange(0, hd, 2, dtype=F32) / hd)
    angles = pos.astype(F32) * jnp.concatenate([inv_freq, inv_freq])[None, :]
    return jnp.cos(angles), jnp.sin(angles)


def solution(mesh):
    groups = mesh.shape["cp"]
    tps = mesh.shape["tp"]

    def local_layer(x_loc, kp_loc, vp_loc, norm_attn, w_query, w_key, w_value, w_out, norm_mlp, w_gate, w_up, w_down):
        rows = x_loc.shape[0]
        pre_dev, kv_loc, hd = kp_loc.shape
        tables = angle_tables(lax.axis_index("cp"), groups, rows // PAIR, pre_dev * groups, hd)

        def layer(exact):
            return layer_call(
                exact, x_loc, kp_loc, vp_loc, *tables, norm_attn, w_query, w_key, w_value, w_out, norm_mlp, w_gate, w_up, w_down, groups, tps
            )

        k_new, v_new, x_out, _, _, _, plain = layer(False)
        x_out = lax.cond(plain[0, 0] == 1, lambda: x_out, lambda: layer(True)[2])
        return tuple(emit_call(x_out, k_new, v_new))

    row_spec = P(("dp", "cp"), None)
    kv_spec = P(("dp", "cp"), "tp", None)
    col_spec = P(None, "tp")
    row_split = P("tp", None)
    vec_spec = P(None)
    return jax.shard_map(
        local_layer,
        mesh=mesh,
        in_specs=(row_spec, kv_spec, kv_spec, vec_spec, col_spec, col_spec, col_spec, row_split, vec_spec, col_spec, col_spec, row_split),
        out_specs=(row_spec, kv_spec, kv_spec),
        check_vma=False,
    )
```

```python
import jax
import jax.numpy as jnp
import numpy as np
from jax import lax
from jax.experimental import pallas as pl
from jax.experimental.pallas import tpu as pltpu
from jax.sharding import PartitionSpec as P

ROPE_THETA = 500000.0
NORM_EPS = 1e-5
LOG2E = 1.4426950408889634
F32 = jnp.float32
BF16 = jnp.bfloat16
MESH = pl.DeviceIdType.MESH
LANES = 128
PAIR = 2
SUB = 8
TILE = 256
NORM_ROWS = 32
WIDE = 512
VMEM_LIMIT = 67043328
S_LIMIT, V_LIMIT = 60.0, 40.0
HBM = pl.BlockSpec(memory_space=pl.ANY)
VMEM = pl.BlockSpec(memory_space=pltpu.VMEM)
(KP, VP, KE, VE, KL, VL, QE, QL, OE, OL) = range(10)
(K_RIGHT, V_RIGHT, K_LEFT, V_LEFT, K_ON, V_ON) = range(6)
(P_OWN, P_SIB, EARLY, LATE) = range(4)
(UP, DOWN, ON_UP, ON_DOWN) = range(4)
(FAR_R, FAR_L, NEAR_R, NEAR_L, SUM_R, SUM_L, OUT_R, OUT_L, ON_R, ON_L) = range(10)


def scoped(name):
    def deco(f):
        def g(*a):
            with jax.named_scope(name):
                return f(*a)

        return g

    return deco


def dma(*shape):
    return pltpu.SemaphoreType.DMA(shape)


def start(copies):
    for c in copies:
        c.start()


def span(at, size, unit=LANES):
    return pl.ds(pl.multiple_of(at, unit), size)


def both(v):
    return lax.rem(v, 2)


def fold_rows(values, op):
    rows, cols = values.shape
    return op(values.reshape(rows // SUB, SUB, cols), axis=0)


def rms(x):
    return x * lax.rsqrt(jnp.mean(x * x, axis=-1, keepdims=True) + NORM_EPS)


def loop(n, body):
    lax.fori_loop(0, n, lambda i, c: (body(i), c)[1], 0)


def remote(src, dst, sems, i, who):
    send, recv = sems
    return pltpu.make_async_remote_copy(src_ref=src, dst_ref=dst, send_sem=send.at[i], recv_sem=recv.at[i], device_id=who, device_id_type=MESH)


def gather_steps(at, sems, ranks, src=None):
    here, up, down, over, size = ranks
    half = size // PAIR
    to_up, to_down = {"tp": up}, {"tp": down}

    def move(i, rank, first, n, who, other=None):
        ref = at(rank, first, n)
        return remote(ref if other is None else other, ref, sems, i, who)

    sends = [
        move(UP, here, 0, size, to_up, src),
        move(DOWN, here, 0, size, to_down, src),
        move(ON_UP, down, 0, half, to_up),
        move(ON_DOWN, up, half, half, to_down),
    ]
    brings = [
        move(UP, down, 0, size, to_up),
        move(DOWN, up, 0, size, to_down),
        move(ON_UP, over, 0, half, to_up),
        move(ON_DOWN, over, half, half, to_down),
    ]
    return sends, brings


def layer_call(exact, x_loc, kp2, vp2, freq, norm_attn, w_query, w_key, w_value, w_out, norm_mlp, w_gate, w_up, w_down, groups, tps):
    rows, d = x_loc.shape
    blk = rows // PAIR
    hd = kp2.shape[2]
    heads = w_query.shape[1] // hd
    ratio = heads // PAIR
    pre = kp2.shape[0]
    chips = groups // PAIR
    assert chips == tps == 4 and pre == rows and hd == LANES and ratio == 3
    deep = PAIR * blk
    n_wide = heads * hd
    side = ratio * PAIR * blk
    half_side = side // PAIR
    per_chip = PAIR * pre
    suf = chips * per_chip
    send = suf + chips * PAIR * rows
    send_pre = send + rows
    d_out = w_out.shape[1]
    w_half = (d_out - WIDE) // PAIR
    w_rows = w_out.shape[0]
    w_part = w_rows // groups
    scale = LOG2E * hd**-0.5
    n_proj = n_wide + 4 * hd
    d_in = tps * n_wide
    ff = w_gate.shape[1]
    n_chunks = rows // TILE
    quarter = TILE // tps
    half = quarter // PAIR
    gate = WIDE // PAIR
    n_a, n_b, n_c = d // WIDE, ff // gate, d // WIDE
    per = n_a + n_b + n_c
    total = per * n_chunks
    slots = 4

    def kernel(x_hbm, kp_hbm, vp_hbm, freq_ref, g_ref, wq_hbm, wk_hbm, wv_hbm, wo_hbm, g2_ref, wg_hbm, wu_hbm, wd_hbm,
               k_out, v_out, out_hbm, o_hbm, wall_hbm, wlast_hbm, plain_out,
               w_buf, x_buf, h_0, h_1, q3, keys, vals, kp_buf, vp_buf, l_ref, a_ref, o_st, o_snd, size_all, size_tp,
               o_buf, act_buf, part, got1, got2, y_own, fin, flag, cos_ref, sin_ref, *rest):
        if exact:
            m_ref, *rest = rest
        l_sem, x_sem, sw_s, sw_r, x_s, x_r, w_s, w_r, d_s, d_r, o_s, o_r, z_s, z_r, y_s, y_r, e_s, e_r, t_sem, c_s, c_r, c_sem = rest
        me, t = lax.axis_index("cp"), lax.axis_index("tp")
        core, chip = both(me), lax.div(me, 2)
        sib = {"cp": me + 1 - PAIR * core}
        x_right, x_left = {"cp": lax.rem(me + 2, groups)}, {"cp": lax.rem(me + groups - 2, groups)}
        up, down, over = [lax.rem(t + j, tps) for j in (1, tps - 1, 2)]

        def local(i, src, dst):
            return pltpu.make_async_copy(src, dst, l_sem.at[i])

        def x_copy(i):
            return pltpu.make_async_copy(x_hbm.at[span(i * TILE, TILE)], x_buf.at[both(i)], x_sem.at[both(i)])

        vp_copy = local(0, vp_hbm, vp_buf)
        kp_copy = local(1, kp_hbm, kp_buf)
        pair_w = PAIR * hd

        def proj_w(pair):
            return pair * pair_w // WIDE, pl.ds(pair * pair_w % WIDE, pair_w)

        w_copies = []
        for pair in range(n_proj // pair_w):
            src, first = (wq_hbm, pair) if pair < ratio else ((wk_hbm, wv_hbm)[pair - ratio], 0)
            slot, lanes = proj_w(pair)
            w_copies.append(local(2 + pair, src.at[:, pl.ds(first * pair_w, pair_w)], w_buf.at[slot, :, lanes]))
        start([vp_copy, kp_copy, x_copy(0)] + w_copies + [x_copy(1)])

        greeted = [{"cp": lax.rem(me + j, groups)} for j in range(1, groups)] + [{"tp": lax.rem(t + j, tps)} for j in range(1, tps)]
        barrier = pltpu.get_barrier_semaphore()
        for who in greeted:
            pl.semaphore_signal(barrier, inc=1, device_id=who, device_id_type=MESH)

        def w_place(which):
            return lambda rank, first, size: wall_hbm.at[span(rank * w_rows + first, size), span(which * w_half, w_half)]

        w_ranks = (t, up, down, over, w_rows)
        w_sends, w_brings = gather_steps(w_place(core), (w_s, w_r), w_ranks, wo_hbm.at[:, span(core * w_half, w_half)])
        w_theirs = gather_steps(w_place(1 - core), (d_s, d_r), w_ranks)[1]

        def part_rows(who):
            return span(who * w_part, w_part, SUB)

        y_steps, x_steps, d_steps = range(tps - 1), range(tps - 1, PAIR * (tps - 1)), range(PAIR * (tps - 1), 3 * tps - 2)

        def w_last(i, arriving=False):
            if i in y_steps:
                src = wo_hbm.at[part_rows(me), pl.ds(PAIR * w_half, WIDE)]
                return remote(src, wlast_hbm.at[y_steps[-1] - i, part_rows(me)], (e_s, e_r), i, {"tp": lax.rem(t + i + 1, tps)})
            back = PAIR * (i - d_steps[0])
            if i in x_steps:
                back = PAIR * (i - y_steps[-1])
                to = {"cp": lax.rem(me + back, groups)}
                owner = lax.rem(me + groups - back, groups) if arriving else me
            else:
                to, owner = sib, lax.rem(me + groups - back, groups)
                if arriving:
                    owner = owner + 1 - PAIR * core
            ref = wlast_hbm.at[:, part_rows(owner)]
            return remote(ref, ref, (e_s, e_r), i, to)

        def w_last_round():
            for i in y_steps:
                w_last(i, True).wait_recv()
            start([w_last(i) for i in x_steps] + [w_last(d_steps[0])])

        @scoped("w_last_on")
        def w_last_on():
            for i in x_steps:
                w_last(i, True).wait_recv()
            start([w_last(i) for i in d_steps[1:]])

        @scoped("w_last_here")
        def w_last_here():
            for i in d_steps:
                w_last(i, True).wait_recv()

        def w_share(i):
            ref = w_brings[i].dst_ref
            return remote(ref, ref, (d_s, d_r), i, sib)

        def o_cols(which):
            return span(which * ratio * hd, ratio * hd)

        def swap(i, arriving=False):
            if i == KP:
                src, dst = keys.at[pl.ds(send_pre, pre)], keys.at[pl.ds(pre, pre)]
            elif i == VP:
                src, dst = vals.at[pl.ds(send_pre, pre)], vals.at[pl.ds(pre, pre)]
            elif i in (KE, VE, KL, VL):
                buf, late = keys if i in (KE, KL) else vals, i in (KL, VL)
                src, dst = buf.at[pl.ds(send + late * blk, blk)], buf.at[pl.ds(suf + late * deep + blk, blk)]
            elif i in (QE, QL):
                at = pl.ds((i - QE) * half_side, half_side)
                src, dst = q3.at[2, :, at], q3.at[1, :, at]
            else:
                src, dst = o_snd.at[i - OE], o_st.at[i - OE, :, o_cols(1 - core if arriving else core)]
            return remote(src, dst, (sw_s, sw_r), i, sib)

        def region(item, slot):
            if item in (P_OWN, P_SIB):
                return pl.ds(slot * per_chip + item * pre, pre)
            return pl.ds(suf + (PAIR * slot + item - EARLY) * deep, deep)

        def ring(item):
            plan = {K_RIGHT: (keys, 0, 1, x_right), V_RIGHT: (vals, 0, 1, x_right), K_LEFT: (keys, 0, 3, x_left), V_LEFT: (vals, 0, 3, x_left),
                    K_ON: (keys, 1, 2, x_right), V_ON: (vals, 3, 2, x_left)}
            return [remote(buf.at[region(item, a)], buf.at[region(item, b)], (x_s.at[item], x_r.at[item]), i, who) for i, (buf, a, b, who) in plan.items()]

        @scoped("ring_on")
        def pass_on(item):
            got = ring(item)
            got[K_RIGHT].wait_recv()
            got[K_ON].start()
            got[V_LEFT].wait_recv()
            got[V_ON].start()

        @scoped("wait_sides")
        def sides_here(item):
            got = ring(item)
            got[V_RIGHT].wait_recv()
            got[K_LEFT].wait_recv()

        @scoped("wait_far")
        def far_here(item):
            got = ring(item)
            got[K_ON].wait_recv()
            got[V_ON].wait_recv()

        h_bufs = (h_0, h_1)

        def norm(i, slot):
            g = g_ref[...].astype(F32)[None, :]
            for r in range(0, TILE, NORM_ROWS):
                h_bufs[slot][r : r + NORM_ROWS, :] = (rms(x_buf[slot, r : r + NORM_ROWS, :].astype(F32)) * g).astype(BF16)

        def project(i, slot):
            h_tile = h_bufs[slot]
            late, sub = lax.div(i, blk // TILE), lax.rem(i, blk // TILE)
            at_rows = span(i * TILE, TILE)
            tab = span(sub * TILE, TILE)
            first = lax.broadcasted_iota(jnp.int32, (TILE, hd), 1) < hd // PAIR

            def table(ref):
                v = ref[tab, :]
                w = pltpu.roll(v, hd // PAIR, 1)
                return jnp.where(first == (late == 0), v, w)

            cos, sin = table(cos_ref), table(sin_ref)
            sin = jnp.where(first, -sin, sin)

            def rope(v):
                return v * cos + pltpu.roll(v, hd // PAIR, 1) * sin

            for pair in range(n_proj // pair_w):
                slot, w_lanes = proj_w(pair)
                out = jnp.dot(h_tile[...], w_buf[slot, :, w_lanes], preferred_element_type=F32)
                heads_new = []
                for hh in range(PAIR):
                    v = out[:, hh * hd : (hh + 1) * hd]
                    head = PAIR * pair + hh
                    at = jnp.where(core == hh, suf + late * deep, send + late * blk) + sub * TILE
                    if head < heads:
                        q_t = rope(v).astype(BF16).astype(F32).T
                        if not exact:
                            n2 = jnp.max(jnp.sum(fold_rows(q_t * q_t, jnp.sum), axis=0, keepdims=True), axis=1, keepdims=True)
                            note(0, jnp.broadcast_to(n2, (1, LANES)))
                        q_t = q_t * scale
                        hi = q_t.astype(BF16)
                        idx = jnp.where(core == head // ratio, 0, 2)
                        col = span(late * half_side + (head % ratio) * blk + sub * TILE, TILE)
                        q3[idx, pl.ds(0, hd), col] = hi
                        q3[idx, pl.ds(hd, hd), col] = (q_t - hi.astype(F32)).astype(BF16)
                    elif head < heads + 2:
                        k = rope(v).astype(BF16)
                        keys[span(at, TILE), :] = k
                        heads_new.append(k)
                        note_rows(1, k.astype(F32))
                    else:
                        v = v.astype(BF16)
                        heads_new.append(v)
                        v_t = v.astype(F32).T
                        note_size(2, v.astype(F32))
                        for b in range(0, TILE, LANES):
                            vals[span(at + b, LANES), :] = v_t[:, b : b + LANES].astype(BF16)
                if heads_new:
                    (kp_buf, vp_buf)[pair - ratio][at_rows] = jnp.concatenate(heads_new, axis=1).reshape(TILE, 2, hd)

        def angles(i):
            shape, at = (NORM_ROWS, hd), span(i * NORM_ROWS, NORM_ROWS, NORM_ROWS)
            early = lax.broadcasted_iota(jnp.int32, shape, 1) < hd // PAIR
            row = lax.broadcasted_iota(jnp.int32, shape, 0) + i * NORM_ROWS
            block = jnp.where(early, me, PAIR * groups - 1 - me)
            angle = (pre * groups + block * blk + row).astype(F32) * freq_ref[...]
            cos_ref[at, :] = jnp.cos(angle)
            sin_ref[at, :] = jnp.sin(angle)

        with jax.named_scope("angles"):
            loop(blk // NORM_ROWS, angles)
        kp_copy.wait()
        vp_copy.wait()
        if not exact:
            size_all[0] = jnp.zeros(size_all.shape[1:], F32)

        def note(i, v):
            if not exact:
                size_all[0, i : i + 1, :] = jnp.maximum(size_all[0, i : i + 1, :], v)

        def note_rows(i, v):
            if not exact:
                n2 = jnp.sum(v * v, axis=1, keepdims=True)
                note(i, jnp.broadcast_to(jnp.max(n2, axis=0, keepdims=True), (1, LANES)))

        def note_size(i, v):
            if not exact:
                note(i, jnp.max(fold_rows(jnp.abs(v), jnp.max), axis=0, keepdims=True))

        def split_prefix(b):
            rows_b = span(b * LANES, LANES)
            k, v = [buf[rows_b].reshape(LANES, PAIR * hd) for buf in (kp_buf, vp_buf)]
            for j in range(PAIR):
                at = span(jnp.where(core == j, 0, send_pre) + b * LANES, LANES)
                k_j, v_j = k[:, j * hd : (j + 1) * hd], v[:, j * hd : (j + 1) * hd].astype(F32)
                keys[at, :] = k_j
                vals[at, :] = v_j.T.astype(BF16)
                note_rows(1, k_j.astype(F32))
                note_size(2, v_j)

        loop(pre // LANES, split_prefix)
        with jax.named_scope("barrier"):
            pl.semaphore_wait(barrier, len(greeted))
        start([swap(KP), swap(VP)] + ring(P_OWN)[:K_ON] + [w_last(i) for i in y_steps] + w_sends[:ON_UP])
        with jax.named_scope("x_wait"):
            x_copy(0).wait()
        norm(0, 0)
        with jax.named_scope("w_wait"):
            for c in w_copies:
                c.wait()

        n_tiles = rows // TILE

        @scoped("project")
        def two_tiles(j):
            i = PAIR * j
            x_copy(i + 1).wait()

            @pl.when(i + 2 < n_tiles)
            def _():
                x_copy(i + 2).start()

            norm(i + 1, 1)
            project(i, 0)

            @pl.when(j == 0)
            def _():
                swap(KP).wait_recv()
                swap(VP).wait_recv()
                start(ring(P_SIB)[:K_ON])

            @pl.when(i + 2 < n_tiles)
            def _():
                x_copy(i + 3).start()
                x_copy(i + 2).wait()

            norm(i + 2, 0)
            project(i + 1, 1)

            @pl.when(j == 0)
            def _():
                start([swap(i) for i in (KE, VE, QE)])

        loop(n_tiles // PAIR, two_tiles)
        start([swap(i) for i in (KL, VL, QL)])
        new_copies = [local(4, kp_buf, k_out), local(5, vp_buf, v_out)]
        start(new_copies)

        def size_copies():
            out = []
            for j in range(1, groups):
                out.append(remote(size_all.at[0], size_all.at[j], (z_s, z_r), j, {"cp": lax.rem(me + j, groups)}))
            return out

        def size_on():
            return [remote(size_tp.at[0], size_tp.at[j], (y_s, y_r), j, {"tp": lax.rem(t + j, tps)}) for j in range(1, tps)]

        flag_copy = local(6, flag, plain_out)

        def sizes_known():
            for c in size_on():
                c.wait_recv()
            top = jnp.max(jnp.max(size_tp[...], axis=0), axis=1)
            fits = (scale * scale * top[0] * top[1] <= S_LIMIT**2) & (top[2] <= 2.0**V_LIMIT)
            flag[0, 0] = fits.astype(jnp.int32)
            flag_copy.start()

        def sizes_meet():
            for c in size_copies():
                c.wait_recv()
            size_tp[0] = jnp.max(size_all[...], axis=0)
            start(size_on())

        if not exact:
            start(size_copies())
        if exact:
            flag[0, 0] = 1
            flag_copy.start()
            m_ref[...] = jnp.full_like(m_ref, -jnp.inf)
        l_ref[...] = jnp.zeros_like(l_ref)
        a_ref[...] = jnp.zeros_like(a_ref)
        with jax.named_scope("swap_wait"):
            for i in range(KE, OE):
                swap(i).wait_recv()

        p_bufs = (o_buf, act_buf)

        def beside(r):
            return pl.ds(r // TILE * blk, blk)

        lead = 0 if exact else 1
        main_unroll = 1 if exact else 4

        def state_at(step):
            who, late, head = step[:3]
            return span(who * side + late * half_side + head * blk, blk)

        def product(step, r, n, shifts):
            who, late, head, key = step
            k = keys[span(key + r, n), :]
            s = jnp.dot(jnp.concatenate([k, k], axis=1), q3[who, :, span(late * half_side + head * blk, blk)], preferred_element_type=F32)
            if shifts is not None:
                row = lax.broadcasted_iota(jnp.int32, s.shape, 0) + r % blk
                col = lax.broadcasted_iota(jnp.int32, s.shape, 1) + shifts[r // blk]
                s = jnp.where(row <= col, s, -jnp.inf)
            return s

        def weights(step, slot, shifts):
            total = None
            for r in range(0, deep, TILE):
                p = jnp.exp2(product(step, r, TILE, shifts))
                p_bufs[slot][:, beside(r)] = p.astype(BF16)
                t8 = fold_rows(p, jnp.sum)
                total = t8 if total is None else total + t8
            l_ref[:, state_at(step)] += total

        def values(step, slot):
            v = jnp.concatenate([vals[span(step[3] + b, LANES), :] for b in range(0, deep, LANES)], axis=1)
            p = jnp.concatenate([p_bufs[slot][:, beside(r)] for r in range(0, deep, TILE)], axis=0)
            a_ref[:, state_at(step)] += jnp.dot(v, p, preferred_element_type=F32)

        def exact_step(step, shifts):
            cols = state_at(step)
            top = m_old = m_ref[:, cols]
            for r in range(0, deep, TILE):
                s = product(step, r, TILE, shifts)
                part[0, :, beside(r)] = s
                top = jnp.maximum(top, jnp.max(s, axis=0, keepdims=True))
            corr = jnp.exp2(m_old - top)
            m_ref[:, cols] = top
            total = l_ref[:, cols] * corr
            for r in range(0, deep, TILE):
                p = jnp.exp2(part[0, :, beside(r)] - top)
                o_buf[:, beside(r)] = p.astype(BF16)
                total += fold_rows(p, jnp.sum)
            l_ref[:, cols] = total
            a_ref[:, cols] = a_ref[:, cols] * corr
            values(step, 0)

        def run(n_steps, unroll, where, service, mask=None):
            def shifts(step):
                return None if mask is None else mask(step)

            def ahead(u, slot):
                weights(where(u), slot, shifts(where(u)))

            if not exact:
                ahead(0, 0)

            @scoped("body")
            def body(i):
                service(i)
                for j in range(unroll):
                    u = unroll * i + j
                    if exact:
                        exact_step(where(u), shifts(where(u)))
                    else:
                        ahead(u + 1, (j + 1) % 2)
                        values(where(u), j % 2)

            trips = (n_steps - lead) // unroll
            loop(trips, body)
            for u in range(unroll * trips, n_steps):
                if u + 1 < n_steps:
                    ahead(u + 1, (u + 1) % 2)
                values(where(u), u % 2)

        def own_where(u):
            who, rest = lax.div(u, PAIR * ratio), lax.rem(u, PAIR * ratio)
            late, head = lax.div(rest, ratio), lax.rem(rest, ratio)
            return who, late, head, suf + late * deep

        def own_mask(step):
            who, late = step[:2]
            q_core = jnp.where(who == 0, core, 1 - core)
            seen = jnp.where(late == 0, q_core, 1 - q_core)
            other = (PAIR * seen - 1) * blk
            return jnp.where(who == 0, 0, other), jnp.where(who == 0, other, 0)

        with jax.named_scope("run_own"):
            run(4 * ratio, 1 if exact else 2, own_where, lambda i: None, own_mask)

        qt = PAIR * ratio
        pc = per_chip // deep
        n_rem = chips - 1
        n_near = jnp.minimum(chip, 1) + lax.div(chip, n_rem)
        b1 = PAIR * qt * pc
        b2 = b1 + qt
        b4 = b2 + n_rem * qt * pc
        b5 = b4 + qt * n_near
        b6 = b5 + qt
        b7 = b6 + qt * (chip - n_near)
        b8 = b7 + n_rem * qt * pc - qt
        b9 = b8 + qt * n_rem
        n_main = b4 + n_rem * qt * pc + PAIR * qt * n_rem

        def where(u):
            def prefix(j):
                i, r = lax.div(j, qt * pc), lax.rem(j, qt * pc)
                return lax.div(r, pc), far_last(i) * per_chip + lax.rem(r, pc) * deep

            def far_last(i):
                return jnp.where(i == 0, 1, jnp.where(i == 1, n_rem, 2))

            def suffix(j, back):
                return lax.rem(j, qt), suf + back * PAIR * deep

            tile = lax.div(u, pc)
            late = lax.div(tile, qt)
            q_i, key = lax.rem(tile, qt), lax.rem(u, pc) * deep
            j9 = suffix(u - b9, far_last(jnp.minimum(chip, 1) + lax.div(u - b9, qt)))
            for first, is_late, (q_n, key_n) in (
                (b1, 1, (u - b1, suf)),
                (b2, 0, prefix(u - b2)),
                (b4, 0, suffix(u - b4, far_last(lax.div(u - b4, qt)))),
                (b5, 1, prefix(u - b5)),
                (b6, 0, suffix(u - b6, 2)),
                (b7, 1, prefix(u - b7 + qt)),
                (b8, 1, (lax.div(u - b8, n_rem), suf + (1 + lax.rem(u - b8, n_rem)) * PAIR * deep)),
                (b9, 1, (j9[0], j9[1] + deep)),
            ):
                here = u >= first
                late, q_i, key = [jnp.where(here, a, b) for a, b in ((is_late, late), (q_n, q_i), (key_n, key))]
            return lax.div(q_i, ratio), late, lax.rem(q_i, ratio), key

        @scoped("finalize")
        def finalize(h):
            for who in range(PAIR):
                for head in range(ratio):
                    at = state_at((who, h, head))
                    inv = 1.0 / jnp.sum(l_ref[:, at], axis=0, keepdims=True)
                    o = (a_ref[:, at] * inv).T.astype(BF16)
                    if who == 0:
                        o_st[h, :, span(core * ratio * hd + head * hd, hd)] = o
                    else:
                        o_snd[h, :, span(head * hd, hd)] = o
            swap(OE + h).start()

        gathers, o_keeps = [], []
        for i, (h, first, n) in enumerate(((0, 0, TILE), (0, TILE, blk - TILE), (1, 0, blk))):
            place = lambda rank, at, size, base=h * blk + first: o_hbm.at[pl.ds(base + at, size), span(rank * n_wide, n_wide)]
            src = o_st.at[h, pl.ds(first, n)]
            gathers.append(gather_steps(place, (o_s.at[i], o_r.at[i]), (t, up, down, over, n), src))
            o_keeps.append(local(i, src, place(t, 0, n)))

        def gather_on(i):
            sends, brings = gathers[i]
            for b, s in zip(brings, sends[ON_UP:]):
                b.wait_recv()
                s.start()

        def gathered(i):
            for b in gathers[i][1][ON_UP:]:
                b.wait_recv()
            o_keeps[i].wait()

        def tile_copies(kind, i, slot):
            def get(j, src, dst):
                return pltpu.make_async_copy(src, dst, t_sem.at[slot, j])

            if kind in (0, 3):
                cols, out = span(i * WIDE, WIDE), []
                for j in range(tps):
                    rank = lax.rem(t + j, tps)
                    at = span(rank * n_wide, n_wide)
                    src = wo_hbm.at[:, cols] if j == 0 else wlast_hbm.at[j - 1] if kind == 3 else wall_hbm.at[at, cols]
                    out.append(get(j, src, w_buf.at[slot, at]))
                return out
            if kind == 1:
                at = span(i * gate, gate)
                return [get(j, w.at[:, at], w_buf.at[slot, :, pl.ds(j * gate, gate)]) for j, w in enumerate((wg_hbm, wu_hbm))]
            return [get(0, wd_hbm.at[:, span(i * WIDE, WIDE)], w_buf.at[slot, pl.ds(0, ff)])]

        def fetch(g):
            i, slot = lax.rem(g, per), lax.rem(g, slots)
            last_a = n_a - 1
            pl.when(g == slots)(w_last_on)
            pl.when(g == last_a)(w_last_here)
            for kind, first, n in ((0, 0, last_a), (3, last_a, 1), (1, n_a, n_b), (2, n_a + n_b, n_c)):
                pl.when((g < total) & (i >= first) & (i < first + n))(lambda: start(tile_copies(kind, last_a if kind == 3 else i - first, slot)))

        def mlp_x(c):
            return pltpu.make_async_copy(x_hbm.at[span(c * TILE, TILE)], x_buf.at[both(c)], x_sem.at[both(c)])

        def start_x(c):
            mlp_x(c).start()

        def o_rows(c):
            return local(3, o_hbm.at[span(c * TILE, TILE)], o_buf)

        def cols_of(cut):
            return span(cut * d // PAIR, d // PAIR)

        def moves(c, cut):
            cols, slot = cols_of(cut), both(c)

            def go(i, src, dst):
                return remote(src, dst, (c_s.at[c, cut], c_r.at[c, cut]), i, {"tp": up if i % 2 == 0 else down})

            def mine(q, first):
                return part.at[slot, span(q * quarter + first, half, half), cols]

            def out(q, first, n):
                return out_hbm.at[span(c * TILE + q * quarter + first, n, half), cols]

            def sums(way, first):
                return got2.at[slot, way, pl.ds(first, half), cols]

            done = fin.at[c, :, cols]
            sends = {
                FAR_R: (mine(over, 0), got1.at[slot, 0, :, cols]),
                FAR_L: (mine(over, half), got1.at[slot, 1, :, cols]),
                NEAR_R: (mine(up, half), sums(0, half)),
                NEAR_L: (mine(down, 0), sums(1, 0)),
                SUM_R: (mine(up, 0), sums(0, 0)),
                SUM_L: (mine(down, half), sums(1, half)),
                OUT_R: (done, out(t, 0, quarter)),
                OUT_L: (done, out(t, 0, quarter)),
                ON_R: (out(down, 0, half), out(down, 0, half)),
                ON_L: (out(up, half, half), out(up, half, half)),
            }
            brings = {
                OUT_R: (done, out(down, 0, quarter)),
                OUT_L: (done, out(up, 0, quarter)),
                ON_R: (out(over, 0, half), out(over, 0, half)),
                ON_L: (out(over, half, half), out(over, half, half)),
            }
            own = pltpu.make_async_copy(done, out(t, 0, quarter), c_sem.at[c, cut])
            return [go(i, *m) for i, m in sends.items()], {i: go(i, *m) for i, m in brings.items()}, own

        def cuts(name):
            def deco(f):
                return scoped(name)(lambda c: loop(2, lambda cut: f(c, cut)))

            return deco

        @cuts("middle")
        def middle(c, cut):
            m = moves(c, cut)[0]
            for way, q, first in ((0, up, 0), (1, down, half)):
                m[FAR_R + way].wait_recv()
                part[both(c), span(q * quarter + first, half, half), cols_of(cut)] += got1[both(c), way, :, cols_of(cut)]
                m[SUM_R + way].start()

        @cuts("finish")
        def finish(c, cut):
            m, _, own = moves(c, cut)
            for i in (NEAR_R, NEAR_L, SUM_R, SUM_L):
                m[i].wait_recv()
            cols, slot = cols_of(cut), both(c)
            rest = got2[slot, 0, :, cols] + got2[slot, 1, :, cols]
            fin[c, :, cols] = (y_own[slot, :, cols] + (part[slot, span(t * quarter, quarter, quarter), cols] + rest)).astype(BF16)
            own.start()
            start(m[OUT_R:ON_R])

        @cuts("forward")
        def forward(c, cut):
            m, b, _ = moves(c, cut)
            for way in range(PAIR):
                b[OUT_R + way].wait_recv()
                m[ON_R + way].start()

        @cuts("drain")
        def drain(c, cut):
            m, b, own = moves(c, cut)
            b[ON_R].wait_recv()
            b[ON_L].wait_recv()
            for s in m[OUT_R:]:
                s.wait_send()
            own.wait()

        @cuts("release")
        def release(c, cut):
            for s in moves(c, cut)[0][:OUT_R]:
                s.wait_send()

        def tiles(n, base, kind, body):
            @scoped("tile_" + "abc"[kind])
            def one(i):
                g = base + i
                fetch(g + slots - 1)
                slot = lax.rem(g, slots)
                at = jnp.minimum(i, n_a - 2) if kind == 0 else i
                for cp in tile_copies(kind, at, slot):
                    cp.wait()
                body(i, slot)

            loop(n, one)

        def chunk_step(c):
            base, slot_c = c * per, both(c)
            for i in (1, 2):
                pl.when(c == i)(lambda i=i: gathered(i))
            pl.when(c >= 1)(lambda: o_rows(c).start())
            pl.when(c >= 2)(lambda: release(c - 2))
            mlp_x(c).wait()
            pl.when(c + 1 < n_chunks)(lambda: start_x(c + 1))
            o_rows(c).wait()

            def tile_a(i, slot):
                at = span(i * WIDE, WIDE)
                part[slot_c, :, at] = x_buf[slot_c, :, at].astype(F32) + jnp.dot(o_buf[...], w_buf[slot], preferred_element_type=F32)

            tiles(n_a, base, 0, tile_a)
            y_own[both(c)] = part[slot_c, span(t * quarter, quarter, quarter), :]

            def norm2(i):
                at = span(i * NORM_ROWS, NORM_ROWS, NORM_ROWS)
                h_0[at, :] = (rms(part[slot_c, at, :]) * g2_ref[...].astype(F32)[None, :]).astype(BF16)

            loop(TILE // NORM_ROWS, norm2)
            pl.when(c == 0)(lambda: gather_on(1))
            pl.when(c >= 1)(lambda: middle(c - 1))

            def tile_b(i, slot):
                pair = jnp.dot(h_0[...], w_buf[slot], preferred_element_type=F32)
                act_buf[:, span(i * gate, gate)] = (jax.nn.silu(pair[:, :gate]) * pair[:, gate:]).astype(BF16)

            tiles(n_b, base + n_a, 1, tile_b)
            pl.when(c >= 2)(lambda: forward(c - 2))

            def tile_c(i, slot):
                part[slot_c, :, span(i * WIDE, WIDE)] = jnp.dot(act_buf[...], w_buf[slot, 0:ff, :], preferred_element_type=F32)
                for cut in range(PAIR):
                    pl.when(i == (cut + 1) * n_c // PAIR - 1)(lambda cut=cut: start(moves(c, cut)[0][:SUM_R]))

            tiles(n_c, base + n_a + n_b, 2, tile_c)
            pl.when(c == 0)(lambda: gather_on(2))
            if not exact:
                pl.when(c == 1)(sizes_known)
            pl.when(c >= 1)(lambda: finish(c - 1))

        def at_trip(events):
            def service(i):
                for when, what in events:
                    pl.when(i == when)(lambda what=what: (what(), None)[1])

            return service

        def suffix_early():
            pass_on(P_OWN)
            pass_on(P_SIB)
            start(ring(EARLY)[:K_ON])

        @scoped("w_on")
        def w_on():
            for b, c in zip(w_brings, w_sends[ON_UP:]):
                b.wait_recv()
                c.start()
            start([w_share(UP), w_share(DOWN)])

        def suffix_late():
            pass_on(EARLY)
            start(ring(LATE)[:K_ON])

        @scoped("early_o")
        def early_o():
            swap(OE, True).wait_recv()
            start(gathers[0][0][:ON_UP] + gathers[1][0][:ON_UP] + o_keeps[:2])

        @scoped("w_rest")
        def w_rest():
            for i in (ON_UP, ON_DOWN):
                w_brings[i].wait_recv()
                w_share(i).start()

        @scoped("first_tiles")
        def first_tiles():
            for b in w_theirs:
                b.wait_recv()
            start_x(0)
            for g in range(slots - 1):
                fetch(g)

        def trip(step):
            return lax.div(step - lead, main_unroll)

        e_done = lax.div(b7 + main_unroll - 1, main_unroll)
        trips = (n_main - lead) // main_unroll
        events = [
            (trip(qt), suffix_early),
            (trip(b2), lambda: [sides_here(P_OWN), sides_here(P_SIB)]),
            (trip(b4 - qt * pc), lambda: [far_here(P_OWN), far_here(P_SIB)]),
            (trip(b4 - qt), w_on),
            (trip(b4 - qt), suffix_late),
            (trip(b4), lambda: sides_here(EARLY)),
            (trip(jnp.where(chip < 2, b8, b6)), lambda: far_here(EARLY)),
            (e_done, lambda: finalize(0)),
            (e_done + 1, early_o),
            (trip(n_main - 40), lambda: [pass_on(LATE), w_last_round()]),
            (trip(b9), lambda: sides_here(LATE)),
            (trip(n_main - 20), w_rest),
            (trip(n_main - 8), first_tiles),
        ]
        events.append((trip(n_main - 8), lambda: gather_on(0)))
        far_late = trip(jnp.where(chip < 2, b9 + qt * (2 - chip), n_main))
        events.append((far_late, lambda: far_here(LATE)))
        if not exact:
            events.append((e_done + 2, sizes_meet))
        with jax.named_scope("run_main"):
            run(n_main, main_unroll, where, at_trip(events))

        pl.when(trip(b9) >= trips)(lambda: sides_here(LATE))
        pl.when(far_late >= trips)(lambda: far_here(LATE))
        finalize(1)
        with jax.named_scope("late_o"):
            swap(OL, True).wait_recv()
            start(gathers[2][0][:ON_UP] + o_keeps[2:])
        with jax.named_scope("gathered"):
            gathered(0)
        o_rows(0).start()
        loop(n_chunks, chunk_step)
        last = n_chunks - 1
        middle(last)
        forward(last - 1)
        finish(last)
        forward(last)
        with jax.named_scope("tail"):
            for c in new_copies + [flag_copy]:
                c.wait()
            loop(n_chunks, drain)
            release(last - 1)
            release(last)
            for i in range(OL + 1):
                swap(i).wait_send()
            for item in (P_OWN, P_SIB, EARLY, LATE):
                for c in ring(item):
                    c.wait_send()
            for c in w_sends + [w_share(i) for i in range(4)] + [w_last(i) for i in range(3 * tps - 2)] + sum([g[0] for g in gathers], []):
                c.wait_send()
            if not exact:
                for c in size_copies() + size_on():
                    c.wait_send()

    n_state = PAIR * side
    scratch = [
        pltpu.VMEM(shape, BF16)
        for shape in (
            (slots, d_in, WIDE), (2, TILE, d), (TILE, d), (TILE, d), (3, PAIR * hd, side), (send_pre + pre, hd), (send_pre + pre, hd), (pre, 2, hd), (pre, 2, hd)
        )
    ]
    scratch += [pltpu.VMEM((SUB, n_state), F32), pltpu.VMEM((hd, n_state), F32)]
    scratch += [pltpu.VMEM(shape, BF16) for shape in ((2, blk, n_wide), (2, blk, ratio * hd))]
    scratch += [pltpu.VMEM((groups, SUB, LANES), F32), pltpu.VMEM((tps, SUB, LANES), F32)]
    scratch += [pltpu.VMEM((TILE, d_in), BF16), pltpu.VMEM((TILE, ff), BF16)]
    scratch += [pltpu.VMEM(shape, F32) for shape in ((2, TILE, d), (2, 2, half, d), (2, 2, quarter, d), (2, quarter, d))]
    scratch += [pltpu.VMEM((n_chunks, quarter, d), BF16), pltpu.SMEM((1, 1), jnp.int32)]
    scratch += [pltpu.VMEM((blk, hd), F32)] * PAIR
    if exact:
        scratch += [pltpu.VMEM((1, n_state), F32)]
    scratch += [dma(*n) for n in ((7,), (2,), (10,), (10,), (4, 6), (4, 6), (4,), (4,), (4,), (4,), (3, 4), (3, 4))]
    scratch += [dma(groups)] * 2 + [dma(tps)] * 2 + [dma(3 * tps - 2)] * 2 + [dma(slots, tps), dma(n_chunks, 2, 10), dma(n_chunks, 2, 10), dma(n_chunks, 2)]
    shapes = [(rows, 2, hd)] * 2 + [(rows, d), (rows, d_in), (d_in, PAIR * w_half), (tps - 1, w_rows, WIDE)]
    return pl.pallas_call(
        kernel,
        in_specs=[HBM] * 3 + [VMEM] * 2 + [HBM] * 4 + [VMEM] + [HBM] * 3,
        out_specs=[HBM] * 7,
        out_shape=[jax.ShapeDtypeStruct(s, BF16) for s in shapes] + [jax.ShapeDtypeStruct((1, 1), jnp.int32)],
        scratch_shapes=scratch,
        compiler_params=pltpu.CompilerParams(collective_id=2 + exact, has_side_effects=True, vmem_limit_bytes=VMEM_LIMIT),
        name="layer_exact" if exact else "layer",
    )(x_loc, kp2, vp2, freq, norm_attn, w_query, w_key, w_value, w_out, norm_mlp, w_gate, w_up, w_down)


def emit_call(x_out, k_new, v_new):
    step = x_out.shape[0] // SUB

    def kernel(x_hbm, k_hbm, v_hbm, x_to, k_to, v_to, x_buf, k_buf, v_buf, r_sem, w_sem):
        moves = [[ref.at[pl.ds(i * step, step)] for ref in (x_hbm, x_buf, x_to)] for i in range(SUB)]
        moves += [(k_hbm, k_buf, k_to), (v_hbm, v_buf, v_to)]
        reads = [pltpu.make_async_copy(src, buf, r_sem.at[i]) for i, (src, buf, _) in enumerate(moves)]
        writes = [pltpu.make_async_copy(buf, dst, w_sem.at[i]) for i, (_, buf, dst) in enumerate(moves)]
        start(reads)
        for r, w in zip(reads, writes):
            r.wait()
            w.start()
        for w in writes:
            w.wait()

    arrays = (x_out, k_new, v_new)
    return pl.pallas_call(
        kernel,
        in_specs=[HBM] * len(arrays),
        out_specs=[HBM] * len(arrays),
        out_shape=[jax.ShapeDtypeStruct(a.shape, a.dtype) for a in arrays],
        scratch_shapes=[pltpu.VMEM(a.shape, a.dtype) for a in arrays] + [dma(SUB + len(arrays))] * 2,
        name="emit",
    )(*arrays)


def solution(mesh):
    groups = mesh.shape["cp"]
    tps = mesh.shape["tp"]

    def local_layer(x_loc, kp_loc, vp_loc, norm_attn, w_query, w_key, w_value, w_out, norm_mlp, w_gate, w_up, w_down):
        rows = x_loc.shape[0]
        pre_dev, kv_loc, hd = kp_loc.shape
        freq = jnp.asarray(np.tile(ROPE_THETA ** (-np.arange(0, hd, PAIR) / hd), PAIR)[None, :], F32)

        def layer(exact):
            return layer_call(
                exact, x_loc, kp_loc, vp_loc, freq, norm_attn, w_query, w_key, w_value, w_out, norm_mlp, w_gate, w_up, w_down, groups, tps
            )

        k_new, v_new, x_out, _, _, _, plain = layer(False)
        x_out = lax.cond(plain[0, 0] == 1, lambda: x_out, lambda: layer(True)[2])
        return tuple(emit_call(x_out, k_new, v_new))

    row_spec = P(("dp", "cp"), None)
    kv_spec = P(("dp", "cp"), "tp", None)
    col_spec = P(None, "tp")
    row_split = P("tp", None)
    vec_spec = P(None)
    return jax.shard_map(
        local_layer,
        mesh=mesh,
        in_specs=(row_spec, kv_spec, kv_spec, vec_spec, col_spec, col_spec, col_spec, row_split, vec_spec, col_spec, col_spec, row_split),
        out_specs=(row_spec, kv_spec, kv_spec),
        check_vma=False,
    )
```

```python
import jax
import jax.numpy as jnp
import numpy as np
from jax import lax
from jax.experimental import pallas as pl
from jax.experimental.pallas import tpu as pltpu
from jax.sharding import PartitionSpec as P

ROPE_THETA = 500000.0
NORM_EPS = 1e-5
LOG2E = 1.4426950408889634
F32 = jnp.float32
BF16 = jnp.bfloat16
MESH = pl.DeviceIdType.MESH
LANES = 128
PAIR = 2
SUB = 8
TILE = 256
NORM_ROWS = 32
WIDE = 512
VMEM_LIMIT = 67043328
S_LIMIT, V_LIMIT = 60.0, 40.0
HBM = pl.BlockSpec(memory_space=pl.ANY)
VMEM = pl.BlockSpec(memory_space=pltpu.VMEM)
(KP, VP, KE, VE, KL, VL, QE, QL, OE, OL) = range(10)
(K_RIGHT, V_RIGHT, K_LEFT, V_LEFT, K_ON, V_ON) = range(6)
(P_OWN, P_SIB, EARLY, LATE) = range(4)
(UP, DOWN, ON_UP, ON_DOWN) = range(4)
(FAR_R, FAR_L, NEAR_R, NEAR_L, SUM_R, SUM_L, OUT_R, OUT_L, ON_R, ON_L) = range(10)


def scoped(name):
    def deco(f):
        def g(*a):
            with jax.named_scope(name):
                return f(*a)

        return g

    return deco


def dma(*shape):
    return pltpu.SemaphoreType.DMA(shape)


def start(copies):
    for c in copies:
        c.start()


def span(at, size, unit=LANES):
    return pl.ds(pl.multiple_of(at, unit), size)


def both(v):
    return lax.rem(v, 2)


def fold_rows(values, op):
    rows, cols = values.shape
    return op(values.reshape(rows // SUB, SUB, cols), axis=0)


def rms(x):
    return x * lax.rsqrt(jnp.mean(x * x, axis=-1, keepdims=True) + NORM_EPS)


def loop(n, body):
    lax.fori_loop(0, n, lambda i, c: (body(i), c)[1], 0)


def remote(src, dst, sems, i, who):
    send, recv = sems
    return pltpu.make_async_remote_copy(src_ref=src, dst_ref=dst, send_sem=send.at[i], recv_sem=recv.at[i], device_id=who, device_id_type=MESH)


def gather_steps(at, sems, ranks, src=None):
    here, up, down, over, size = ranks
    half = size // PAIR
    to_up, to_down = {"tp": up}, {"tp": down}

    def move(i, rank, first, n, who, other=None):
        ref = at(rank, first, n)
        return remote(ref if other is None else other, ref, sems, i, who)

    sends = [
        move(UP, here, 0, size, to_up, src),
        move(DOWN, here, 0, size, to_down, src),
        move(ON_UP, down, 0, half, to_up),
        move(ON_DOWN, up, half, half, to_down),
    ]
    brings = [
        move(UP, down, 0, size, to_up),
        move(DOWN, up, 0, size, to_down),
        move(ON_UP, over, 0, half, to_up),
        move(ON_DOWN, over, half, half, to_down),
    ]
    return sends, brings


def layer_call(exact, x_loc, kp2, vp2, freq, norm_attn, w_query, w_key, w_value, w_out, norm_mlp, w_gate, w_up, w_down, groups, tps):
    rows, d = x_loc.shape
    blk = rows // PAIR
    hd = kp2.shape[2]
    heads = w_query.shape[1] // hd
    ratio = heads // PAIR
    pre = kp2.shape[0]
    chips = groups // PAIR
    assert chips == tps == 4 and pre == rows and hd == LANES and ratio == 3
    deep = PAIR * blk
    n_wide = heads * hd
    side = ratio * PAIR * blk
    half_side = side // PAIR
    per_chip = PAIR * pre
    suf = chips * per_chip
    send = suf + chips * PAIR * rows
    send_pre = send + rows
    d_out = w_out.shape[1]
    w_half = (d_out - WIDE) // PAIR
    w_rows = w_out.shape[0]
    w_part = w_rows // groups
    scale = LOG2E * hd**-0.5
    n_proj = n_wide + 4 * hd
    d_in = tps * n_wide
    ff = w_gate.shape[1]
    n_chunks = rows // TILE
    quarter = TILE // tps
    half = quarter // PAIR
    gate = WIDE // PAIR
    n_a, n_b, n_c = d // WIDE, ff // gate, d // WIDE
    per = n_a + n_b + n_c
    total = per * n_chunks
    slots = 4

    def kernel(x_hbm, kp_hbm, vp_hbm, freq_ref, g_ref, wq_hbm, wk_hbm, wv_hbm, wo_hbm, g2_ref, wg_hbm, wu_hbm, wd_hbm,
               k_out, v_out, out_hbm, o_hbm, wall_hbm, wlast_hbm, plain_out,
               w_buf, x_buf, h_0, h_1, q3, keys, vals, kp_buf, vp_buf, l_ref, a_ref, o_st, o_snd, size_all, size_tp,
               o_buf, act_buf, part, got1, got2, y_own, fin, flag, cos_ref, sin_ref, *rest):
        if exact:
            m_ref, *rest = rest
        l_sem, x_sem, sw_s, sw_r, x_s, x_r, w_s, w_r, d_s, d_r, o_s, o_r, z_s, z_r, y_s, y_r, e_s, e_r, t_sem, c_s, c_r, c_sem = rest
        me, t = lax.axis_index("cp"), lax.axis_index("tp")
        core, chip = both(me), lax.div(me, 2)
        sib = {"cp": me + 1 - PAIR * core}
        x_right, x_left = {"cp": lax.rem(me + 2, groups)}, {"cp": lax.rem(me + groups - 2, groups)}
        up, down, over = [lax.rem(t + j, tps) for j in (1, tps - 1, 2)]

        def local(i, src, dst):
            return pltpu.make_async_copy(src, dst, l_sem.at[i])

        def x_copy(i):
            return pltpu.make_async_copy(x_hbm.at[span(i * TILE, TILE)], x_buf.at[both(i)], x_sem.at[both(i)])

        vp_copy = local(0, vp_hbm, vp_buf)
        kp_copy = local(1, kp_hbm, kp_buf)
        pair_w = PAIR * hd

        def proj_w(pair):
            return pair * pair_w // WIDE, pl.ds(pair * pair_w % WIDE, pair_w)

        w_copies = []
        for pair in range(n_proj // pair_w):
            src, first = (wq_hbm, pair) if pair < ratio else ((wk_hbm, wv_hbm)[pair - ratio], 0)
            slot, lanes = proj_w(pair)
            w_copies.append(local(2 + pair, src.at[:, pl.ds(first * pair_w, pair_w)], w_buf.at[slot, :, lanes]))
        start([vp_copy, kp_copy, x_copy(0)] + w_copies + [x_copy(1)])

        greeted = [{"cp": lax.rem(me + j, groups)} for j in range(1, groups)] + [{"tp": lax.rem(t + j, tps)} for j in range(1, tps)]
        barrier = pltpu.get_barrier_semaphore()
        for who in greeted:
            pl.semaphore_signal(barrier, inc=1, device_id=who, device_id_type=MESH)

        def w_place(which):
            return lambda rank, first, size: wall_hbm.at[span(rank * w_rows + first, size), span(which * w_half, w_half)]

        w_ranks = (t, up, down, over, w_rows)
        w_sends, w_brings = gather_steps(w_place(core), (w_s, w_r), w_ranks, wo_hbm.at[:, span(core * w_half, w_half)])
        w_theirs = gather_steps(w_place(1 - core), (d_s, d_r), w_ranks)[1]

        def part_rows(who):
            return span(who * w_part, w_part, SUB)

        y_steps, x_steps, d_steps = range(tps - 1), range(tps - 1, PAIR * (tps - 1)), range(PAIR * (tps - 1), 3 * tps - 2)

        def w_last(i, arriving=False):
            if i in y_steps:
                src = wo_hbm.at[part_rows(me), pl.ds(PAIR * w_half, WIDE)]
                return remote(src, wlast_hbm.at[y_steps[-1] - i, part_rows(me)], (e_s, e_r), i, {"tp": lax.rem(t + i + 1, tps)})
            back = PAIR * (i - d_steps[0])
            if i in x_steps:
                back = PAIR * (i - y_steps[-1])
                to = {"cp": lax.rem(me + back, groups)}
                owner = lax.rem(me + groups - back, groups) if arriving else me
            else:
                to, owner = sib, lax.rem(me + groups - back, groups)
                if arriving:
                    owner = owner + 1 - PAIR * core
            ref = wlast_hbm.at[:, part_rows(owner)]
            return remote(ref, ref, (e_s, e_r), i, to)

        def w_last_round():
            for i in y_steps:
                w_last(i, True).wait_recv()
            start([w_last(i) for i in x_steps] + [w_last(d_steps[0])])

        @scoped("w_last_on")
        def w_last_on():
            for i in x_steps:
                w_last(i, True).wait_recv()
            start([w_last(i) for i in d_steps[1:]])

        @scoped("w_last_here")
        def w_last_here():
            for i in d_steps:
                w_last(i, True).wait_recv()

        def w_share(i):
            ref = w_brings[i].dst_ref
            return remote(ref, ref, (d_s, d_r), i, sib)

        def o_cols(which):
            return span(which * ratio * hd, ratio * hd)

        def swap(i, arriving=False):
            if i == KP:
                src, dst = keys.at[pl.ds(send_pre, pre)], keys.at[pl.ds(pre, pre)]
            elif i == VP:
                src, dst = vals.at[pl.ds(send_pre, pre)], vals.at[pl.ds(pre, pre)]
            elif i in (KE, VE, KL, VL):
                buf, late = keys if i in (KE, KL) else vals, i in (KL, VL)
                src, dst = buf.at[pl.ds(send + late * blk, blk)], buf.at[pl.ds(suf + late * deep + blk, blk)]
            elif i in (QE, QL):
                at = pl.ds((i - QE) * half_side, half_side)
                src, dst = q3.at[2, :, at], q3.at[1, :, at]
            else:
                src, dst = o_snd.at[i - OE], o_st.at[i - OE, :, o_cols(1 - core if arriving else core)]
            return remote(src, dst, (sw_s, sw_r), i, sib)

        def region(item, slot):
            if item in (P_OWN, P_SIB):
                return pl.ds(slot * per_chip + item * pre, pre)
            return pl.ds(suf + (PAIR * slot + item - EARLY) * deep, deep)

        def ring(item):
            plan = {K_RIGHT: (keys, 0, 1, x_right), V_RIGHT: (vals, 0, 1, x_right), K_LEFT: (keys, 0, 3, x_left), V_LEFT: (vals, 0, 3, x_left),
                    K_ON: (keys, 1, 2, x_right), V_ON: (vals, 3, 2, x_left)}
            return [remote(buf.at[region(item, a)], buf.at[region(item, b)], (x_s.at[item], x_r.at[item]), i, who) for i, (buf, a, b, who) in plan.items()]

        @scoped("ring_on")
        def pass_on(item):
            got = ring(item)
            got[K_RIGHT].wait_recv()
            got[K_ON].start()
            got[V_LEFT].wait_recv()
            got[V_ON].start()

        @scoped("wait_sides")
        def sides_here(item):
            got = ring(item)
            got[V_RIGHT].wait_recv()
            got[K_LEFT].wait_recv()

        @scoped("wait_far")
        def far_here(item):
            got = ring(item)
            got[K_ON].wait_recv()
            got[V_ON].wait_recv()

        h_bufs = (h_0, h_1)

        def norm(i, slot):
            g = g_ref[...].astype(F32)[None, :]
            for r in range(0, TILE, NORM_ROWS):
                h_bufs[slot][r : r + NORM_ROWS, :] = (rms(x_buf[slot, r : r + NORM_ROWS, :].astype(F32)) * g).astype(BF16)

        def project(i, slot):
            h_tile = h_bufs[slot]
            late, sub = lax.div(i, blk // TILE), lax.rem(i, blk // TILE)
            at_rows = span(i * TILE, TILE)
            tab = span(sub * TILE, TILE)
            first = lax.broadcasted_iota(jnp.int32, (TILE, hd), 1) < hd // PAIR

            def table(ref):
                v = ref[tab, :]
                w = pltpu.roll(v, hd // PAIR, 1)
                return jnp.where(first == (late == 0), v, w)

            cos, sin = table(cos_ref), table(sin_ref)
            sin = jnp.where(first, -sin, sin)

            def rope(v):
                return v * cos + pltpu.roll(v, hd // PAIR, 1) * sin

            for pair in range(n_proj // pair_w):
                slot, w_lanes = proj_w(pair)
                out = jnp.dot(h_tile[...], w_buf[slot, :, w_lanes], preferred_element_type=F32)
                heads_new = []
                for hh in range(PAIR):
                    v = out[:, hh * hd : (hh + 1) * hd]
                    head = PAIR * pair + hh
                    at = jnp.where(core == hh, suf + late * deep, send + late * blk) + sub * TILE
                    if head < heads:
                        q_t = rope(v).astype(BF16).astype(F32).T
                        if not exact:
                            n2 = jnp.max(jnp.sum(fold_rows(q_t * q_t, jnp.sum), axis=0, keepdims=True), axis=1, keepdims=True)
                            note(0, jnp.broadcast_to(n2, (1, LANES)))
                        q_t = q_t * scale
                        hi = q_t.astype(BF16)
                        idx = jnp.where(core == head // ratio, 0, 2)
                        col = span(late * half_side + (head % ratio) * blk + sub * TILE, TILE)
                        q3[idx, pl.ds(0, hd), col] = hi
                        q3[idx, pl.ds(hd, hd), col] = (q_t - hi.astype(F32)).astype(BF16)
                    elif head < heads + 2:
                        k = rope(v).astype(BF16)
                        keys[span(at, TILE), :] = k
                        heads_new.append(k)
                        note_rows(1, k.astype(F32))
                    else:
                        v = v.astype(BF16)
                        heads_new.append(v)
                        v_t = v.astype(F32).T
                        note_size(2, v.astype(F32))
                        for b in range(0, TILE, LANES):
                            vals[span(at + b, LANES), :] = v_t[:, b : b + LANES].astype(BF16)
                if heads_new:
                    (kp_buf, vp_buf)[pair - ratio][at_rows] = jnp.concatenate(heads_new, axis=1).reshape(TILE, 2, hd)

        def angles(i):
            shape, at = (NORM_ROWS, hd), span(i * NORM_ROWS, NORM_ROWS, NORM_ROWS)
            early = lax.broadcasted_iota(jnp.int32, shape, 1) < hd // PAIR
            row = lax.broadcasted_iota(jnp.int32, shape, 0) + i * NORM_ROWS
            block = jnp.where(early, me, PAIR * groups - 1 - me)
            angle = (pre * groups + block * blk + row).astype(F32) * freq_ref[...]
            cos_ref[at, :] = jnp.cos(angle)
            sin_ref[at, :] = jnp.sin(angle)

        with jax.named_scope("angles"):
            loop(blk // NORM_ROWS, angles)
        kp_copy.wait()
        vp_copy.wait()
        if not exact:
            size_all[0] = jnp.zeros(size_all.shape[1:], F32)

        def note(i, v):
            if not exact:
                size_all[0, i : i + 1, :] = jnp.maximum(size_all[0, i : i + 1, :], v)

        def note_rows(i, v):
            if not exact:
                n2 = jnp.sum(v * v, axis=1, keepdims=True)
                note(i, jnp.broadcast_to(jnp.max(n2, axis=0, keepdims=True), (1, LANES)))

        def note_size(i, v):
            if not exact:
                note(i, jnp.max(fold_rows(jnp.abs(v), jnp.max), axis=0, keepdims=True))

        def split_prefix(b):
            rows_b = span(b * LANES, LANES)
            k, v = [buf[rows_b].reshape(LANES, PAIR * hd) for buf in (kp_buf, vp_buf)]
            for j in range(PAIR):
                at = span(jnp.where(core == j, 0, send_pre) + b * LANES, LANES)
                k_j, v_j = k[:, j * hd : (j + 1) * hd], v[:, j * hd : (j + 1) * hd].astype(F32)
                keys[at, :] = k_j
                vals[at, :] = v_j.T.astype(BF16)
                note_rows(1, k_j.astype(F32))
                note_size(2, v_j)

        loop(pre // LANES, split_prefix)
        with jax.named_scope("barrier"):
            pl.semaphore_wait(barrier, len(greeted))
        start([swap(KP), swap(VP)] + ring(P_OWN)[:K_ON] + [w_last(i) for i in y_steps] + w_sends[:ON_UP])
        with jax.named_scope("x_wait"):
            x_copy(0).wait()
        norm(0, 0)
        with jax.named_scope("w_wait"):
            for c in w_copies:
                c.wait()

        n_tiles = rows // TILE

        @scoped("project")
        def two_tiles(j):
            i = PAIR * j
            x_copy(i + 1).wait()

            @pl.when(i + 2 < n_tiles)
            def _():
                x_copy(i + 2).start()

            norm(i + 1, 1)
            project(i, 0)

            @pl.when(j == 0)
            def _():
                swap(KP).wait_recv()
                swap(VP).wait_recv()
                start(ring(P_SIB)[:K_ON])

            @pl.when(i + 2 < n_tiles)
            def _():
                x_copy(i + 3).start()
                x_copy(i + 2).wait()

            norm(i + 2, 0)
            project(i + 1, 1)

            @pl.when(j == 0)
            def _():
                start([swap(i) for i in (KE, VE, QE)])

        loop(n_tiles // PAIR, two_tiles)
        start([swap(i) for i in (KL, VL, QL)])
        new_copies = [local(4, kp_buf, k_out), local(5, vp_buf, v_out)]
        start(new_copies)

        def size_copies():
            out = []
            for j in range(1, groups):
                out.append(remote(size_all.at[0], size_all.at[j], (z_s, z_r), j, {"cp": lax.rem(me + j, groups)}))
            return out

        def size_on():
            return [remote(size_tp.at[0], size_tp.at[j], (y_s, y_r), j, {"tp": lax.rem(t + j, tps)}) for j in range(1, tps)]

        flag_copy = local(6, flag, plain_out)

        def sizes_known():
            for c in size_on():
                c.wait_recv()
            top = jnp.max(jnp.max(size_tp[...], axis=0), axis=1)
            fits = (scale * scale * top[0] * top[1] <= S_LIMIT**2) & (top[2] <= 2.0**V_LIMIT)
            flag[0, 0] = fits.astype(jnp.int32)
            flag_copy.start()

        def sizes_meet():
            for c in size_copies():
                c.wait_recv()
            size_tp[0] = jnp.max(size_all[...], axis=0)
            start(size_on())

        if not exact:
            start(size_copies())
        if exact:
            flag[0, 0] = 1
            flag_copy.start()
            m_ref[...] = jnp.full_like(m_ref, -jnp.inf)
        l_ref[...] = jnp.zeros_like(l_ref)
        a_ref[...] = jnp.zeros_like(a_ref)
        with jax.named_scope("swap_wait"):
            for i in range(KE, OE):
                swap(i).wait_recv()

        p_bufs = (o_buf, act_buf)

        def beside(r):
            return pl.ds(r // TILE * blk, blk)

        lead = 0 if exact else 1
        main_unroll = 1 if exact else 4

        def state_at(step):
            who, late, head = step[:3]
            return span(who * side + late * half_side + head * blk, blk)

        def product(step, r, n, shifts):
            who, late, head, key = step
            k = keys[span(key + r, n), :]
            s = jnp.dot(jnp.concatenate([k, k], axis=1), q3[who, :, span(late * half_side + head * blk, blk)], preferred_element_type=F32)
            if shifts is not None:
                row = lax.broadcasted_iota(jnp.int32, s.shape, 0) + r % blk
                col = lax.broadcasted_iota(jnp.int32, s.shape, 1) + shifts[r // blk]
                s = jnp.where(row <= col, s, -jnp.inf)
            return s

        def weights(step, slot, shifts):
            total = None
            for r in range(0, deep, TILE):
                p = jnp.exp2(product(step, r, TILE, shifts))
                p_bufs[slot][:, beside(r)] = p.astype(BF16)
                t8 = fold_rows(p, jnp.sum)
                total = t8 if total is None else total + t8
            l_ref[:, state_at(step)] += total

        def values(step, slot):
            v = jnp.concatenate([vals[span(step[3] + b, LANES), :] for b in range(0, deep, LANES)], axis=1)
            p = jnp.concatenate([p_bufs[slot][:, beside(r)] for r in range(0, deep, TILE)], axis=0)
            a_ref[:, state_at(step)] += jnp.dot(v, p, preferred_element_type=F32)

        def exact_step(step, shifts):
            cols = state_at(step)
            top = m_old = m_ref[:, cols]
            for r in range(0, deep, TILE):
                s = product(step, r, TILE, shifts)
                part[0, :, beside(r)] = s
                top = jnp.maximum(top, jnp.max(s, axis=0, keepdims=True))
            corr = jnp.exp2(m_old - top)
            m_ref[:, cols] = top
            total = l_ref[:, cols] * corr
            for r in range(0, deep, TILE):
                p = jnp.exp2(part[0, :, beside(r)] - top)
                o_buf[:, beside(r)] = p.astype(BF16)
                total += fold_rows(p, jnp.sum)
            l_ref[:, cols] = total
            a_ref[:, cols] = a_ref[:, cols] * corr
            values(step, 0)

        def run(n_steps, unroll, where, service, mask=None):
            def shifts(step):
                return None if mask is None else mask(step)

            def ahead(u, slot):
                weights(where(u), slot, shifts(where(u)))

            if not exact:
                ahead(0, 0)

            @scoped("body")
            def body(i):
                service(i)
                for j in range(unroll):
                    u = unroll * i + j
                    if exact:
                        exact_step(where(u), shifts(where(u)))
                    else:
                        ahead(u + 1, (j + 1) % 2)
                        values(where(u), j % 2)

            trips = (n_steps - lead) // unroll
            loop(trips, body)
            for u in range(unroll * trips, n_steps):
                if u + 1 < n_steps:
                    ahead(u + 1, (u + 1) % 2)
                values(where(u), u % 2)

        def own_where(u):
            who, rest = lax.div(u, PAIR * ratio), lax.rem(u, PAIR * ratio)
            late, head = lax.div(rest, ratio), lax.rem(rest, ratio)
            return who, late, head, suf + late * deep

        def own_mask(step):
            who, late = step[:2]
            q_core = jnp.where(who == 0, core, 1 - core)
            seen = jnp.where(late == 0, q_core, 1 - q_core)
            other = (PAIR * seen - 1) * blk
            return jnp.where(who == 0, 0, other), jnp.where(who == 0, other, 0)

        with jax.named_scope("run_own"):
            run(4 * ratio, 1 if exact else 2, own_where, lambda i: None, own_mask)

        qt = PAIR * ratio
        pc = per_chip // deep
        n_rem = chips - 1
        n_near = jnp.minimum(chip, 1) + lax.div(chip, n_rem)
        b1 = PAIR * qt * pc
        b2 = b1 + qt
        b4 = b2 + n_rem * qt * pc
        b5 = b4 + qt * n_near
        b6 = b5 + qt
        b7 = b6 + qt * (chip - n_near)
        b8 = b7 + n_rem * qt * pc - qt
        b9 = b8 + qt * n_rem
        n_main = b4 + n_rem * qt * pc + PAIR * qt * n_rem

        def where(u):
            def prefix(j):
                i, r = lax.div(j, qt * pc), lax.rem(j, qt * pc)
                return lax.div(r, pc), far_last(i) * per_chip + lax.rem(r, pc) * deep

            def far_last(i):
                return jnp.where(i == 0, 1, jnp.where(i == 1, n_rem, 2))

            def suffix(j, back):
                return lax.rem(j, qt), suf + back * PAIR * deep

            tile = lax.div(u, pc)
            late = lax.div(tile, qt)
            q_i, key = lax.rem(tile, qt), lax.rem(u, pc) * deep
            j9 = suffix(u - b9, far_last(jnp.minimum(chip, 1) + lax.div(u - b9, qt)))
            for first, is_late, (q_n, key_n) in (
                (b1, 1, (u - b1, suf)),
                (b2, 0, prefix(u - b2)),
                (b4, 0, suffix(u - b4, far_last(lax.div(u - b4, qt)))),
                (b5, 1, prefix(u - b5)),
                (b6, 0, suffix(u - b6, 2)),
                (b7, 1, prefix(u - b7 + qt)),
                (b8, 1, (lax.div(u - b8, n_rem), suf + (1 + lax.rem(u - b8, n_rem)) * PAIR * deep)),
                (b9, 1, (j9[0], j9[1] + deep)),
            ):
                here = u >= first
                late, q_i, key = [jnp.where(here, a, b) for a, b in ((is_late, late), (q_n, q_i), (key_n, key))]
            return lax.div(q_i, ratio), late, lax.rem(q_i, ratio), key

        @scoped("finalize")
        def finalize(h):
            for who in range(PAIR):
                for head in range(ratio):
                    at = state_at((who, h, head))
                    inv = 1.0 / jnp.sum(l_ref[:, at], axis=0, keepdims=True)
                    o = (a_ref[:, at] * inv).T.astype(BF16)
                    if who == 0:
                        o_st[h, :, span(core * ratio * hd + head * hd, hd)] = o
                    else:
                        o_snd[h, :, span(head * hd, hd)] = o
            swap(OE + h).start()

        gathers, o_keeps = [], []
        for i, (h, first, n) in enumerate(((0, 0, TILE), (0, TILE, blk - TILE), (1, 0, blk))):
            place = lambda rank, at, size, base=h * blk + first: o_hbm.at[pl.ds(base + at, size), span(rank * n_wide, n_wide)]
            src = o_st.at[h, pl.ds(first, n)]
            gathers.append(gather_steps(place, (o_s.at[i], o_r.at[i]), (t, up, down, over, n), src))
            o_keeps.append(local(i, src, place(t, 0, n)))

        def gather_on(i):
            sends, brings = gathers[i]
            for b, s in zip(brings, sends[ON_UP:]):
                b.wait_recv()
                s.start()

        def gathered(i):
            for b in gathers[i][1][ON_UP:]:
                b.wait_recv()
            o_keeps[i].wait()

        def tile_copies(kind, i, slot):
            def get(j, src, dst):
                return pltpu.make_async_copy(src, dst, t_sem.at[slot, j])

            if kind in (0, 3):
                cols, out = span(i * WIDE, WIDE), []
                for j in range(tps):
                    rank = lax.rem(t + j, tps)
                    at = span(rank * n_wide, n_wide)
                    src = wo_hbm.at[:, cols] if j == 0 else wlast_hbm.at[j - 1] if kind == 3 else wall_hbm.at[at, cols]
                    out.append(get(j, src, w_buf.at[slot, at]))
                return out
            if kind == 1:
                at = span(i * gate, gate)
                return [get(j, w.at[:, at], w_buf.at[slot, :, pl.ds(j * gate, gate)]) for j, w in enumerate((wg_hbm, wu_hbm))]
            return [get(0, wd_hbm.at[:, span(i * WIDE, WIDE)], w_buf.at[slot, pl.ds(0, ff)])]

        def fetch(g):
            i, slot = lax.rem(g, per), lax.rem(g, slots)
            last_a = n_a - 1
            pl.when(g == slots)(w_last_on)
            pl.when(g == last_a)(w_last_here)
            for kind, first, n in ((0, 0, last_a), (3, last_a, 1), (1, n_a, n_b), (2, n_a + n_b, n_c)):
                pl.when((g < total) & (i >= first) & (i < first + n))(lambda: start(tile_copies(kind, last_a if kind == 3 else i - first, slot)))

        def mlp_x(c):
            return pltpu.make_async_copy(x_hbm.at[span(c * TILE, TILE)], x_buf.at[both(c)], x_sem.at[both(c)])

        def start_x(c):
            mlp_x(c).start()

        def o_rows(c):
            return local(3, o_hbm.at[span(c * TILE, TILE)], o_buf)

        def cols_of(cut):
            return span(cut * d // PAIR, d // PAIR)

        def moves(c, cut):
            cols, slot = cols_of(cut), both(c)

            def go(i, src, dst):
                return remote(src, dst, (c_s.at[c, cut], c_r.at[c, cut]), i, {"tp": up if i % 2 == 0 else down})

            def mine(q, first):
                return part.at[slot, span(q * quarter + first, half, half), cols]

            def out(q, first, n):
                return out_hbm.at[span(c * TILE + q * quarter + first, n, half), cols]

            def sums(way, first):
                return got2.at[slot, way, pl.ds(first, half), cols]

            done = fin.at[c, :, cols]
            sends = {
                FAR_R: (mine(over, 0), got1.at[slot, 0, :, cols]),
                FAR_L: (mine(over, half), got1.at[slot, 1, :, cols]),
                NEAR_R: (mine(up, half), sums(0, half)),
                NEAR_L: (mine(down, 0), sums(1, 0)),
                SUM_R: (mine(up, 0), sums(0, 0)),
                SUM_L: (mine(down, half), sums(1, half)),
                OUT_R: (done, out(t, 0, quarter)),
                OUT_L: (done, out(t, 0, quarter)),
                ON_R: (out(down, 0, half), out(down, 0, half)),
                ON_L: (out(up, half, half), out(up, half, half)),
            }
            brings = {
                OUT_R: (done, out(down, 0, quarter)),
                OUT_L: (done, out(up, 0, quarter)),
                ON_R: (out(over, 0, half), out(over, 0, half)),
                ON_L: (out(over, half, half), out(over, half, half)),
            }
            own = pltpu.make_async_copy(done, out(t, 0, quarter), c_sem.at[c, cut])
            return [go(i, *m) for i, m in sends.items()], {i: go(i, *m) for i, m in brings.items()}, own

        def cuts(name):
            def deco(f):
                return scoped(name)(lambda c: loop(2, lambda cut: f(c, cut)))

            return deco

        @cuts("middle")
        def middle(c, cut):
            m = moves(c, cut)[0]
            for way, q, first in ((0, up, 0), (1, down, half)):
                m[FAR_R + way].wait_recv()
                part[both(c), span(q * quarter + first, half, half), cols_of(cut)] += got1[both(c), way, :, cols_of(cut)]
                m[SUM_R + way].start()

        @cuts("finish")
        def finish(c, cut):
            m, _, own = moves(c, cut)
            for i in (NEAR_R, NEAR_L, SUM_R, SUM_L):
                m[i].wait_recv()
            cols, slot = cols_of(cut), both(c)
            rest = got2[slot, 0, :, cols] + got2[slot, 1, :, cols]
            fin[c, :, cols] = (y_own[slot, :, cols] + (part[slot, span(t * quarter, quarter, quarter), cols] + rest)).astype(BF16)
            own.start()
            start(m[OUT_R:ON_R])

        @cuts("forward")
        def forward(c, cut):
            m, b, _ = moves(c, cut)
            for way in range(PAIR):
                b[OUT_R + way].wait_recv()
                m[ON_R + way].start()

        @cuts("drain")
        def drain(c, cut):
            m, b, own = moves(c, cut)
            b[ON_R].wait_recv()
            b[ON_L].wait_recv()
            for s in m[OUT_R:]:
                s.wait_send()
            own.wait()

        @cuts("release")
        def release(c, cut):
            for s in moves(c, cut)[0][:OUT_R]:
                s.wait_send()

        def tiles(n, base, kind, body):
            @scoped("tile_" + "abc"[kind])
            def one(i):
                g = base + i
                fetch(g + slots - 1)
                slot = lax.rem(g, slots)
                at = jnp.minimum(i, n_a - 2) if kind == 0 else i
                for cp in tile_copies(kind, at, slot):
                    cp.wait()
                body(i, slot)

            loop(n, one)

        def chunk_step(c):
            base, slot_c = c * per, both(c)
            for i in (1, 2):
                pl.when(c == i)(lambda i=i: gathered(i))
            pl.when(c >= 1)(lambda: o_rows(c).start())
            pl.when(c >= 2)(lambda: release(c - 2))
            mlp_x(c).wait()
            pl.when(c + 1 < n_chunks)(lambda: start_x(c + 1))
            o_rows(c).wait()

            def tile_a(i, slot):
                at = span(i * WIDE, WIDE)
                part[slot_c, :, at] = x_buf[slot_c, :, at].astype(F32) + jnp.dot(o_buf[...], w_buf[slot], preferred_element_type=F32)

            tiles(n_a, base, 0, tile_a)
            y_own[both(c)] = part[slot_c, span(t * quarter, quarter, quarter), :]

            def norm2(i):
                at = span(i * NORM_ROWS, NORM_ROWS, NORM_ROWS)
                h_0[at, :] = (rms(part[slot_c, at, :]) * g2_ref[...].astype(F32)[None, :]).astype(BF16)

            loop(TILE // NORM_ROWS, norm2)
            pl.when(c == 0)(lambda: gather_on(1))
            pl.when(c >= 1)(lambda: middle(c - 1))

            def tile_b(i, slot):
                pair = jnp.dot(h_0[...], w_buf[slot], preferred_element_type=F32)
                act_buf[:, span(i * gate, gate)] = (jax.nn.silu(pair[:, :gate]) * pair[:, gate:]).astype(BF16)

            tiles(n_b, base + n_a, 1, tile_b)
            pl.when(c >= 2)(lambda: forward(c - 2))

            def tile_c(i, slot):
                part[slot_c, :, span(i * WIDE, WIDE)] = jnp.dot(act_buf[...], w_buf[slot, 0:ff, :], preferred_element_type=F32)
                for cut in range(PAIR):
                    pl.when(i == (cut + 1) * n_c // PAIR - 1)(lambda cut=cut: start(moves(c, cut)[0][:SUM_R]))

            tiles(n_c, base + n_a + n_b, 2, tile_c)
            pl.when(c == 0)(lambda: gather_on(2))
            if not exact:
                pl.when(c == 1)(sizes_known)
            pl.when(c >= 1)(lambda: finish(c - 1))

        def at_trip(events):
            def service(i):
                for when, what in events:
                    pl.when(i == when)(lambda what=what: (what(), None)[1])

            return service

        def suffix_early():
            pass_on(P_OWN)
            pass_on(P_SIB)
            start(ring(EARLY)[:K_ON])

        @scoped("w_on")
        def w_on():
            for b, c in zip(w_brings, w_sends[ON_UP:]):
                b.wait_recv()
                c.start()
            start([w_share(UP), w_share(DOWN)])

        def suffix_late():
            pass_on(EARLY)
            start(ring(LATE)[:K_ON])

        @scoped("early_o")
        def early_o():
            swap(OE, True).wait_recv()
            start(gathers[0][0][:ON_UP] + o_keeps[:2])

        @scoped("w_rest")
        def w_rest():
            for i in (ON_UP, ON_DOWN):
                w_brings[i].wait_recv()
                w_share(i).start()

        @scoped("first_tiles")
        def first_tiles():
            for b in w_theirs:
                b.wait_recv()
            start_x(0)
            for g in range(slots - 1):
                fetch(g)

        def trip(step):
            return lax.div(step - lead, main_unroll)

        e_done = lax.div(b7 + main_unroll - 1, main_unroll)
        trips = (n_main - lead) // main_unroll
        events = [
            (trip(qt), suffix_early),
            (trip(b2), lambda: [sides_here(P_OWN), sides_here(P_SIB)]),
            (trip(b4 - qt * pc), lambda: [far_here(P_OWN), far_here(P_SIB)]),
            (trip(b4 - qt), w_on),
            (trip(b4 - qt), suffix_late),
            (trip(b4), lambda: sides_here(EARLY)),
            (trip(jnp.where(chip < 2, b8, b6)), lambda: far_here(EARLY)),
            (e_done, lambda: finalize(0)),
            (e_done + 1, early_o),
            (trip(n_main - 40), lambda: [pass_on(LATE), w_last_round()]),
            (trip(b9), lambda: sides_here(LATE)),
            (trip(n_main - 20), w_rest),
            (trip(n_main - 8), first_tiles),
        ]
        events.append((trip(n_main - 12), lambda: [gather_on(0), start(gathers[1][0][:ON_UP])]))
        far_late = trip(jnp.where(chip < 2, b9 + qt * (2 - chip), n_main))
        events.append((far_late, lambda: far_here(LATE)))
        if not exact:
            events.append((e_done + 2, sizes_meet))
        with jax.named_scope("run_main"):
            run(n_main, main_unroll, where, at_trip(events))

        pl.when(trip(b9) >= trips)(lambda: sides_here(LATE))
        pl.when(far_late >= trips)(lambda: far_here(LATE))
        finalize(1)
        with jax.named_scope("late_o"):
            swap(OL, True).wait_recv()
            start(gathers[2][0][:ON_UP] + o_keeps[2:])
        with jax.named_scope("gathered"):
            gathered(0)
        o_rows(0).start()
        loop(n_chunks, chunk_step)
        last = n_chunks - 1
        middle(last)
        forward(last - 1)
        finish(last)
        forward(last)
        with jax.named_scope("tail"):
            for c in new_copies + [flag_copy]:
                c.wait()
            loop(n_chunks, drain)
            release(last - 1)
            release(last)
            for i in range(OL + 1):
                swap(i).wait_send()
            for item in (P_OWN, P_SIB, EARLY, LATE):
                for c in ring(item):
                    c.wait_send()
            for c in w_sends + [w_share(i) for i in range(4)] + [w_last(i) for i in range(3 * tps - 2)] + sum([g[0] for g in gathers], []):
                c.wait_send()
            if not exact:
                for c in size_copies() + size_on():
                    c.wait_send()

    n_state = PAIR * side
    scratch = [
        pltpu.VMEM(shape, BF16)
        for shape in (
            (slots, d_in, WIDE), (2, TILE, d), (TILE, d), (TILE, d), (3, PAIR * hd, side), (send_pre + pre, hd), (send_pre + pre, hd), (pre, 2, hd), (pre, 2, hd)
        )
    ]
    scratch += [pltpu.VMEM((SUB, n_state), F32), pltpu.VMEM((hd, n_state), F32)]
    scratch += [pltpu.VMEM(shape, BF16) for shape in ((2, blk, n_wide), (2, blk, ratio * hd))]
    scratch += [pltpu.VMEM((groups, SUB, LANES), F32), pltpu.VMEM((tps, SUB, LANES), F32)]
    scratch += [pltpu.VMEM((TILE, d_in), BF16), pltpu.VMEM((TILE, ff), BF16)]
    scratch += [pltpu.VMEM(shape, F32) for shape in ((2, TILE, d), (2, 2, half, d), (2, 2, quarter, d), (2, quarter, d))]
    scratch += [pltpu.VMEM((n_chunks, quarter, d), BF16), pltpu.SMEM((1, 1), jnp.int32)]
    scratch += [pltpu.VMEM((blk, hd), F32)] * PAIR
    if exact:
        scratch += [pltpu.VMEM((1, n_state), F32)]
    scratch += [dma(*n) for n in ((7,), (2,), (10,), (10,), (4, 6), (4, 6), (4,), (4,), (4,), (4,), (3, 4), (3, 4))]
    scratch += [dma(groups)] * 2 + [dma(tps)] * 2 + [dma(3 * tps - 2)] * 2 + [dma(slots, tps), dma(n_chunks, 2, 10), dma(n_chunks, 2, 10), dma(n_chunks, 2)]
    shapes = [(rows, 2, hd)] * 2 + [(rows, d), (rows, d_in), (d_in, PAIR * w_half), (tps - 1, w_rows, WIDE)]
    return pl.pallas_call(
        kernel,
        in_specs=[HBM] * 3 + [VMEM] * 2 + [HBM] * 4 + [VMEM] + [HBM] * 3,
        out_specs=[HBM] * 7,
        out_shape=[jax.ShapeDtypeStruct(s, BF16) for s in shapes] + [jax.ShapeDtypeStruct((1, 1), jnp.int32)],
        scratch_shapes=scratch,
        compiler_params=pltpu.CompilerParams(collective_id=2 + exact, has_side_effects=True, vmem_limit_bytes=VMEM_LIMIT),
        name="layer_exact" if exact else "layer",
    )(x_loc, kp2, vp2, freq, norm_attn, w_query, w_key, w_value, w_out, norm_mlp, w_gate, w_up, w_down)


def emit_call(x_out, k_new, v_new):
    step = x_out.shape[0] // SUB

    def kernel(x_hbm, k_hbm, v_hbm, x_to, k_to, v_to, x_buf, k_buf, v_buf, r_sem, w_sem):
        moves = [[ref.at[pl.ds(i * step, step)] for ref in (x_hbm, x_buf, x_to)] for i in range(SUB)]
        moves += [(k_hbm, k_buf, k_to), (v_hbm, v_buf, v_to)]
        reads = [pltpu.make_async_copy(src, buf, r_sem.at[i]) for i, (src, buf, _) in enumerate(moves)]
        writes = [pltpu.make_async_copy(buf, dst, w_sem.at[i]) for i, (_, buf, dst) in enumerate(moves)]
        start(reads)
        for r, w in zip(reads, writes):
            r.wait()
            w.start()
        for w in writes:
            w.wait()

    arrays = (x_out, k_new, v_new)
    return pl.pallas_call(
        kernel,
        in_specs=[HBM] * len(arrays),
        out_specs=[HBM] * len(arrays),
        out_shape=[jax.ShapeDtypeStruct(a.shape, a.dtype) for a in arrays],
        scratch_shapes=[pltpu.VMEM(a.shape, a.dtype) for a in arrays] + [dma(SUB + len(arrays))] * 2,
        name="emit",
    )(*arrays)


def solution(mesh):
    groups = mesh.shape["cp"]
    tps = mesh.shape["tp"]

    def local_layer(x_loc, kp_loc, vp_loc, norm_attn, w_query, w_key, w_value, w_out, norm_mlp, w_gate, w_up, w_down):
        rows = x_loc.shape[0]
        pre_dev, kv_loc, hd = kp_loc.shape
        freq = jnp.asarray(np.tile(ROPE_THETA ** (-np.arange(0, hd, PAIR) / hd), PAIR)[None, :], F32)

        def layer(exact):
            return layer_call(
                exact, x_loc, kp_loc, vp_loc, freq, norm_attn, w_query, w_key, w_value, w_out, norm_mlp, w_gate, w_up, w_down, groups, tps
            )

        k_new, v_new, x_out, _, _, _, plain = layer(False)
        x_out = lax.cond(plain[0, 0] == 1, lambda: x_out, lambda: layer(True)[2])
        return tuple(emit_call(x_out, k_new, v_new))

    row_spec = P(("dp", "cp"), None)
    kv_spec = P(("dp", "cp"), "tp", None)
    col_spec = P(None, "tp")
    row_split = P("tp", None)
    vec_spec = P(None)
    return jax.shard_map(
        local_layer,
        mesh=mesh,
        in_specs=(row_spec, kv_spec, kv_spec, vec_spec, col_spec, col_spec, col_spec, row_split, vec_spec, col_spec, col_spec, row_split),
        out_specs=(row_spec, kv_spec, kv_spec),
        check_vma=False,
    )
```
